8 devices in a mesh: kpt: 1 (over z), col: 2 (over y), row: 4 (over x, core).
Axes of the slice: x: 2, y: 2, z: 1, core: 2. Of those that a mesh axis runs over, the one named last changes fastest.
Arguments:
- z_in: float32 [6144, 1024], P('kpt', ('col', 'row'))
- v_panels: float32 [6144, 6144], P(('kpt', 'row'), 'col')
- t_factors: float32 [192, 32, 32], P('kpt')
Outputs:
- output: float32 [6144, 1024], P(('kpt', 'row'), 'col')
All inputs are finite; a program needn't handle non-finite values.
Results may differ from the reference program's by a relative error of at most 0.001.
Values sent between devices are 32-bit elements.
A program may use at most 1 GiB of HBM per device.

```python
import jax
import jax.numpy as jnp
from jax import lax

N = 6144
BLK = 32
M = 1024
ROWS = 4
COLS = 2

PANELS = N // BLK
PRECISE = lax.Precision.HIGHEST


def setup_inputs(seed: int = 0, part: int = 0) -> dict:
    base_key = jax.random.fold_in(jax.random.key(seed), part)
    key_v, key_tau, key_z = jax.random.split(base_key, 3)
    row_ids = jnp.arange(N)[:, None]

    def build_panel(panel_idx):
        col_ids = panel_idx * BLK + jnp.arange(BLK)
        noise = jax.random.normal(jax.random.fold_in(key_v, panel_idx), (N, BLK), jnp.float32)
        spread = jax.random.uniform(jax.random.fold_in(key_tau, panel_idx), (BLK,), jnp.float32, 0.25, 3.0)
        tail_len = jnp.maximum(N - 1 - col_ids, 1).astype(jnp.float32)
        scale = jnp.sqrt(spread / tail_len)
        panel = jnp.where(row_ids > col_ids, noise * scale, (row_ids == col_ids).astype(jnp.float32))
        gram_mat = jnp.dot(panel.T, panel, precision=PRECISE, preferred_element_type=jnp.float32)
        t_inverse = jnp.triu(gram_mat, 1) + 0.5 * jnp.diag(jnp.diag(gram_mat))
        t_mat = jnp.triu(jnp.linalg.inv(t_inverse))
        return panel, t_mat

    panels, t_factors = lax.map(build_panel, jnp.arange(PANELS))
    v_panels = panels.reshape(PANELS // COLS, COLS, PANELS // ROWS, ROWS, BLK, BLK)
    v_panels = v_panels.transpose(3, 2, 4, 1, 0, 5).reshape(N, N)
    z_in = jax.random.normal(key_z, (N, M), jnp.float32)
    return {"z_in": z_in, "v_panels": v_panels, "t_factors": t_factors}


def reference(z_in, v_panels, t_factors):
    panels = v_panels.reshape(N, COLS, PANELS // COLS, BLK).transpose(2, 1, 0, 3).reshape(PANELS, N, BLK)

    def apply_panel(z_cur, panel_pair):
        panel, t_mat = panel_pair
        s_part = jnp.dot(panel.T, z_cur, precision=PRECISE, preferred_element_type=jnp.float32)
        w_part = jnp.dot(t_mat, s_part, precision=PRECISE, preferred_element_type=jnp.float32)
        z_next = z_cur - jnp.dot(panel, w_part, precision=PRECISE, preferred_element_type=jnp.float32)
        return z_next, None

    z_out, _ = lax.scan(apply_panel, z_in, (panels, t_factors), reverse=True)
    return z_out
```

```python
import jax
import jax.numpy as jnp
from jax import lax
from jax.experimental import pallas as pl
from jax.experimental.pallas import tpu as pltpu
from jax.sharding import PartitionSpec as P

PRECISE = lax.Precision.HIGHEST
MESH = pl.DeviceIdType.MESH

W = 32
ROWS = 1536
TILE = 256
HALF = 128
NT = ROWS // TILE
NB = 24
VT = 4 * sum(range(1, NT + 1))
AHEAD = 12


def _dot(a, b, ca, cb):
    return lax.dot_general(a, b, (((ca,), (cb,)), ((), ())), precision=PRECISE, preferred_element_type=jnp.float32)


def _base(b):
    q, i = b // 4, b % 4
    return 4 * (NT * q - (q * (q - 1)) // 2) + i * (NT - q)


def _panel(idx):
    return jnp.where(idx < HALF, 2 * (idx // W), 2 * ((idx - HALF) // W) + 1)


def _kernel(zt_in, v_in, t0_in, out, vbuf, zt, t0, acc, srecv, wbuf, usend, urecv, ufull, tbuf,
            loc_sem, ys_sem, yr_sem, os_sem, or_sem, fs_sem, fr_sem, zs_sem, zr_sem,
            ss_sem, sr_sem, us_sem, ur_sem, hs_sem, hr_sem, misc_sem, outs_sem, outr_sem):
    ridx = lax.axis_index("row")
    y = lax.axis_index("col")
    x, c = ridx // 2, ridx % 2
    xn = {"row": (ridx + 2) % 4}
    sib = {"row": ridx + 1 - 2 * c}
    yn = {"col": 1 - y}

    barrier = pltpu.get_barrier_semaphore()
    for dev in (xn, sib, yn):
        pl.semaphore_signal(barrier, inc=1, device_id=dev, device_id_type=MESH)

    def remote(src, dst, send, recv, dev):
        return pltpu.make_async_remote_copy(src, dst, send, recv, device_id=dev, device_id_type=MESH)

    def slab(b, rho, par):
        start = (rho * VT + _base(b)) * TILE + 64 * (b % 4)
        return vbuf.at[pl.ds(pl.multiple_of(start, 64), ROWS - 64 * b), pl.ds(pl.multiple_of(par * HALF, HALF), HALF)]

    def v_local(b):
        return pltpu.make_async_copy(v_in.at[pl.ds(64 * b, ROWS - 64 * b), pl.ds(HALF * b, HALF)], slab(b, c, y), loc_sem.at[b])

    def v_y(b, par):
        return remote(slab(b, c, par), slab(b, c, par), ys_sem.at[b], yr_sem.at[b], yn)

    def v_own(b, rho):
        return remote(slab(b, rho, y), slab(b, rho, y), os_sem.at[b], or_sem.at[b], sib)

    def v_fwd(b, rho):
        return remote(slab(b, rho, 1 - y), slab(b, rho, 1 - y), fs_sem.at[b], fr_sem.at[b], sib)

    def v_issue(b):
        v_local(b).wait()
        v_y(b, y).start()
        v_own(b, c).start()

    def static_block(b, fn):
        for qq in range(NT):

            @pl.when(b // 4 == qq)
            def _(qq=qq):
                for ii in range(4):

                    @pl.when(b % 4 == ii)
                    def _(ii=ii):
                        fn(4 * qq + ii)

    def z_own(rho):
        return pltpu.make_async_copy(
            zt_in.at[:, pl.ds(pl.multiple_of((2 * x + rho) * ROWS, HALF), ROWS)],
            zt.at[x, :, pl.ds(rho * ROWS, ROWS)], misc_sem.at[rho])

    def z_chunk(t, j, g):
        off = (j // 2) * ROWS + t * TILE + (j % 2) * HALF
        return remote(
            zt_in.at[:, pl.ds(pl.multiple_of(2 * (1 - x) * ROWS + off, HALF), HALF)],
            zt.at[g, :, pl.ds(pl.multiple_of(off, HALF), HALF)],
            zs_sem.at[4 * t + j], zr_sem.at[4 * t + j], xn)

    t0_copy = pltpu.make_async_copy(t0_in, t0, misc_sem.at[2])

    for b in range(NB - 1, NB - 5, -1):
        v_local(b).start()
    for rho in range(2):
        z_own(rho).start()
    t0_copy.start()
    for b in range(NB - 5, -1, -1):
        v_local(b).start()
    for b in range(NB):
        if b % 4:
            for rho in range(2):
                vbuf[pl.ds((rho * VT + _base(b)) * TILE, 64 * (b % 4)), :] = jnp.zeros((64 * (b % 4), TILE), jnp.float32)

    pl.semaphore_wait(barrier, 3)
    for b in range(NB - 1, NB - 1 - AHEAD, -1):
        v_issue(b)
        if b == NB - 2:
            for j in range(4):
                z_chunk(NT - 1, j, x).start()
    for rho in range(2):
        z_own(rho).wait()
    t0_copy.wait()

    def rows(b, t, rho):
        return pl.ds(pl.multiple_of((rho * VT + _base(b) + t - b // 4) * TILE, TILE), TILE)

    def cols(t, rho):
        return pl.ds(pl.multiple_of(rho * ROWS + t * TILE, TILE), TILE)

    def s_copy(g, b):
        return remote(acc.at[g], srecv.at[g, b % 2], ss_sem.at[g], sr_sem.at[g, b % 2], xn)

    def weights(g, b):
        s_copy(g, b).wait_recv()
        s_sum = acc[g] + srecv[g, b % 2]
        wbuf[...] = _dot(s_sum, tbuf[b % 2], 1, 1)
        s_copy(g, b).wait_send()

    def update(g, b, t, rho):
        z_new = zt[g, :, cols(t, rho)] - _dot(wbuf[...], vbuf[rows(b, t, rho), :], 1, 1)
        zt[g, :, cols(t, rho)] = z_new
        return z_new

    def sweep(g, k):
        @pl.when(k < NB - 1)
        def _():
            weights(g, k + 1)

        acc[g] = jnp.zeros((HALF, TILE), jnp.float32)

        @pl.when(k % 4 == 3)
        def _():
            acc[g] += sum(_dot(zt[g, :, cols(k // 4, rho)], vbuf[rows(k, k // 4, rho), :], 1, 0) for rho in range(2))

        def tile(t, carry):
            acc[g] += sum(_dot(update(g, k + 1, t, rho), vbuf[rows(k, t, rho), :], 1, 0) for rho in range(2))
            return carry

        lax.fori_loop((k + 1) // 4, NT, tile, 0)
        s_copy(g, k).start()

    def u_copy(b):
        return remote(usend, urecv.at[b % 4], us_sem, ur_sem.at[b % 4], xn)

    def half_copy(b, half):
        part = ufull.at[b % 2, pl.ds(pl.multiple_of(half * HALF, HALF), HALF), :]
        return remote(part, part, hs_sem, hr_sem.at[b % 2], sib)

    def gram(b):
        def tile(t, total):
            for rho in range(2):
                v_own_cols = vbuf[rows(b, t, rho), pl.ds(pl.multiple_of(c * HALF, HALF), HALF)]
                usend[...] += _dot(v_own_cols, vbuf[rows(b, t, rho), :], 0, 0)
            return total

        usend[...] = jnp.zeros((HALF, TILE), jnp.float32)
        lax.fori_loop(b // 4, NT, tile, 0)
        u_copy(b).start()

    def u_half(b):
        u_copy(b).wait()
        total = usend[...] + urecv[b % 4]
        pa = 2 * (lax.broadcasted_iota(jnp.int32, (HALF, TILE), 0) // W) + c
        pb = _panel(lax.broadcasted_iota(jnp.int32, (HALF, TILE), 1))

        @pl.when(b < NB - 1)
        def _():
            half_copy(b + 1, c).wait_send()

        ufull[b % 2, pl.ds(pl.multiple_of(c * HALF, HALF), HALF), :] = jnp.where(pa < pb, total, 0.0)
        half_copy(b, c).start()

    def merge(b):
        half_copy(b, 1 - c).wait_recv()
        u_all = ufull[b % 2]
        even, odd = t0[b, 0], t0[b, 1]
        ra = lax.broadcasted_iota(jnp.int32, (HALF, HALF), 0) // W
        rb = lax.broadcasted_iota(jnp.int32, (HALF, HALF), 1) // W
        pairs = jnp.where(ra == rb, u_all[:HALF, HALF:], 0.0)
        slot = b % 2
        tbuf[slot, :HALF, :HALF] = even
        tbuf[slot, :HALF, HALF:] = -_dot(_dot(even, pairs, 1, 0), odd, 1, 0)
        tbuf[slot, HALF:, :HALF] = jnp.zeros((HALF, HALF), jnp.float32)
        tbuf[slot, HALF:, HALF:] = odd
        pa = _panel(lax.broadcasted_iota(jnp.int32, (TILE, TILE), 0))
        pb = _panel(lax.broadcasted_iota(jnp.int32, (TILE, TILE), 1))
        for size in (2, 4):
            level = (pa // (2 * size) == pb // (2 * size)) & (pa // size < pb // size)
            t_now = tbuf[slot]
            tbuf[slot] = t_now - _dot(t_now, _dot(jnp.where(level, u_all, 0.0), t_now, 1, 0), 1, 0)

    def step(s, carry):
        k = NB + 2 - s

        @pl.when(k < NB)
        def _():
            @pl.when(k % 4 == 3)
            def _():
                for j in range(4):
                    z_chunk(k // 4, j, 1 - x).wait_recv()

            sweep(0, k)
            sweep(1, k)

            @pl.when(k >= 4)
            def _():
                z_chunk(k // 4 - 1, 3 - k % 4, x).start()

            @pl.when(k >= AHEAD)
            def _():
                static_block(k - AHEAD, v_issue)

        @pl.when((k >= 1) & (k <= NB))
        def _():
            u_half(k - 1)

        @pl.when(k >= 3)
        def _():
            def forward(b):
                v_y(b, 1 - y).wait_recv()
                v_fwd(b, c).start()

            static_block(k - 3, forward)

        @pl.when((k >= 2) & (k < NB + 2))
        def _():
            def arrived(b):
                v_own(b, 1 - c).wait_recv()
                v_fwd(b, 1 - c).wait_recv()

            static_block(k - 2, arrived)
            gram(k - 2)

        @pl.when((k >= 1) & (k <= NB))
        def _():
            merge(k - 1)

        return carry

    lax.fori_loop(0, NB + 3, step, 0)

    def out_rows(g):
        return pl.ds(pl.multiple_of((2 * g + c) * HALF, HALF), HALF)

    def out_local(g):
        return pltpu.make_async_copy(zt.at[g, :, pl.ds(pl.multiple_of(c * ROWS, HALF), ROWS)], out.at[out_rows(g), :], misc_sem.at[g])

    def out_sib(g):
        return remote(zt.at[g, :, pl.ds(pl.multiple_of((1 - c) * ROWS, HALF), ROWS)], out.at[out_rows(g), :],
                      outs_sem.at[g], outr_sem.at[g], sib)

    def out_from_sib(g):
        part = out.at[pl.ds(pl.multiple_of((2 * g + 1 - c) * HALF, HALF), HALF), :]
        return remote(part, part, outs_sem.at[g], outr_sem.at[g], sib)

    for g in range(2):
        weights(g, 0)

        def last(t, carry, g=g):
            for rho in range(2):
                update(g, 0, t, rho)
            return carry

        lax.fori_loop(0, NT, last, 0)
        out_local(g).start()
        out_sib(g).start()

    half_copy(0, c).wait_send()
    for b in range(NB):
        v_y(b, y).wait_send()
        v_own(b, c).wait_send()
        v_fwd(b, c).wait_send()
        z_chunk(b // 4, b % 4, x).wait_send()
    for g in range(2):
        out_local(g).wait()
        out_sib(g).wait_send()
        out_from_sib(g).wait_recv()


def solution(mesh):
    def local_run(z_cols, v_local, t_local):
        f32 = jnp.float32
        t6 = t_local.reshape(NB, 4, 2, W, W).transpose(0, 2, 1, 3, 4)[:, :, :, :, None, :]
        same = jnp.eye(4, dtype=bool)[None, None, :, None, :, None]
        t0 = jnp.where(same, t6, 0.0).reshape(NB, 2, HALF, HALF)
        any_spec = pl.BlockSpec(memory_space=pl.ANY)
        dma = pltpu.SemaphoreType.DMA
        z_t = pl.pallas_call(
            _kernel,
            out_shape=jax.ShapeDtypeStruct((4 * HALF, ROWS), f32),
            in_specs=[any_spec] * 3,
            out_specs=any_spec,
            scratch_shapes=[
                pltpu.VMEM((2 * VT * TILE, TILE), f32),
                pltpu.VMEM((2, HALF, 2 * ROWS), f32),
                pltpu.VMEM((NB, 2, HALF, HALF), f32),
                pltpu.VMEM((2, HALF, TILE), f32),
                pltpu.VMEM((2, 2, HALF, TILE), f32),
                pltpu.VMEM((HALF, TILE), f32),
                pltpu.VMEM((HALF, TILE), f32),
                pltpu.VMEM((4, HALF, TILE), f32),
                pltpu.VMEM((2, TILE, TILE), f32),
                pltpu.VMEM((2, TILE, TILE), f32),
                *[dma((NB,))] * 9,
                dma((2,)), dma((2, 2)), dma, dma((4,)), dma, dma((2,)), dma((3,)), dma((2,)), dma((2,)),
            ],
            compiler_params=pltpu.CompilerParams(collective_id=0, has_side_effects=True, vmem_limit_bytes=63 * 2**20),
            name="backtransform",
        )(z_cols.T, v_local, t0)
        return z_t.T

    return jax.shard_map(
        local_run,
        mesh=mesh,
        in_specs=(P("kpt", ("col", "row")), P(("kpt", "row"), "col"), P("kpt", None, None)),
        out_specs=P(("kpt", "row"), "col"),
        check_vma=False,
    )
```

```python
import jax
import jax.numpy as jnp
from jax import lax
from jax.experimental import pallas as pl
from jax.experimental.pallas import tpu as pltpu
from jax.sharding import PartitionSpec as P

PRECISE = lax.Precision.HIGHEST
MESH = pl.DeviceIdType.MESH

W = 32
ROWS = 1536
TILE = 256
HALF = 128
NT = ROWS // TILE
NB = 24
VT = 4 * sum(range(1, NT + 1))
AHEAD = 12


def _dot(a, b, ca, cb):
    return lax.dot_general(a, b, (((ca,), (cb,)), ((), ())), precision=PRECISE, preferred_element_type=jnp.float32)


def _base(b):
    q, i = b // 4, b % 4
    return 4 * (NT * q - (q * (q - 1)) // 2) + i * (NT - q)


def _panel(idx):
    return jnp.where(idx < HALF, 2 * (idx // W), 2 * ((idx - HALF) // W) + 1)


def _pairs(lo, n, body):
    def two(h, carry):
        body(lo + 2 * h)
        body(lo + 2 * h + 1)
        return carry

    lax.fori_loop(0, n // 2, two, 0)

    @pl.when(n % 2 == 1)
    def _():
        body(lo + n - 1)


def _kernel(zt_in, v_in, tt_in, out, vbuf, vtr, zt, tt, acc, srecv, wbuf, usend, urecv, uhalf, ufull, tbuf,
            loc_sem, ys_sem, yr_sem, os_sem, or_sem, fs_sem, fr_sem, zs_sem, zr_sem,
            ss_sem, sr_sem, us_sem, ur_sem, hs_sem, hr_sem, ts_sem, tr_sem, tt_sem, zo_sem, out_sem, outs_sem, outr_sem):
    ridx = lax.axis_index("row")
    y = lax.axis_index("col")
    x, c = ridx // 2, ridx % 2
    xn = {"row": (ridx + 2) % 4}
    sib = {"row": ridx + 1 - 2 * c}
    yn = {"col": 1 - y}

    barrier = pltpu.get_barrier_semaphore()
    for dev in (xn, sib, yn):
        pl.semaphore_signal(barrier, inc=1, device_id=dev, device_id_type=MESH)

    def remote(src, dst, send, recv, dev):
        return pltpu.make_async_remote_copy(src, dst, send, recv, device_id=dev, device_id_type=MESH)

    def slab(b, rho, par):
        start = (rho * VT + _base(b)) * TILE + 64 * (b % 4)
        return vbuf.at[pl.ds(pl.multiple_of(start, 64), ROWS - 64 * b), pl.ds(pl.multiple_of(par * HALF, HALF), HALF)]

    def v_local(b):
        return pltpu.make_async_copy(v_in.at[pl.ds(64 * b, ROWS - 64 * b), pl.ds(HALF * b, HALF)], slab(b, c, y), loc_sem.at[b])

    def v_y(b, par):
        return remote(slab(b, c, par), slab(b, c, par), ys_sem.at[b], yr_sem.at[b], yn)

    def v_own(b, rho):
        return remote(slab(b, rho, y), slab(b, rho, y), os_sem.at[b], or_sem.at[b], sib)

    def v_fwd(b, rho):
        return remote(slab(b, rho, 1 - y), slab(b, rho, 1 - y), fs_sem.at[b], fr_sem.at[b], sib)

    def v_issue(b):
        v_local(b).wait()
        v_y(b, y).start()
        v_own(b, c).start()

    def static_block(b, fn):
        for qq in range(NT):

            @pl.when(b // 4 == qq)
            def _(qq=qq):
                for ii in range(4):

                    @pl.when(b % 4 == ii)
                    def _(ii=ii):
                        fn(4 * qq + ii)

    def z_own(t, rho):
        return pltpu.make_async_copy(
            zt_in.at[:, pl.ds(pl.multiple_of((2 * x + rho) * ROWS + t * TILE, TILE), TILE)],
            zt.at[x, :, pl.ds((2 * t + rho) * TILE, TILE)], zo_sem.at[2 * t + rho])

    def z_chunk(t, j, g):
        src = (2 * (1 - x) + j // 2) * ROWS + t * TILE + (j % 2) * HALF
        return remote(
            zt_in.at[:, pl.ds(pl.multiple_of(src, HALF), HALF)],
            zt.at[g, :, pl.ds(pl.multiple_of(2 * t * TILE + j * HALF, HALF), HALF)],
            zs_sem.at[4 * t + j], zr_sem.at[4 * t + j], xn)

    tt_copy = pltpu.make_async_copy(tt_in, tt, tt_sem)

    for b in range(NB - 1, NB - 5, -1):
        v_local(b).start()
    tt_copy.start()
    for t in range(NT - 1, -1, -1):
        for rho in range(2):
            z_own(t, rho).start()
    for b in range(NB - 5, -1, -1):
        v_local(b).start()
    for b in range(NB):
        if b % 4:
            for rho in range(2):
                vbuf[pl.ds((rho * VT + _base(b)) * TILE, 64 * (b % 4)), :] = jnp.zeros((64 * (b % 4), TILE), jnp.float32)

    pl.semaphore_wait(barrier, 3)
    for b in range(NB - 1, NB - 1 - AHEAD, -1):
        v_issue(b)
        if b == NB - 2:
            for j in range(4):
                z_chunk(NT - 1, j, x).start()
    for t in range(NT):
        for rho in range(2):
            z_own(t, rho).wait()
    tt_copy.wait()

    def rows(b, t, rho):
        return pl.ds(pl.multiple_of((rho * VT + _base(b) + t - b // 4) * TILE, TILE), TILE)

    def v_tile(b, t):
        return jnp.concatenate([vbuf[rows(b, t, rho), :] for rho in range(2)], axis=0)

    def cols(t):
        return pl.ds(pl.multiple_of(t * 2 * TILE, 2 * TILE), 2 * TILE)

    def s_copy(g, b):
        return remote(acc.at[g], srecv.at[g, b % 2], ss_sem.at[g], sr_sem.at[g, b % 2], xn)

    def weights(g, b):
        if g == 0:

            @pl.when(b % 2 != c)
            def _():
                t_copy(b).wait_recv()

        s_copy(g, b).wait_recv()
        s_sum = acc[g] + srecv[g, b % 2]
        wbuf[...] = _dot(s_sum, tbuf[b % 2], 1, 0)
        s_copy(g, b).wait_send()

    def update(g, b, t):
        if g == 0:
            v_tr = v_tile(b, t).T
            vtr[:, cols(t)] = v_tr
        else:
            v_tr = vtr[:, cols(t)]
        zt[g, :, cols(t)] = zt[g, :, cols(t)] - _dot(wbuf[...], v_tr, 1, 0)

    def partial_s(g, b, t):
        acc[g] += _dot(zt[g, :, cols(t)], v_tile(b, t), 1, 0)

    def sweep(g, k):
        @pl.when(k < NB - 1)
        def _():
            weights(g, k + 1)

        acc[g] = jnp.zeros((HALF, TILE), jnp.float32)
        first = (k + 1) // 4
        late = jnp.where(k % 4 == 3, 0, 1)

        @pl.when(late == 1)
        def _():
            update(g, k + 1, first)

        def both(t):
            partial_s(g, k, t - 1)
            update(g, k + 1, t)

        _pairs(first + late, NT - first - late, both)
        partial_s(g, k, NT - 1)
        s_copy(g, k).start()

    def u_copy(b):
        return remote(usend, urecv.at[b % 4], us_sem, ur_sem.at[b % 4], xn)

    half_copy = remote(uhalf, ufull.at[pl.ds(pl.multiple_of(c * HALF, HALF), HALF), :], hs_sem, hr_sem, sib)

    def t_copy(b):
        return remote(tbuf.at[b % 2], tbuf.at[b % 2], ts_sem, tr_sem.at[b % 2], sib)

    def gram(b):
        def tile(t):
            own = jnp.concatenate(
                [vbuf[rows(b, t, rho), pl.ds(pl.multiple_of(c * HALF, HALF), HALF)] for rho in range(2)], axis=0)
            usend[...] += _dot(own, v_tile(b, t), 0, 0)

        usend[...] = jnp.zeros((HALF, TILE), jnp.float32)
        _pairs(b // 4, NT - b // 4, tile)
        u_copy(b).start()

    def u_half(b):
        u_copy(b).wait()
        total = usend[...] + urecv[b % 4]
        pa = 2 * (lax.broadcasted_iota(jnp.int32, (HALF, TILE), 0) // W) + c
        pb = _panel(lax.broadcasted_iota(jnp.int32, (HALF, TILE), 1))
        half = jnp.where(pa < pb, total, 0.0)

        @pl.when(b % 2 == c)
        def _():
            ufull[pl.ds(pl.multiple_of(c * HALF, HALF), HALF), :] = half

        @pl.when(b % 2 != c)
        def _():
            @pl.when(b < NB - 2)
            def _():
                half_copy.wait_send()

            uhalf[...] = half
            half_copy.start()

    def merge(b):
        half_copy.wait_recv()
        u_all = ufull[...]
        slot = b % 2

        @pl.when(b < NB - 2)
        def _():
            t_copy(b).wait_send()

        same = (lax.broadcasted_iota(jnp.int32, (HALF, HALF), 0) // W) == (lax.broadcasted_iota(jnp.int32, (HALF, HALF), 1) // W)

        def diagonal(par):
            stack = jnp.concatenate([tt[8 * b + 2 * i + par] for i in range(4)], axis=0)
            return jnp.where(same, jnp.concatenate([stack] * 4, axis=1), 0.0)

        even, odd = diagonal(0), diagonal(1)
        pairs = jnp.where(same, u_all[:HALF, HALF:], 0.0)
        tbuf[slot, :HALF, :HALF] = even
        tbuf[slot, :HALF, HALF:] = jnp.zeros((HALF, HALF), jnp.float32)
        tbuf[slot, HALF:, :HALF] = -_dot(_dot(odd, pairs, 1, 1), even, 1, 0)
        tbuf[slot, HALF:, HALF:] = odd
        pa = _panel(lax.broadcasted_iota(jnp.int32, (TILE, TILE), 0))
        pb = _panel(lax.broadcasted_iota(jnp.int32, (TILE, TILE), 1))
        for size in (2, 4):
            level = (pa // (2 * size) == pb // (2 * size)) & (pa // size < pb // size)
            t_now = tbuf[slot]
            tbuf[slot] = t_now - _dot(_dot(t_now, jnp.where(level, u_all, 0.0), 1, 1), t_now, 1, 0)
        t_copy(b).start()

    def step(s, carry):
        k = NB + 2 - s

        @pl.when(k < NB)
        def _():
            @pl.when(k % 4 == 3)
            def _():
                for j in range(4):
                    z_chunk(k // 4, j, 1 - x).wait_recv()

            sweep(0, k)
            sweep(1, k)

            @pl.when(k >= AHEAD)
            def _():
                static_block(k - AHEAD, v_issue)

        @pl.when((k >= 6) & (k < NB + 2))
        def _():
            z_chunk((k - 6) // 4, 3 - (k - 6) % 4, x).start()

        @pl.when((k >= 1) & (k <= NB))
        def _():
            u_half(k - 1)

        @pl.when(k >= 3)
        def _():
            def forward(b):
                v_y(b, 1 - y).wait_recv()
                v_fwd(b, c).start()

            static_block(k - 3, forward)

        @pl.when((k >= 2) & (k < NB + 2))
        def _():
            def arrived(b):
                v_own(b, 1 - c).wait_recv()
                v_fwd(b, 1 - c).wait_recv()

            static_block(k - 2, arrived)
            gram(k - 2)

        @pl.when((k >= 1) & (k <= NB) & ((k - 1) % 2 == c))
        def _():
            merge(k - 1)

        return carry

    lax.fori_loop(0, NB + 3, step, 0)

    def out_rows(g):
        return pl.ds(pl.multiple_of((2 * g + c) * HALF, HALF), HALF)

    def out_cols(t):
        return pl.ds(t * TILE, TILE)

    def out_local(g, t):
        return pltpu.make_async_copy(
            zt.at[g, :, pl.ds(pl.multiple_of((2 * t + c) * TILE, TILE), TILE)], out.at[out_rows(g), out_cols(t)],
            out_sem.at[g * NT + t])

    def out_sib(g, t):
        return remote(
            zt.at[g, :, pl.ds(pl.multiple_of((2 * t + 1 - c) * TILE, TILE), TILE)], out.at[out_rows(g), out_cols(t)],
            outs_sem.at[g * NT + t], outr_sem.at[g * NT + t], sib)

    def out_from_sib(g, t):
        part = out.at[pl.ds(pl.multiple_of((2 * g + 1 - c) * HALF, HALF), HALF), out_cols(t)]
        return remote(part, part, outs_sem.at[g * NT + t], outr_sem.at[g * NT + t], sib)

    for g in range(2):
        weights(g, 0)
        _pairs(0, NT, lambda t, g=g: update(g, 0, t))
        for t in range(NT):
            out_local(g, t).start()
            out_sib(g, t).start()

    half_copy.wait_send()
    t_copy(0).wait_send()
    for b in range(NB):
        v_y(b, y).wait_send()
        v_own(b, c).wait_send()
        v_fwd(b, c).wait_send()
        z_chunk(b // 4, b % 4, x).wait_send()
    for g in range(2):
        for t in range(NT):
            out_local(g, t).wait()
            out_sib(g, t).wait_send()
            out_from_sib(g, t).wait_recv()


def solution(mesh):
    def local_run(z_cols, v_local, t_local):
        f32 = jnp.float32
        any_spec = pl.BlockSpec(memory_space=pl.ANY)
        dma = pltpu.SemaphoreType.DMA
        z_t = pl.pallas_call(
            _kernel,
            out_shape=jax.ShapeDtypeStruct((4 * HALF, ROWS), f32),
            in_specs=[any_spec] * 3,
            out_specs=any_spec,
            scratch_shapes=[
                pltpu.VMEM((2 * VT * TILE, TILE), f32),
                pltpu.VMEM((TILE, 2 * ROWS), f32),
                pltpu.VMEM((2, HALF, 2 * ROWS), f32),
                pltpu.VMEM((NB * 8, W, W), f32),
                pltpu.VMEM((2, HALF, TILE), f32),
                pltpu.VMEM((2, 2, HALF, TILE), f32),
                pltpu.VMEM((HALF, TILE), f32),
                pltpu.VMEM((HALF, TILE), f32),
                pltpu.VMEM((4, HALF, TILE), f32),
                pltpu.VMEM((HALF, TILE), f32),
                pltpu.VMEM((TILE, TILE), f32),
                pltpu.VMEM((2, TILE, TILE), f32),
                *[dma((NB,))] * 9,
                dma((2,)), dma((2, 2)), dma, dma((4,)), dma, dma, dma, dma((2,)), dma, *[dma((2 * NT,))] * 4,
            ],
            compiler_params=pltpu.CompilerParams(collective_id=0, has_side_effects=True, vmem_limit_bytes=63 * 2**20),
            name="backtransform",
        )(z_cols.T, v_local, t_local.transpose(0, 2, 1))
        return z_t.T

    return jax.shard_map(
        local_run,
        mesh=mesh,
        in_specs=(P("kpt", ("col", "row")), P(("kpt", "row"), "col"), P("kpt", None, None)),
        out_specs=P(("kpt", "row"), "col"),
        check_vma=False,
    )
```

```python
import jax
import jax.numpy as jnp
from jax import lax
from jax.experimental import pallas as pl
from jax.experimental.pallas import tpu as pltpu
from jax.sharding import PartitionSpec as P

PRECISE = lax.Precision.HIGHEST
MESH = pl.DeviceIdType.MESH

W = 32
ROWS = 1536
TILE = 256
HALF = 128
NT = ROWS // TILE
NB = 24
VT = 4 * sum(range(1, NT + 1))
AHEAD = 12


def _dot(a, b, ca, cb):
    return lax.dot_general(a, b, (((ca,), (cb,)), ((), ())), precision=PRECISE, preferred_element_type=jnp.float32)


def _base(b):
    q, i = b // 4, b % 4
    return 4 * (NT * q - (q * (q - 1)) // 2) + i * (NT - q)


def _panel(idx):
    return jnp.where(idx < HALF, 2 * (idx // W), 2 * ((idx - HALF) // W) + 1)


def _pairs(lo, n, body):
    def two(h, carry):
        body(lo + 2 * h)
        body(lo + 2 * h + 1)
        return carry

    lax.fori_loop(0, n // 2, two, 0)

    @pl.when(n % 2 == 1)
    def _():
        body(lo + n - 1)


def _kernel(zt_in, v_in, tt_in, out, vbuf, vtr, zt, tt, acc, srecv, wbuf, gacc, usend, urecv, uhalf, upack, tbuf,
            loc_sem, ys_sem, yr_sem, os_sem, or_sem, fs_sem, fr_sem, zs_sem, zr_sem,
            ss_sem, sr_sem, us_sem, ur_sem, hs_sem, hr_sem, ts_sem, tr_sem, tt_sem, zo_sem, out_sem, outs_sem, outr_sem):
    ridx = lax.axis_index("row")
    y = lax.axis_index("col")
    x, c = ridx // 2, ridx % 2
    xn = {"row": (ridx + 2) % 4}
    sib = {"row": ridx + 1 - 2 * c}
    yn = {"col": 1 - y}

    barrier = pltpu.get_barrier_semaphore()
    for dev in (xn, sib, yn):
        pl.semaphore_signal(barrier, inc=1, device_id=dev, device_id_type=MESH)

    def remote(src, dst, send, recv, dev):
        return pltpu.make_async_remote_copy(src, dst, send, recv, device_id=dev, device_id_type=MESH)

    def slab(b, rho, par):
        start = (rho * VT + _base(b)) * TILE + 64 * (b % 4)
        return vbuf.at[pl.ds(pl.multiple_of(start, 64), ROWS - 64 * b), pl.ds(pl.multiple_of(par * HALF, HALF), HALF)]

    def v_local(b):
        return pltpu.make_async_copy(v_in.at[pl.ds(64 * b, ROWS - 64 * b), pl.ds(HALF * b, HALF)], slab(b, c, y), loc_sem.at[b])

    def v_y(b, par):
        return remote(slab(b, c, par), slab(b, c, par), ys_sem.at[b], yr_sem.at[b], yn)

    def v_own(b, rho):
        return remote(slab(b, rho, y), slab(b, rho, y), os_sem.at[b], or_sem.at[b], sib)

    def v_fwd(b, rho):
        return remote(slab(b, rho, 1 - y), slab(b, rho, 1 - y), fs_sem.at[b], fr_sem.at[b], sib)

    def v_issue(b):
        v_local(b).wait()
        v_y(b, y).start()
        v_own(b, c).start()

    def static_block(b, fn):
        for qq in range(NT):

            @pl.when(b // 4 == qq)
            def _(qq=qq):
                for ii in range(4):

                    @pl.when(b % 4 == ii)
                    def _(ii=ii):
                        fn(4 * qq + ii)

    def z_own(t, rho):
        return pltpu.make_async_copy(
            zt_in.at[:, pl.ds(pl.multiple_of((2 * x + rho) * ROWS + t * TILE, TILE), TILE)],
            zt.at[x, :, pl.ds((2 * t + rho) * TILE, TILE)], zo_sem.at[2 * t + rho])

    def z_chunk(t, j, g):
        src = (2 * (1 - x) + j // 2) * ROWS + t * TILE + (j % 2) * HALF
        return remote(
            zt_in.at[:, pl.ds(pl.multiple_of(src, HALF), HALF)],
            zt.at[g, :, pl.ds(pl.multiple_of(2 * t * TILE + j * HALF, HALF), HALF)],
            zs_sem.at[4 * t + j], zr_sem.at[4 * t + j], xn)

    tt_copy = pltpu.make_async_copy(tt_in, tt, tt_sem)

    for b in range(NB - 1, NB - 5, -1):
        v_local(b).start()
    tt_copy.start()
    for t in range(NT - 1, -1, -1):
        for rho in range(2):
            z_own(t, rho).start()
    for b in range(NB - 5, -1, -1):
        v_local(b).start()
    for b in range(NB):
        if b % 4:
            for rho in range(2):
                vbuf[pl.ds((rho * VT + _base(b)) * TILE, 64 * (b % 4)), :] = jnp.zeros((64 * (b % 4), TILE), jnp.float32)

    pl.semaphore_wait(barrier, 3)
    for b in range(NB - 1, NB - 1 - AHEAD, -1):
        v_issue(b)
        if b == NB - 2:
            for j in range(4):
                z_chunk(NT - 1, j, x).start()
    for t in range(NT):
        for rho in range(2):
            z_own(t, rho).wait()
    tt_copy.wait()

    def rows(b, t, rho):
        return pl.ds(pl.multiple_of((rho * VT + _base(b) + t - b // 4) * TILE, TILE), TILE)

    def v_tile(b, t):
        return jnp.concatenate([vbuf[rows(b, t, rho), :] for rho in range(2)], axis=0)

    def cols(t):
        return pl.ds(pl.multiple_of(t * 2 * TILE, 2 * TILE), 2 * TILE)

    def s_copy(g, b):
        return remote(acc.at[g], srecv.at[g, b % 2], ss_sem.at[g], sr_sem.at[g, b % 2], xn)

    def weights(g, b):
        if g == 0:

            @pl.when(b % 2 != c)
            def _():
                t_copy(b).wait_recv()

        s_copy(g, b).wait_recv()
        s_sum = acc[g] + srecv[g, b % 2]
        wbuf[...] = _dot(s_sum, tbuf[b % 2], 1, 0)
        s_copy(g, b).wait_send()

    def update(g, b, t):
        if g == 0:
            v_tr = v_tile(b, t).T
            vtr[:, cols(t)] = v_tr
        else:
            v_tr = vtr[:, cols(t)]
        zt[g, :, cols(t)] = zt[g, :, cols(t)] - _dot(wbuf[...], v_tr, 1, 0)

    def partial_s(g, b, t):
        acc[g] += _dot(zt[g, :, cols(t)], v_tile(b, t), 1, 0)

    def sweep(g, k):
        @pl.when(k < NB - 1)
        def _():
            weights(g, k + 1)

        acc[g] = jnp.zeros((HALF, TILE), jnp.float32)
        first = (k + 1) // 4
        late = jnp.where(k % 4 == 3, 0, 1)

        @pl.when(late == 1)
        def _():
            update(g, k + 1, first)

        def both(t):
            partial_s(g, k, t - 1)
            update(g, k + 1, t)

        _pairs(first + late, NT - first - late, both)
        partial_s(g, k, NT - 1)
        s_copy(g, k).start()

    ra = lax.broadcasted_iota(jnp.int32, (HALF, HALF), 0) // W
    rb = lax.broadcasted_iota(jnp.int32, (HALF, HALF), 1) // W

    def u_copy(b):
        return remote(usend.at[b % 2], urecv.at[b % 4], us_sem.at[b % 2], ur_sem.at[b % 4], xn)

    half_copy = remote(uhalf, upack.at[c], hs_sem, hr_sem, sib)

    def t_copy(b):
        return remote(tbuf.at[b % 2], tbuf.at[b % 2], ts_sem, tr_sem.at[b % 2], sib)

    def gram(b):
        def tile(t):
            own = jnp.concatenate(
                [vbuf[rows(b, t, rho), pl.ds(pl.multiple_of(c * HALF, HALF), HALF)] for rho in range(2)], axis=0)
            gacc[...] += _dot(own, v_tile(b, t), 0, 0)

        gacc[...] = jnp.zeros((HALF, TILE), jnp.float32)
        _pairs(b // 4, NT - b // 4, tile)

        def cols_of(par):
            return gacc[:, pl.ds(pl.multiple_of(par * HALF, HALF), HALF)]

        usend[b % 2] = jnp.where(ra <= rb, cols_of(1 - c), cols_of(c))
        u_copy(b).start()

    def u_half(b):
        u_copy(b).wait()
        total = usend[b % 2] + urecv[b % 4]

        @pl.when(b % 2 == c)
        def _():
            upack[c] = total

        @pl.when(b % 2 != c)
        def _():
            @pl.when(b < NB - 2)
            def _():
                half_copy.wait_send()

            uhalf[...] = total
            half_copy.start()

    def merge(b):
        half_copy.wait_recv()
        slot = b % 2

        @pl.when(b < NB - 2)
        def _():
            t_copy(b).wait_send()

        same = ra == rb

        def diagonal(par):
            stack = jnp.concatenate([tt[8 * b + 2 * i + par] for i in range(4)], axis=0)
            return jnp.where(same, jnp.concatenate([stack] * 4, axis=1), 0.0)

        even_part, odd_part = upack[0], upack[1]
        eo = jnp.where(ra <= rb, even_part, 0.0).T
        u_tr = jnp.concatenate([
            jnp.concatenate([jnp.where(ra > rb, even_part, 0.0), jnp.where(ra < rb, odd_part, 0.0).T], axis=1),
            jnp.concatenate([eo, jnp.where(ra > rb, odd_part, 0.0)], axis=1)], axis=0)
        even, odd = diagonal(0), diagonal(1)
        pairs = jnp.where(same, eo, 0.0)
        tbuf[slot, :HALF, :HALF] = even
        tbuf[slot, :HALF, HALF:] = jnp.zeros((HALF, HALF), jnp.float32)
        tbuf[slot, HALF:, :HALF] = -_dot(_dot(odd, pairs, 1, 0), even, 1, 0)
        tbuf[slot, HALF:, HALF:] = odd
        pa = _panel(lax.broadcasted_iota(jnp.int32, (TILE, TILE), 0))
        pb = _panel(lax.broadcasted_iota(jnp.int32, (TILE, TILE), 1))
        for size in (2, 4):
            level = (pa // (2 * size) == pb // (2 * size)) & (pa // size > pb // size)
            t_now = tbuf[slot]
            tbuf[slot] = t_now - _dot(_dot(t_now, jnp.where(level, u_tr, 0.0), 1, 0), t_now, 1, 0)
        t_copy(b).start()

    def step(s, carry):
        k = NB + 2 - s

        @pl.when(k < NB)
        def _():
            @pl.when(k % 4 == 3)
            def _():
                for j in range(4):
                    z_chunk(k // 4, j, 1 - x).wait_recv()

            sweep(0, k)
            sweep(1, k)

            @pl.when(k >= AHEAD)
            def _():
                static_block(k - AHEAD, v_issue)

        @pl.when((k >= 1) & (k <= NB) & ((k - 1) % 2 != c))
        def _():
            u_half(k - 1)

        @pl.when(k >= 3)
        def _():
            def forward(b):
                v_y(b, 1 - y).wait_recv()
                v_fwd(b, c).start()

            static_block(k - 3, forward)

        @pl.when((k >= 2) & (k < NB + 2))
        def _():
            def arrived(b):
                v_own(b, 1 - c).wait_recv()
                v_fwd(b, 1 - c).wait_recv()

            static_block(k - 2, arrived)
            gram(k - 2)

        @pl.when((k >= 6) & (k < NB + 2))
        def _():
            z_chunk((k - 6) // 4, 3 - (k - 6) % 4, x).start()

        @pl.when((k >= 1) & (k <= NB) & ((k - 1) % 2 == c))
        def _():
            u_half(k - 1)
            merge(k - 1)

        return carry

    lax.fori_loop(0, NB + 3, step, 0)

    def out_rows(g):
        return pl.ds(pl.multiple_of((2 * g + c) * HALF, HALF), HALF)

    def out_cols(t):
        return pl.ds(t * TILE, TILE)

    def out_local(g, t):
        return pltpu.make_async_copy(
            zt.at[g, :, pl.ds(pl.multiple_of((2 * t + c) * TILE, TILE), TILE)], out.at[out_rows(g), out_cols(t)],
            out_sem.at[g * NT + t])

    def out_sib(g, t):
        return remote(
            zt.at[g, :, pl.ds(pl.multiple_of((2 * t + 1 - c) * TILE, TILE), TILE)], out.at[out_rows(g), out_cols(t)],
            outs_sem.at[g * NT + t], outr_sem.at[g * NT + t], sib)

    def out_from_sib(g, t):
        part = out.at[pl.ds(pl.multiple_of((2 * g + 1 - c) * HALF, HALF), HALF), out_cols(t)]
        return remote(part, part, outs_sem.at[g * NT + t], outr_sem.at[g * NT + t], sib)

    for g in range(2):
        weights(g, 0)
        _pairs(0, NT, lambda t, g=g: update(g, 0, t))
        for t in range(NT):
            out_local(g, t).start()
            out_sib(g, t).start()

    half_copy.wait_send()
    t_copy(0).wait_send()
    for b in range(NB):
        v_y(b, y).wait_send()
        v_own(b, c).wait_send()
        v_fwd(b, c).wait_send()
        z_chunk(b // 4, b % 4, x).wait_send()
    for g in range(2):
        for t in range(NT):
            out_local(g, t).wait()
            out_sib(g, t).wait_send()
            out_from_sib(g, t).wait_recv()


def solution(mesh):
    def local_run(z_cols, v_local, t_local):
        f32 = jnp.float32
        any_spec = pl.BlockSpec(memory_space=pl.ANY)
        dma = pltpu.SemaphoreType.DMA
        z_t = pl.pallas_call(
            _kernel,
            out_shape=jax.ShapeDtypeStruct((4 * HALF, ROWS), f32),
            in_specs=[any_spec] * 3,
            out_specs=any_spec,
            scratch_shapes=[
                pltpu.VMEM((2 * VT * TILE, TILE), f32),
                pltpu.VMEM((TILE, 2 * ROWS), f32),
                pltpu.VMEM((2, HALF, 2 * ROWS), f32),
                pltpu.VMEM((NB * 8, W, W), f32),
                pltpu.VMEM((2, HALF, TILE), f32),
                pltpu.VMEM((2, 2, HALF, TILE), f32),
                pltpu.VMEM((HALF, TILE), f32),
                pltpu.VMEM((HALF, TILE), f32),
                pltpu.VMEM((2, HALF, HALF), f32),
                pltpu.VMEM((4, HALF, HALF), f32),
                pltpu.VMEM((HALF, HALF), f32),
                pltpu.VMEM((2, HALF, HALF), f32),
                pltpu.VMEM((2, TILE, TILE), f32),
                *[dma((NB,))] * 9,
                dma((2,)), dma((2, 2)), dma((2,)), dma((4,)), dma, dma, dma, dma((2,)), dma, *[dma((2 * NT,))] * 4,
            ],
            compiler_params=pltpu.CompilerParams(collective_id=0, has_side_effects=True, vmem_limit_bytes=63 * 2**20),
            name="backtransform",
        )(z_cols.T, v_local, t_local.transpose(0, 2, 1))
        return z_t.T

    return jax.shard_map(
        local_run,
        mesh=mesh,
        in_specs=(P("kpt", ("col", "row")), P(("kpt", "row"), "col"), P("kpt", None, None)),
        out_specs=P(("kpt", "row"), "col"),
        check_vma=False,
    )
```

```python
import jax
import jax.numpy as jnp
from jax import lax
from jax.experimental import pallas as pl
from jax.experimental.pallas import tpu as pltpu
from jax.sharding import PartitionSpec as P

PRECISE = lax.Precision.HIGHEST
MESH = pl.DeviceIdType.MESH

W = 32
ROWS = 1536
TILE = 256
HALF = 128
NT = ROWS // TILE
NB = 24
VT = 4 * sum(range(1, NT + 1))
AHEAD = 12


def _dot(a, b, ca, cb):
    return lax.dot_general(a, b, (((ca,), (cb,)), ((), ())), precision=PRECISE, preferred_element_type=jnp.float32)


def _base(b):
    q, i = b // 4, b % 4
    return 4 * (NT * q - (q * (q - 1)) // 2) + i * (NT - q)


def _panel(idx):
    return jnp.where(idx < HALF, 2 * (idx // W), 2 * ((idx - HALF) // W) + 1)


def _pairs(lo, n, body):
    def two(h, carry):
        body(lo + 2 * h)
        body(lo + 2 * h + 1)
        return carry

    lax.fori_loop(0, n // 2, two, 0)

    @pl.when(n % 2 == 1)
    def _():
        body(lo + n - 1)


def _kernel(zt_in, v_in, tt_in, out, vbuf, vtr, zt, tt, acc, srecv, wbuf, gacc, usend, urecv, uhalf, upack, tbuf,
            loc_sem, ys_sem, yr_sem, os_sem, or_sem, fs_sem, fr_sem, zs_sem, zr_sem,
            ss_sem, sr_sem, us_sem, ur_sem, hs_sem, hr_sem, ts_sem, tr_sem, tt_sem, zo_sem, out_sem, outs_sem, outr_sem):
    ridx = lax.axis_index("row")
    y = lax.axis_index("col")
    x, c = ridx // 2, ridx % 2
    xn = {"row": (ridx + 2) % 4}
    sib = {"row": ridx + 1 - 2 * c}
    yn = {"col": 1 - y}

    barrier = pltpu.get_barrier_semaphore()
    for dev in (xn, sib, yn):
        pl.semaphore_signal(barrier, inc=1, device_id=dev, device_id_type=MESH)

    def remote(src, dst, send, recv, dev):
        return pltpu.make_async_remote_copy(src, dst, send, recv, device_id=dev, device_id_type=MESH)

    def slab(b, rho, par):
        start = (rho * VT + _base(b)) * TILE + 64 * (b % 4)
        return vbuf.at[pl.ds(pl.multiple_of(start, 64), ROWS - 64 * b), pl.ds(pl.multiple_of(par * HALF, HALF), HALF)]

    def v_local(b):
        return pltpu.make_async_copy(v_in.at[pl.ds(64 * b, ROWS - 64 * b), pl.ds(HALF * b, HALF)], slab(b, c, y), loc_sem.at[b])

    def v_y(b, par):
        return remote(slab(b, c, par), slab(b, c, par), ys_sem.at[b], yr_sem.at[b], yn)

    def v_own(b, rho):
        return remote(slab(b, rho, y), slab(b, rho, y), os_sem.at[b], or_sem.at[b], sib)

    def v_fwd(b, rho):
        return remote(slab(b, rho, 1 - y), slab(b, rho, 1 - y), fs_sem.at[b], fr_sem.at[b], sib)

    def v_issue(b):
        v_local(b).wait()
        v_y(b, y).start()
        v_own(b, c).start()

    def static_block(b, fn):
        for qq in range(NT):

            @pl.when(b // 4 == qq)
            def _(qq=qq):
                for ii in range(4):

                    @pl.when(b % 4 == ii)
                    def _(ii=ii):
                        fn(4 * qq + ii)

    def z_own(t, rho):
        return pltpu.make_async_copy(
            zt_in.at[:, pl.ds(pl.multiple_of((2 * x + rho) * ROWS + t * TILE, TILE), TILE)],
            zt.at[x, :, pl.ds((2 * t + rho) * TILE, TILE)], zo_sem.at[2 * t + rho])

    def z_chunk(t, j, g):
        src = (2 * (1 - x) + j // 2) * ROWS + t * TILE + (j % 2) * HALF
        return remote(
            zt_in.at[:, pl.ds(pl.multiple_of(src, HALF), HALF)],
            zt.at[g, :, pl.ds(pl.multiple_of(2 * t * TILE + j * HALF, HALF), HALF)],
            zs_sem.at[4 * t + j], zr_sem.at[4 * t + j], xn)

    tt_copy = pltpu.make_async_copy(tt_in, tt, tt_sem)

    for b in range(NB - 1, NB - 5, -1):
        v_local(b).start()
    tt_copy.start()
    for t in range(NT - 1, -1, -1):
        for rho in range(2):
            z_own(t, rho).start()
    for b in range(NB - 5, -1, -1):
        v_local(b).start()
    for b in range(NB):
        if b % 4:
            for rho in range(2):
                vbuf[pl.ds((rho * VT + _base(b)) * TILE, 64 * (b % 4)), :] = jnp.zeros((64 * (b % 4), TILE), jnp.float32)

    pl.semaphore_wait(barrier, 3)
    for b in range(NB - 1, NB - 1 - AHEAD, -1):
        v_issue(b)
        if b == NB - 2:
            for j in range(4):
                z_chunk(NT - 1, j, x).start()
    for t in range(NT):
        for rho in range(2):
            z_own(t, rho).wait()
    tt_copy.wait()

    def rows(b, t, rho):
        return pl.ds(pl.multiple_of((rho * VT + _base(b) + t - b // 4) * TILE, TILE), TILE)

    def v_tile(b, t):
        return jnp.concatenate([vbuf[rows(b, t, rho), :] for rho in range(2)], axis=0)

    def cols(t):
        return pl.ds(pl.multiple_of(t * 2 * TILE, 2 * TILE), 2 * TILE)

    def s_copy(g, b):
        return remote(acc.at[g], srecv.at[g, b % 2], ss_sem.at[g], sr_sem.at[g, b % 2], xn)

    def weights(g, b):
        if g == 0:

            @pl.when(b % 2 != c)
            def _():
                t_copy(b).wait_recv()

        s_copy(g, b).wait_recv()
        s_sum = acc[g] + srecv[g, b % 2]
        wbuf[...] = _dot(s_sum, tbuf[b % 4], 1, 0)
        s_copy(g, b).wait_send()

    def update(g, b, t):
        if g == 0:
            v_tr = v_tile(b, t).T
            vtr[:, cols(t)] = v_tr
        else:
            v_tr = vtr[:, cols(t)]
        zt[g, :, cols(t)] = zt[g, :, cols(t)] - _dot(wbuf[...], v_tr, 1, 0)

    def partial_s(g, b, t):
        acc[g] += _dot(zt[g, :, cols(t)], v_tile(b, t), 1, 0)

    def sweep(g, k):
        @pl.when(k < NB - 1)
        def _():
            weights(g, k + 1)

        acc[g] = jnp.zeros((HALF, TILE), jnp.float32)
        first = (k + 1) // 4
        late = jnp.where(k % 4 == 3, 0, 1)

        @pl.when(late == 1)
        def _():
            update(g, k + 1, first)

        def both(t):
            partial_s(g, k, t - 1)
            update(g, k + 1, t)

        _pairs(first + late, NT - first - late, both)
        partial_s(g, k, NT - 1)
        s_copy(g, k).start()

    ra = lax.broadcasted_iota(jnp.int32, (HALF, HALF), 0) // W
    rb = lax.broadcasted_iota(jnp.int32, (HALF, HALF), 1) // W

    def u_copy(b):
        return remote(usend.at[b % 2], urecv.at[b % 4], us_sem.at[b % 2], ur_sem.at[b % 4], xn)

    half_copy = remote(uhalf, upack.at[c], hs_sem, hr_sem, sib)

    def t_copy(b):
        return remote(tbuf.at[b % 4], tbuf.at[b % 4], ts_sem, tr_sem.at[b % 4], sib)

    def gram(b):
        def tile(t):
            own = jnp.concatenate(
                [vbuf[rows(b, t, rho), pl.ds(pl.multiple_of(c * HALF, HALF), HALF)] for rho in range(2)], axis=0)
            gacc[...] += _dot(own, v_tile(b, t), 0, 0)

        gacc[...] = jnp.zeros((HALF, TILE), jnp.float32)
        _pairs(b // 4, NT - b // 4, tile)

        def cols_of(par):
            return gacc[:, pl.ds(pl.multiple_of(par * HALF, HALF), HALF)]

        usend[b % 2] = jnp.where(ra <= rb, cols_of(1 - c), cols_of(c))
        u_copy(b).start()

    def u_half(b):
        u_copy(b).wait()
        total = usend[b % 2] + urecv[b % 4]

        @pl.when(b % 2 == c)
        def _():
            upack[c] = total

        @pl.when(b % 2 != c)
        def _():
            @pl.when(b < NB - 2)
            def _():
                half_copy.wait_send()

            uhalf[...] = total
            half_copy.start()

    def merge(b):
        half_copy.wait_recv()
        slot = b % 4

        @pl.when(b < NB - 2)
        def _():
            t_copy(b).wait_send()

        same = ra == rb

        def diagonal(par):
            stack = jnp.concatenate([tt[8 * b + 2 * i + par] for i in range(4)], axis=0)
            return jnp.where(same, jnp.concatenate([stack] * 4, axis=1), 0.0)

        even_part, odd_part = upack[0], upack[1]
        eo = jnp.where(ra <= rb, even_part, 0.0).T
        u_tr = jnp.concatenate([
            jnp.concatenate([jnp.where(ra > rb, even_part, 0.0), jnp.where(ra < rb, odd_part, 0.0).T], axis=1),
            jnp.concatenate([eo, jnp.where(ra > rb, odd_part, 0.0)], axis=1)], axis=0)
        even, odd = diagonal(0), diagonal(1)
        pairs = jnp.where(same, eo, 0.0)
        tbuf[slot, :HALF, :HALF] = even
        tbuf[slot, :HALF, HALF:] = jnp.zeros((HALF, HALF), jnp.float32)
        tbuf[slot, HALF:, :HALF] = -_dot(_dot(odd, pairs, 1, 0), even, 1, 0)
        tbuf[slot, HALF:, HALF:] = odd
        pa = _panel(lax.broadcasted_iota(jnp.int32, (TILE, TILE), 0))
        pb = _panel(lax.broadcasted_iota(jnp.int32, (TILE, TILE), 1))
        for size in (2, 4):
            level = (pa // (2 * size) == pb // (2 * size)) & (pa // size > pb // size)
            t_now = tbuf[slot]
            tbuf[slot] = t_now - _dot(_dot(t_now, jnp.where(level, u_tr, 0.0), 1, 0), t_now, 1, 0)
        t_copy(b).start()

    def step(s, carry):
        k = NB + 1 - s
        b_sweep = jnp.where(k == NB, NB - 1, k)
        sweeps = (k < NB - 1) | (k == NB)

        @pl.when(sweeps)
        def _():
            @pl.when(b_sweep % 4 == 3)
            def _():
                for j in range(4):
                    z_chunk(b_sweep // 4, j, 1 - x).wait_recv()

            sweep(0, b_sweep)

        @pl.when(k >= 2)
        def _():
            def forward(b):
                v_y(b, 1 - y).wait_recv()
                v_fwd(b, c).start()

            static_block(k - 2, forward)

        @pl.when((k >= 1) & (k <= NB) & ((k - 1) % 2 != c))
        def _():
            u_half(k - 1)

        @pl.when(sweeps)
        def _():
            sweep(1, b_sweep)

        @pl.when((k >= AHEAD) & (k < NB))
        def _():
            static_block(k - AHEAD, v_issue)

        @pl.when(k >= 2)
        def _():
            def arrived(b):
                v_own(b, 1 - c).wait_recv()
                v_fwd(b, 1 - c).wait_recv()

            static_block(k - 2, arrived)
            gram(k - 2)

        @pl.when(k >= 6)
        def _():
            z_chunk((k - 6) // 4, 3 - (k - 6) % 4, x).start()

        b_merge = jnp.where(k == 0, 0, k - 1)

        @pl.when((k != 1) & (k <= NB) & (b_merge % 2 == c))
        def _():
            u_half(b_merge)
            merge(b_merge)

        return carry

    lax.fori_loop(0, NB + 2, step, 0)

    def out_rows(g):
        return pl.ds(pl.multiple_of((2 * g + c) * HALF, HALF), HALF)

    def out_cols(t):
        return pl.ds(t * TILE, TILE)

    def out_local(g, t):
        return pltpu.make_async_copy(
            zt.at[g, :, pl.ds(pl.multiple_of((2 * t + c) * TILE, TILE), TILE)], out.at[out_rows(g), out_cols(t)],
            out_sem.at[g * NT + t])

    def out_sib(g, t):
        return remote(
            zt.at[g, :, pl.ds(pl.multiple_of((2 * t + 1 - c) * TILE, TILE), TILE)], out.at[out_rows(g), out_cols(t)],
            outs_sem.at[g * NT + t], outr_sem.at[g * NT + t], sib)

    def out_from_sib(g, t):
        part = out.at[pl.ds(pl.multiple_of((2 * g + 1 - c) * HALF, HALF), HALF), out_cols(t)]
        return remote(part, part, outs_sem.at[g * NT + t], outr_sem.at[g * NT + t], sib)

    for g in range(2):
        weights(g, 0)
        _pairs(0, NT, lambda t, g=g: update(g, 0, t))
        for t in range(NT):
            out_local(g, t).start()
            out_sib(g, t).start()

    half_copy.wait_send()
    t_copy(0).wait_send()
    for b in range(NB):
        v_y(b, y).wait_send()
        v_own(b, c).wait_send()
        v_fwd(b, c).wait_send()
        z_chunk(b // 4, b % 4, x).wait_send()
    for g in range(2):
        for t in range(NT):
            out_local(g, t).wait()
            out_sib(g, t).wait_send()
            out_from_sib(g, t).wait_recv()


def solution(mesh):
    def local_run(z_cols, v_local, t_local):
        f32 = jnp.float32
        any_spec = pl.BlockSpec(memory_space=pl.ANY)
        dma = pltpu.SemaphoreType.DMA
        z_t = pl.pallas_call(
            _kernel,
            out_shape=jax.ShapeDtypeStruct((4 * HALF, ROWS), f32),
            in_specs=[any_spec] * 3,
            out_specs=any_spec,
            scratch_shapes=[
                pltpu.VMEM((2 * VT * TILE, TILE), f32),
                pltpu.VMEM((TILE, 2 * ROWS), f32),
                pltpu.VMEM((2, HALF, 2 * ROWS), f32),
                pltpu.VMEM((NB * 8, W, W), f32),
                pltpu.VMEM((2, HALF, TILE), f32),
                pltpu.VMEM((2, 2, HALF, TILE), f32),
                pltpu.VMEM((HALF, TILE), f32),
                pltpu.VMEM((HALF, TILE), f32),
                pltpu.VMEM((2, HALF, HALF), f32),
                pltpu.VMEM((4, HALF, HALF), f32),
                pltpu.VMEM((HALF, HALF), f32),
                pltpu.VMEM((2, HALF, HALF), f32),
                pltpu.VMEM((4, TILE, TILE), f32),
                *[dma((NB,))] * 9,
                dma((2,)), dma((2, 2)), dma((2,)), dma((4,)), dma, dma, dma, dma((4,)), dma, *[dma((2 * NT,))] * 4,
            ],
            compiler_params=pltpu.CompilerParams(collective_id=0, has_side_effects=True, vmem_limit_bytes=63 * 2**20),
            name="backtransform",
        )(z_cols.T, v_local, t_local.transpose(0, 2, 1))
        return z_t.T

    return jax.shard_map(
        local_run,
        mesh=mesh,
        in_specs=(P("kpt", ("col", "row")), P(("kpt", "row"), "col"), P("kpt", None, None)),
        out_specs=P(("kpt", "row"), "col"),
        check_vma=False,
    )
```

```python
import jax
import jax.numpy as jnp
from jax import lax
from jax.experimental import pallas as pl
from jax.experimental.pallas import tpu as pltpu
from jax.sharding import PartitionSpec as P

PRECISE = lax.Precision.HIGHEST
MESH = pl.DeviceIdType.MESH

W = 32
ROWS = 1536
TILE = 256
HALF = 128
NT = ROWS // TILE
NB = 24
VT = 4 * sum(range(1, NT + 1))
AHEAD = 12


def _dot(a, b, ca, cb):
    return lax.dot_general(a, b, (((ca,), (cb,)), ((), ())), precision=PRECISE, preferred_element_type=jnp.float32)


def _base(b):
    q, i = b // 4, b % 4
    return 4 * (NT * q - (q * (q - 1)) // 2) + i * (NT - q)


def _panel(idx):
    return jnp.where(idx < HALF, 2 * (idx // W), 2 * ((idx - HALF) // W) + 1)


def _pairs(lo, n, body):
    def two(h, carry):
        body(lo + 2 * h)
        body(lo + 2 * h + 1)
        return carry

    lax.fori_loop(0, n // 2, two, 0)

    @pl.when(n % 2 == 1)
    def _():
        body(lo + n - 1)


def _kernel(z_in, v_in, t_in, out, vbuf, vtr, zt, zst, t_raw, tt, acc, srecv, wbuf, gacc, usend, urecv, uhalf, upack, tbuf,
            loc_sem, ys_sem, yr_sem, os_sem, or_sem, fs_sem, fr_sem, zs_sem, zr_sem,
            ss_sem, sr_sem, us_sem, ur_sem, hs_sem, hr_sem, ts_sem, tr_sem, tt_sem, zo_sem, out_sem, outs_sem, outr_sem):
    ridx = lax.axis_index("row")
    y = lax.axis_index("col")
    x, c = ridx // 2, ridx % 2
    xn = {"row": (ridx + 2) % 4}
    sib = {"row": ridx + 1 - 2 * c}
    yn = {"col": 1 - y}

    barrier = pltpu.get_barrier_semaphore()
    for dev in (xn, sib, yn):
        pl.semaphore_signal(barrier, inc=1, device_id=dev, device_id_type=MESH)

    def remote(src, dst, send, recv, dev):
        return pltpu.make_async_remote_copy(src, dst, send, recv, device_id=dev, device_id_type=MESH)

    def slab(b, rho, par):
        start = (rho * VT + _base(b)) * TILE + 64 * (b % 4)
        return vbuf.at[pl.ds(pl.multiple_of(start, 64), ROWS - 64 * b), pl.ds(pl.multiple_of(par * HALF, HALF), HALF)]

    def v_local(b):
        return pltpu.make_async_copy(v_in.at[pl.ds(64 * b, ROWS - 64 * b), pl.ds(HALF * b, HALF)], slab(b, c, y), loc_sem.at[b])

    def v_y(b, par):
        return remote(slab(b, c, par), slab(b, c, par), ys_sem.at[b], yr_sem.at[b], yn)

    def v_own(b, rho):
        return remote(slab(b, rho, y), slab(b, rho, y), os_sem.at[b], or_sem.at[b], sib)

    def v_fwd(b, rho):
        return remote(slab(b, rho, 1 - y), slab(b, rho, 1 - y), fs_sem.at[b], fr_sem.at[b], sib)

    def v_issue(b):
        v_local(b).wait()
        v_y(b, y).start()
        v_own(b, c).start()

    def static_block(b, fn):
        for qq in range(NT):

            @pl.when(b // 4 == qq)
            def _(qq=qq):
                for ii in range(4):

                    @pl.when(b % 4 == ii)
                    def _(ii=ii):
                        fn(4 * qq + ii)

    def z_own(t, rho):
        return pltpu.make_async_copy(
            z_in.at[pl.ds(pl.multiple_of((2 * x + rho) * ROWS + t * TILE, TILE), TILE), :],
            zst.at[x, t, pl.ds(rho * TILE, TILE), :], zo_sem.at[2 * t + rho])

    def z_chunk(t, j, g):
        src = (2 * (1 - x) + j // 2) * ROWS + t * TILE + (j % 2) * HALF
        return remote(
            z_in.at[pl.ds(pl.multiple_of(src, HALF), HALF), :],
            zst.at[g, t, pl.ds(pl.multiple_of(j * HALF, HALF), HALF), :],
            zs_sem.at[4 * t + j], zr_sem.at[4 * t + j], xn)

    t_copy_in = pltpu.make_async_copy(t_in, t_raw, tt_sem)

    for b in range(NB - 1, NB - 5, -1):
        v_local(b).start()
    t_copy_in.start()
    for t in range(NT - 1, -1, -1):
        for rho in range(2):
            z_own(t, rho).start()
    for b in range(NB - 5, -1, -1):
        v_local(b).start()
    for b in range(NB):
        if b % 4:
            for rho in range(2):
                vbuf[pl.ds((rho * VT + _base(b)) * TILE, 64 * (b % 4)), :] = jnp.zeros((64 * (b % 4), TILE), jnp.float32)

    pl.semaphore_wait(barrier, 3)
    for b in range(NB - 1, NB - 1 - AHEAD, -1):
        v_issue(b)
        if b == NB - 2:
            for j in range(4):
                z_chunk(NT - 1, j, x).start()
    for t in range(NT):
        for rho in range(2):
            z_own(t, rho).wait()
    t_copy_in.wait()

    def t_row(i, carry):
        tt[pl.ds(i, NB * 8, stride=W), :] = t_raw[i].T
        return carry

    lax.fori_loop(0, W, t_row, 0)

    def rows(b, t, rho):
        return pl.ds(pl.multiple_of((rho * VT + _base(b) + t - b // 4) * TILE, TILE), TILE)

    def v_tile(b, t):
        return jnp.concatenate([vbuf[rows(b, t, rho), :] for rho in range(2)], axis=0)

    def cols(t):
        return pl.ds(pl.multiple_of(t * 2 * TILE, 2 * TILE), 2 * TILE)

    def s_copy(g, b):
        return remote(acc.at[g], srecv.at[g, b % 2], ss_sem.at[g], sr_sem.at[g, b % 2], xn)

    def weights(g, b):
        if g == 0:

            @pl.when(b % 2 != c)
            def _():
                t_copy(b).wait_recv()

        s_copy(g, b).wait_recv()
        s_sum = acc[g] + srecv[g, b % 2]
        wbuf[...] = _dot(s_sum, tbuf[b % 4], 1, 0)
        s_copy(g, b).wait_send()

    def update(g, b, t):
        if g == 0:
            v_tr = v_tile(b, t).T
            vtr[:, cols(t)] = v_tr
        else:
            v_tr = vtr[:, cols(t)]
        zt[g, :, cols(t)] = zt[g, :, cols(t)] - _dot(wbuf[...], v_tr, 1, 0)

    def partial_s(g, b, t):
        acc[g] += _dot(zt[g, :, cols(t)], v_tile(b, t), 1, 0)

    def sweep(g, k):
        @pl.when(k < NB - 1)
        def _():
            weights(g, k + 1)

        acc[g] = jnp.zeros((HALF, TILE), jnp.float32)
        first = (k + 1) // 4
        late = jnp.where(k % 4 == 3, 0, 1)

        @pl.when(late == 1)
        def _():
            update(g, k + 1, first)

        def both(t):
            partial_s(g, k, t - 1)
            update(g, k + 1, t)

        _pairs(first + late, NT - first - late, both)
        partial_s(g, k, NT - 1)
        s_copy(g, k).start()

    ra = lax.broadcasted_iota(jnp.int32, (HALF, HALF), 0) // W
    rb = lax.broadcasted_iota(jnp.int32, (HALF, HALF), 1) // W

    def u_copy(b):
        return remote(usend.at[b % 2], urecv.at[b % 4], us_sem.at[b % 2], ur_sem.at[b % 4], xn)

    half_copy = remote(uhalf, upack.at[c], hs_sem, hr_sem, sib)

    def t_copy(b):
        return remote(tbuf.at[b % 4], tbuf.at[b % 4], ts_sem, tr_sem.at[b % 4], sib)

    def gram(b):
        def tile(t):
            own = jnp.concatenate(
                [vbuf[rows(b, t, rho), pl.ds(pl.multiple_of(c * HALF, HALF), HALF)] for rho in range(2)], axis=0)
            gacc[...] += _dot(own, v_tile(b, t), 0, 0)

        gacc[...] = jnp.zeros((HALF, TILE), jnp.float32)
        _pairs(b // 4, NT - b // 4, tile)

        def cols_of(par):
            return gacc[:, pl.ds(pl.multiple_of(par * HALF, HALF), HALF)]

        usend[b % 2] = jnp.where(ra <= rb, cols_of(1 - c), cols_of(c))
        u_copy(b).start()

    def u_half(b):
        u_copy(b).wait()
        total = usend[b % 2] + urecv[b % 4]

        @pl.when(b % 2 == c)
        def _():
            upack[c] = total

        @pl.when(b % 2 != c)
        def _():
            @pl.when(b < NB - 2)
            def _():
                half_copy.wait_send()

            uhalf[...] = total
            half_copy.start()

    def merge(b):
        half_copy.wait_recv()
        slot = b % 4

        @pl.when(b < NB - 2)
        def _():
            t_copy(b).wait_send()

        same = ra == rb

        def diagonal(par):
            at = [pl.multiple_of((8 * b + 2 * i + par) * W, W) for i in range(4)]
            stack = jnp.concatenate([tt[pl.ds(row, W), :] for row in at], axis=0)
            return jnp.where(same, jnp.concatenate([stack] * 4, axis=1), 0.0).T

        even_part, odd_part = upack[0], upack[1]
        eo = jnp.where(ra <= rb, even_part, 0.0).T
        u_tr = jnp.concatenate([
            jnp.concatenate([jnp.where(ra > rb, even_part, 0.0), jnp.where(ra < rb, odd_part, 0.0).T], axis=1),
            jnp.concatenate([eo, jnp.where(ra > rb, odd_part, 0.0)], axis=1)], axis=0)
        even, odd = diagonal(0), diagonal(1)
        pairs = jnp.where(same, eo, 0.0)
        tbuf[slot, :HALF, :HALF] = even
        tbuf[slot, :HALF, HALF:] = jnp.zeros((HALF, HALF), jnp.float32)
        tbuf[slot, HALF:, :HALF] = -_dot(_dot(odd, pairs, 1, 0), even, 1, 0)
        tbuf[slot, HALF:, HALF:] = odd
        pa = _panel(lax.broadcasted_iota(jnp.int32, (TILE, TILE), 0))
        pb = _panel(lax.broadcasted_iota(jnp.int32, (TILE, TILE), 1))
        for size in (2, 4):
            level = (pa // (2 * size) == pb // (2 * size)) & (pa // size > pb // size)
            t_now = tbuf[slot]
            tbuf[slot] = t_now - _dot(_dot(t_now, jnp.where(level, u_tr, 0.0), 1, 0), t_now, 1, 0)
        t_copy(b).start()

    def step(s, carry):
        k = NB + 1 - s
        b_sweep = jnp.where(k == NB, NB - 1, k)
        sweeps = (k < NB - 1) | (k == NB)

        @pl.when(sweeps)
        def _():
            @pl.when(b_sweep % 4 == 3)
            def _():
                for j in range(4):
                    z_chunk(b_sweep // 4, j, 1 - x).wait_recv()
                for g in range(2):
                    zt[g, :, cols(b_sweep // 4)] = zst[g, b_sweep // 4].T

            sweep(0, b_sweep)

        @pl.when(k >= 2)
        def _():
            def forward(b):
                v_y(b, 1 - y).wait_recv()
                v_fwd(b, c).start()

            static_block(k - 2, forward)

        @pl.when((k >= 1) & (k <= NB) & ((k - 1) % 2 != c))
        def _():
            u_half(k - 1)

        @pl.when(sweeps)
        def _():
            sweep(1, b_sweep)

        @pl.when((k >= AHEAD) & (k < NB))
        def _():
            static_block(k - AHEAD, v_issue)

        @pl.when(k >= 2)
        def _():
            def arrived(b):
                v_own(b, 1 - c).wait_recv()
                v_fwd(b, 1 - c).wait_recv()

            static_block(k - 2, arrived)
            gram(k - 2)

        @pl.when(k >= 6)
        def _():
            z_chunk((k - 6) // 4, 3 - (k - 6) % 4, x).start()

        b_merge = jnp.where(k == 0, 0, k - 1)

        @pl.when((k != 1) & (k <= NB) & (b_merge % 2 == c))
        def _():
            u_half(b_merge)
            merge(b_merge)

        return carry

    lax.fori_loop(0, NB + 2, step, 0)

    def out_part(g, t, core):
        return out.at[pl.ds(t * TILE, TILE), pl.ds(pl.multiple_of((2 * g + core) * HALF, HALF), HALF)]

    def z_part(g, t, rho):
        return zst.at[g, t, pl.ds(pl.multiple_of(rho * TILE, TILE), TILE), :]

    def out_local(g, t):
        return pltpu.make_async_copy(z_part(g, t, c), out_part(g, t, c), out_sem.at[g * NT + t])

    def out_sib(g, t):
        return remote(z_part(g, t, 1 - c), out_part(g, t, c), outs_sem.at[g * NT + t], outr_sem.at[g * NT + t], sib)

    def out_from_sib(g, t):
        part = out_part(g, t, 1 - c)
        return remote(part, part, outs_sem.at[g * NT + t], outr_sem.at[g * NT + t], sib)

    for g in range(2):
        weights(g, 0)

        def last(t, g=g):
            update(g, 0, t)
            zst[g, t] = zt[g, :, cols(t)].T

        _pairs(0, NT, last)
        for t in range(NT):
            out_local(g, t).start()
            out_sib(g, t).start()

    half_copy.wait_send()
    t_copy(0).wait_send()
    for b in range(NB):
        v_y(b, y).wait_send()
        v_own(b, c).wait_send()
        v_fwd(b, c).wait_send()
        z_chunk(b // 4, b % 4, x).wait_send()
    for g in range(2):
        for t in range(NT):
            out_local(g, t).wait()
            out_sib(g, t).wait_send()
            out_from_sib(g, t).wait_recv()


def solution(mesh):
    def local_run(z_cols, v_local, t_local):
        f32 = jnp.float32
        any_spec = pl.BlockSpec(memory_space=pl.ANY)
        dma = pltpu.SemaphoreType.DMA
        return pl.pallas_call(
            _kernel,
            out_shape=jax.ShapeDtypeStruct((ROWS, 4 * HALF), f32),
            in_specs=[any_spec] * 3,
            out_specs=any_spec,
            scratch_shapes=[
                pltpu.VMEM((2 * VT * TILE, TILE), f32),
                pltpu.VMEM((TILE, 2 * ROWS), f32),
                pltpu.VMEM((2, HALF, 2 * ROWS), f32),
                pltpu.VMEM((2, NT, 2 * TILE, HALF), f32),
                pltpu.VMEM((W, W, NB * 8), f32),
                pltpu.VMEM((NB * 8 * W, W), f32),
                pltpu.VMEM((2, HALF, TILE), f32),
                pltpu.VMEM((2, 2, HALF, TILE), f32),
                pltpu.VMEM((HALF, TILE), f32),
                pltpu.VMEM((HALF, TILE), f32),
                pltpu.VMEM((2, HALF, HALF), f32),
                pltpu.VMEM((4, HALF, HALF), f32),
                pltpu.VMEM((HALF, HALF), f32),
                pltpu.VMEM((2, HALF, HALF), f32),
                pltpu.VMEM((4, TILE, TILE), f32),
                *[dma((NB,))] * 9,
                dma((2,)), dma((2, 2)), dma((2,)), dma((4,)), dma, dma, dma, dma((4,)), dma, *[dma((2 * NT,))] * 4,
            ],
            compiler_params=pltpu.CompilerParams(collective_id=0, has_side_effects=True, vmem_limit_bytes=63 * 2**20),
            name="backtransform",
        )(z_cols, v_local, t_local.transpose(1, 2, 0))

    return jax.shard_map(
        local_run,
        mesh=mesh,
        in_specs=(P("kpt", ("col", "row")), P(("kpt", "row"), "col"), P("kpt", None, None)),
        out_specs=P(("kpt", "row"), "col"),
        check_vma=False,
    )
```

```python
import jax
import jax.numpy as jnp
from jax import lax
from jax.experimental import pallas as pl
from jax.experimental.pallas import tpu as pltpu
from jax.sharding import PartitionSpec as P

PRECISE = lax.Precision.HIGHEST
MESH = pl.DeviceIdType.MESH

W = 32
ROWS = 1536
TILE = 256
HALF = 128
NT = ROWS // TILE
NB = 24
VT = 4 * sum(range(1, NT + 1))
PITCH = 40
AHEAD = 12


def _dot(a, b, ca, cb):
    return lax.dot_general(a, b, (((ca,), (cb,)), ((), ())), precision=PRECISE, preferred_element_type=jnp.float32)


def _base(b):
    q, i = b // 4, b % 4
    return 4 * (NT * q - (q * (q - 1)) // 2) + i * (NT - q)


def _panel(idx):
    return jnp.where(idx < HALF, 2 * (idx // W), 2 * ((idx - HALF) // W) + 1)


def _pairs(lo, n, body):
    def two(h, carry):
        body(lo + 2 * h)
        body(lo + 2 * h + 1)
        return carry

    lax.fori_loop(0, n // 2, two, 0)

    @pl.when(n % 2 == 1)
    def _():
        body(lo + n - 1)


def _kernel(z_in, v_in, t_in, out, vbuf, vtr, zt, zst, t_raw, tt, acc, srecv, wbuf, gacc, usend, urecv, uhalf, upack, tbuf,
            loc_sem, ys_sem, yr_sem, os_sem, or_sem, fs_sem, fr_sem, zs_sem, zr_sem,
            ss_sem, sr_sem, us_sem, ur_sem, hs_sem, hr_sem, ts_sem, tr_sem, tt_sem, zo_sem, out_sem, outs_sem, outr_sem):
    ridx = lax.axis_index("row")
    y = lax.axis_index("col")
    x, c = ridx // 2, ridx % 2
    xn = {"row": (ridx + 2) % 4}
    sib = {"row": ridx + 1 - 2 * c}
    yn = {"col": 1 - y}

    barrier = pltpu.get_barrier_semaphore()
    for dev in (xn, sib, yn):
        pl.semaphore_signal(barrier, inc=1, device_id=dev, device_id_type=MESH)

    def remote(src, dst, send, recv, dev):
        return pltpu.make_async_remote_copy(src, dst, send, recv, device_id=dev, device_id_type=MESH)

    def slab(b, rho, par):
        start = (rho * VT + _base(b)) * TILE + 64 * (b % 4)
        return vbuf.at[pl.ds(pl.multiple_of(start, 64), ROWS - 64 * b), pl.ds(pl.multiple_of(par * HALF, HALF), HALF)]

    def v_local(b):
        return pltpu.make_async_copy(v_in.at[pl.ds(64 * b, ROWS - 64 * b), pl.ds(HALF * b, HALF)], slab(b, c, y), loc_sem.at[b])

    def v_y(b, par):
        return remote(slab(b, c, par), slab(b, c, par), ys_sem.at[b], yr_sem.at[b], yn)

    def v_own(b, rho):
        return remote(slab(b, rho, y), slab(b, rho, y), os_sem.at[b], or_sem.at[b], sib)

    def v_fwd(b, rho):
        return remote(slab(b, rho, 1 - y), slab(b, rho, 1 - y), fs_sem.at[b], fr_sem.at[b], sib)

    def v_issue(b):
        v_local(b).wait()
        v_y(b, y).start()
        v_own(b, c).start()

    def static_block(b, fn):
        for qq in range(NT):

            @pl.when(b // 4 == qq)
            def _(qq=qq):
                for ii in range(4):

                    @pl.when(b % 4 == ii)
                    def _(ii=ii):
                        fn(4 * qq + ii)

    def z_own(t, rho):
        return pltpu.make_async_copy(
            z_in.at[pl.ds(pl.multiple_of((2 * x + rho) * ROWS + t * TILE, TILE), TILE), :],
            zst.at[x, t, pl.ds(rho * TILE, TILE), :], zo_sem.at[2 * t + rho])

    def z_chunk(t, j, g):
        src = (2 * (1 - x) + j // 2) * ROWS + t * TILE + (j % 2) * HALF
        return remote(
            z_in.at[pl.ds(pl.multiple_of(src, HALF), HALF), :],
            zst.at[g, t, pl.ds(pl.multiple_of(j * HALF, HALF), HALF), :],
            zs_sem.at[4 * t + j], zr_sem.at[4 * t + j], xn)

    t_copy_in = pltpu.make_async_copy(t_in, t_raw, tt_sem)

    for b in range(NB - 1, NB - 5, -1):
        v_local(b).start()
    t_copy_in.start()
    for t in range(NT - 1, -1, -1):
        for rho in range(2):
            z_own(t, rho).start()
    for b in range(NB - 5, -1, -1):
        v_local(b).start()
    for b in range(NB):
        if b % 4:
            for rho in range(2):
                vbuf[pl.ds((rho * VT + _base(b)) * TILE, 64 * (b % 4)), :] = jnp.zeros((64 * (b % 4), TILE), jnp.float32)

    pl.semaphore_wait(barrier, 3)
    for b in range(NB - 1, NB - 1 - AHEAD, -1):
        v_issue(b)
        if b == NB - 2:
            for j in range(4):
                z_chunk(NT - 1, j, x).start()

    def rows(b, t, rho):
        return pl.ds(pl.multiple_of((rho * VT + _base(b) + t - b // 4) * TILE, TILE), TILE)

    def v_tile(b, t):
        return jnp.concatenate([vbuf[rows(b, t, rho), :] for rho in range(2)], axis=0)

    def cols(t):
        return pl.ds(pl.multiple_of(t * 2 * TILE, 2 * TILE), 2 * TILE)

    def s_copy(g, b):
        return remote(acc.at[g], srecv.at[g, b % 2], ss_sem.at[g], sr_sem.at[g, b % 2], xn)

    def weights(g, b):
        if g == 0:

            @pl.when(b % 2 != c)
            def _():
                t_copy(b).wait_recv()

        s_copy(g, b).wait_recv()
        s_sum = acc[g] + srecv[g, b % 2]
        wbuf[...] = _dot(s_sum, tbuf[b % 4], 1, 0)
        s_copy(g, b).wait_send()

    def update(g, b, t):
        if g == 0:
            v_tr = v_tile(b, t).T
            vtr[:, cols(t)] = v_tr
        else:
            v_tr = vtr[:, cols(t)]
        zt[g, :, cols(t)] = zt[g, :, cols(t)] - _dot(wbuf[...], v_tr, 1, 0)

    def partial_s(g, b, t):
        acc[g] += _dot(zt[g, :, cols(t)], v_tile(b, t), 1, 0)

    def sweep(g, k):
        @pl.when(k < NB - 1)
        def _():
            weights(g, k + 1)

        acc[g] = jnp.zeros((HALF, TILE), jnp.float32)
        first = (k + 1) // 4
        late = jnp.where(k % 4 == 3, 0, 1)

        @pl.when(late == 1)
        def _():
            update(g, k + 1, first)

        def both(t):
            partial_s(g, k, t - 1)
            update(g, k + 1, t)

        _pairs(first + late, NT - first - late, both)
        partial_s(g, k, NT - 1)
        s_copy(g, k).start()

    ra = lax.broadcasted_iota(jnp.int32, (HALF, HALF), 0) // W
    rb = lax.broadcasted_iota(jnp.int32, (HALF, HALF), 1) // W

    def u_copy(b):
        return remote(usend.at[b % 2], urecv.at[b % 4], us_sem.at[b % 2], ur_sem.at[b % 4], xn)

    half_copy = remote(uhalf, upack.at[c], hs_sem, hr_sem, sib)

    def t_copy(b):
        return remote(tbuf.at[b % 4], tbuf.at[b % 4], ts_sem, tr_sem.at[b % 4], sib)

    def gram(b):
        def tile(t):
            own = jnp.concatenate(
                [vbuf[rows(b, t, rho), pl.ds(pl.multiple_of(c * HALF, HALF), HALF)] for rho in range(2)], axis=0)
            gacc[...] += _dot(own, v_tile(b, t), 0, 0)

        gacc[...] = jnp.zeros((HALF, TILE), jnp.float32)
        _pairs(b // 4, NT - b // 4, tile)

        def cols_of(par):
            return gacc[:, pl.ds(pl.multiple_of(par * HALF, HALF), HALF)]

        usend[b % 2] = jnp.where(ra <= rb, cols_of(1 - c), cols_of(c))
        u_copy(b).start()

    def u_half(b):
        u_copy(b).wait()
        total = usend[b % 2] + urecv[b % 4]

        @pl.when(b % 2 == c)
        def _():
            upack[c] = total

        @pl.when(b % 2 != c)
        def _():
            @pl.when(b < NB - 2)
            def _():
                half_copy.wait_send()

            uhalf[...] = total
            half_copy.start()

    def merge(b):
        half_copy.wait_recv()
        slot = b % 4

        @pl.when(b < NB - 2)
        def _():
            t_copy(b).wait_send()

        same = ra == rb

        def diagonal(par):
            at = [pl.multiple_of((8 * b + 2 * i + par) * PITCH, 8) for i in range(4)]
            stack = jnp.concatenate([tt[pl.ds(row, W), :] for row in at], axis=0)
            return jnp.where(same, jnp.concatenate([stack] * 4, axis=1), 0.0).T

        lo, hi = slice(0, HALF // 2), slice(HALF // 2, HALF)
        even_part, odd_part = upack[0], upack[1]
        ee, oo = jnp.where(ra > rb, even_part, 0.0), jnp.where(ra > rb, odd_part, 0.0)
        oe, eo = jnp.where(ra <= rb, even_part, 0.0).T, jnp.where(ra < rb, odd_part, 0.0).T

        def quad(a, b_, c_, d, rows_, cols_):
            return jnp.concatenate([
                jnp.concatenate([a[rows_, cols_], b_[rows_, cols_]], axis=1),
                jnp.concatenate([c_[rows_, cols_], d[rows_, cols_]], axis=1)], axis=0)

        even, odd = diagonal(0), diagonal(1)
        cross = -_dot(_dot(odd, jnp.where(same, oe, 0.0), 1, 0), even, 1, 0)
        zero = jnp.zeros((HALF, HALF), jnp.float32)
        pa, pb = ra % 2, rb % 2
        t_diag = []
        for part in (lo, hi):
            t_now = quad(even, zero, cross, odd, part, part)
            u_now = jnp.where(pa > pb, quad(ee, eo, oe, oo, part, part), 0.0)
            t_diag.append(t_now - _dot(_dot(t_now, u_now, 1, 0), t_now, 1, 0))
        t_lo, t_hi = t_diag
        t_off = -_dot(_dot(t_hi, quad(ee, eo, oe, oo, hi, lo), 1, 0), t_lo, 1, 0)
        half0 = jnp.zeros((HALF // 2, HALF // 2), jnp.float32)
        for rows_, out_rows in ((lo, 0), (hi, HALF)):
            tbuf[slot, out_rows : out_rows + HALF // 2, :] = jnp.concatenate(
                [t_lo[rows_, lo], half0, t_lo[rows_, hi], half0], axis=1)
            tbuf[slot, out_rows + HALF // 2 : out_rows + HALF, :] = jnp.concatenate(
                [t_off[rows_, lo], t_hi[rows_, lo], t_off[rows_, hi], t_hi[rows_, hi]], axis=1)
        t_copy(b).start()

    def step(s, carry):
        k = NB + 1 - s
        b_sweep = jnp.where(k == NB, NB - 1, k)
        sweeps = (k < NB - 1) | (k == NB)

        @pl.when(sweeps)
        def _():
            @pl.when(b_sweep % 4 == 3)
            def _():
                for j in range(4):
                    z_chunk(b_sweep // 4, j, 1 - x).wait_recv()
                for rho in range(2):
                    z_own(b_sweep // 4, rho).wait()
                for g in range(2):
                    zt[g, :, cols(b_sweep // 4)] = zst[g, b_sweep // 4].T

            sweep(0, b_sweep)

        @pl.when(k >= 2)
        def _():
            def forward(b):
                v_y(b, 1 - y).wait_recv()
                v_fwd(b, c).start()

            static_block(k - 2, forward)

        @pl.when(k == NB)
        def _():
            t_copy_in.wait()

            def t_row(i, carry):
                tt[pl.ds(i, NB * 8, stride=PITCH), :] = t_raw[i].T
                return carry

            lax.fori_loop(0, W, t_row, 0)

        @pl.when((k >= 1) & (k <= NB) & ((k - 1) % 2 != c))
        def _():
            u_half(k - 1)

        @pl.when(sweeps)
        def _():
            sweep(1, b_sweep)

        @pl.when((k >= AHEAD) & (k < NB))
        def _():
            static_block(k - AHEAD, v_issue)

        @pl.when(k >= 2)
        def _():
            def arrived(b):
                v_own(b, 1 - c).wait_recv()
                v_fwd(b, 1 - c).wait_recv()

            static_block(k - 2, arrived)
            gram(k - 2)

        @pl.when(k >= 6)
        def _():
            z_chunk((k - 6) // 4, 3 - (k - 6) % 4, x).start()

        b_merge = jnp.where(k == 0, 0, k - 1)

        @pl.when((k != 1) & (k <= NB) & (b_merge % 2 == c))
        def _():
            u_half(b_merge)
            merge(b_merge)

        return carry

    lax.fori_loop(0, NB + 2, step, 0)

    def out_part(g, t, core):
        return out.at[pl.ds(t * TILE, TILE), pl.ds(pl.multiple_of((2 * g + core) * HALF, HALF), HALF)]

    def z_part(g, t, rho):
        return zst.at[g, t, pl.ds(pl.multiple_of(rho * TILE, TILE), TILE), :]

    def out_local(g, t):
        return pltpu.make_async_copy(z_part(g, t, c), out_part(g, t, c), out_sem.at[g * NT + t])

    def out_sib(g, t):
        return remote(z_part(g, t, 1 - c), out_part(g, t, c), outs_sem.at[g * NT + t], outr_sem.at[g * NT + t], sib)

    def out_from_sib(g, t):
        part = out_part(g, t, 1 - c)
        return remote(part, part, outs_sem.at[g * NT + t], outr_sem.at[g * NT + t], sib)

    for g in range(2):
        weights(g, 0)

        def last(t, g=g):
            update(g, 0, t)
            zst[g, t] = zt[g, :, cols(t)].T

        _pairs(0, NT, last)
        for t in range(NT):
            out_local(g, t).start()
            out_sib(g, t).start()

    half_copy.wait_send()
    t_copy(0).wait_send()
    for b in range(NB):
        v_y(b, y).wait_send()
        v_own(b, c).wait_send()
        v_fwd(b, c).wait_send()
        z_chunk(b // 4, b % 4, x).wait_send()
    for g in range(2):
        for t in range(NT):
            out_local(g, t).wait()
            out_sib(g, t).wait_send()
            out_from_sib(g, t).wait_recv()


def solution(mesh):
    def local_run(z_cols, v_local, t_local):
        f32 = jnp.float32
        any_spec = pl.BlockSpec(memory_space=pl.ANY)
        dma = pltpu.SemaphoreType.DMA
        return pl.pallas_call(
            _kernel,
            out_shape=jax.ShapeDtypeStruct((ROWS, 4 * HALF), f32),
            in_specs=[any_spec] * 3,
            out_specs=any_spec,
            scratch_shapes=[
                pltpu.VMEM((2 * VT * TILE, TILE), f32),
                pltpu.VMEM((TILE, 2 * ROWS), f32),
                pltpu.VMEM((2, HALF, 2 * ROWS), f32),
                pltpu.VMEM((2, NT, 2 * TILE, HALF), f32),
                pltpu.VMEM((W, W, NB * 8), f32),
                pltpu.VMEM((NB * 8 * PITCH, W), f32),
                pltpu.VMEM((2, HALF, TILE), f32),
                pltpu.VMEM((2, 2, HALF, TILE), f32),
                pltpu.VMEM((HALF, TILE), f32),
                pltpu.VMEM((HALF, TILE), f32),
                pltpu.VMEM((2, HALF, HALF), f32),
                pltpu.VMEM((4, HALF, HALF), f32),
                pltpu.VMEM((HALF, HALF), f32),
                pltpu.VMEM((2, HALF, HALF), f32),
                pltpu.VMEM((4, TILE, TILE), f32),
                *[dma((NB,))] * 9,
                dma((2,)), dma((2, 2)), dma((2,)), dma((4,)), dma, dma, dma, dma((4,)), dma, *[dma((2 * NT,))] * 4,
            ],
            compiler_params=pltpu.CompilerParams(collective_id=0, has_side_effects=True, vmem_limit_bytes=63 * 2**20),
            name="backtransform",
        )(z_cols, v_local, t_local.transpose(1, 2, 0))

    return jax.shard_map(
        local_run,
        mesh=mesh,
        in_specs=(P("kpt", ("col", "row")), P(("kpt", "row"), "col"), P("kpt", None, None)),
        out_specs=P(("kpt", "row"), "col"),
        check_vma=False,
    )
```

```python
import jax
import jax.numpy as jnp
from jax import lax
from jax.experimental import pallas as pl
from jax.experimental.pallas import tpu as pltpu
from jax.sharding import PartitionSpec as P

PRECISE = lax.Precision.HIGHEST
MESH = pl.DeviceIdType.MESH

W = 32
ROWS = 1536
TILE = 256
HALF = 128
NT = ROWS // TILE
NB = 24
VT = 4 * sum(range(1, NT + 1))
PITCH = 40
AHEAD = 12


def _dot(a, b, ca, cb):
    return lax.dot_general(a, b, (((ca,), (cb,)), ((), ())), precision=PRECISE, preferred_element_type=jnp.float32)


def _base(b):
    q, i = b // 4, b % 4
    return 4 * (NT * q - (q * (q - 1)) // 2) + i * (NT - q)


def _panel(idx):
    return jnp.where(idx < HALF, 2 * (idx // W), 2 * ((idx - HALF) // W) + 1)


def _pairs(lo, n, body):
    def two(h, carry):
        body(lo + 2 * h)
        body(lo + 2 * h + 1)
        return carry

    lax.fori_loop(0, n // 2, two, 0)

    @pl.when(n % 2 == 1)
    def _():
        body(lo + n - 1)


def _kernel(z_in, v_in, t_in, out, vbuf, vtr, zt, zst, t_raw, tt, acc, srecv, wbuf, gacc, usend, urecv, uhalf, upack, tbuf,
            loc_sem, ys_sem, yr_sem, os_sem, or_sem, fs_sem, fr_sem, zs_sem, zr_sem,
            ss_sem, sr_sem, us_sem, ur_sem, hs_sem, hr_sem, ts_sem, tr_sem, tt_sem, zo_sem, out_sem, outs_sem, outr_sem):
    ridx = lax.axis_index("row")
    y = lax.axis_index("col")
    x, c = ridx // 2, ridx % 2
    xn = {"row": (ridx + 2) % 4}
    sib = {"row": ridx + 1 - 2 * c}
    yn = {"col": 1 - y}

    barrier = pltpu.get_barrier_semaphore()
    for dev in (xn, sib, yn):
        pl.semaphore_signal(barrier, inc=1, device_id=dev, device_id_type=MESH)

    def remote(src, dst, send, recv, dev):
        return pltpu.make_async_remote_copy(src, dst, send, recv, device_id=dev, device_id_type=MESH)

    def slab(b, rho, par):
        start = (rho * VT + _base(b)) * TILE + 64 * (b % 4)
        return vbuf.at[pl.ds(pl.multiple_of(start, 64), ROWS - 64 * b), pl.ds(pl.multiple_of(par * HALF, HALF), HALF)]

    def v_local(b):
        return pltpu.make_async_copy(v_in.at[pl.ds(64 * b, ROWS - 64 * b), pl.ds(HALF * b, HALF)], slab(b, c, y), loc_sem.at[b])

    def v_y(b, par):
        return remote(slab(b, c, par), slab(b, c, par), ys_sem.at[b], yr_sem.at[b], yn)

    def v_own(b, rho):
        return remote(slab(b, rho, y), slab(b, rho, y), os_sem.at[b], or_sem.at[b], sib)

    def v_fwd(b, rho):
        return remote(slab(b, rho, 1 - y), slab(b, rho, 1 - y), fs_sem.at[b], fr_sem.at[b], sib)

    def v_issue(b):
        v_local(b).wait()
        v_y(b, y).start()
        v_own(b, c).start()

    def static_block(b, fn):
        for qq in range(NT):

            @pl.when(b // 4 == qq)
            def _(qq=qq):
                for ii in range(4):

                    @pl.when(b % 4 == ii)
                    def _(ii=ii):
                        fn(4 * qq + ii)

    def z_own(t, rho):
        return pltpu.make_async_copy(
            z_in.at[pl.ds(pl.multiple_of((2 * x + rho) * ROWS + t * TILE, TILE), TILE), :],
            zst.at[x, t, pl.ds(rho * TILE, TILE), :], zo_sem.at[2 * t + rho])

    def z_chunk(t, j, g):
        src = (2 * (1 - x) + j // 2) * ROWS + t * TILE + (j % 2) * HALF
        return remote(
            z_in.at[pl.ds(pl.multiple_of(src, HALF), HALF), :],
            zst.at[g, t, pl.ds(pl.multiple_of(j * HALF, HALF), HALF), :],
            zs_sem.at[4 * t + j], zr_sem.at[4 * t + j], xn)

    t_copy_in = pltpu.make_async_copy(t_in, t_raw, tt_sem)

    for b in range(NB - 1, NB - 5, -1):
        v_local(b).start()
    t_copy_in.start()
    for t in range(NT - 1, -1, -1):
        for rho in range(2):
            z_own(t, rho).start()
    for b in range(NB - 5, -1, -1):
        v_local(b).start()
    for b in range(NB):
        if b % 4:
            for rho in range(2):
                vbuf[pl.ds((rho * VT + _base(b)) * TILE, 64 * (b % 4)), :] = jnp.zeros((64 * (b % 4), TILE), jnp.float32)

    pl.semaphore_wait(barrier, 3)
    for b in range(NB - 1, NB - 1 - AHEAD, -1):
        v_issue(b)
        if b == NB - 2:
            for j in range(4):
                z_chunk(NT - 1, j, x).start()

    def rows(b, t, rho):
        return pl.ds(pl.multiple_of((rho * VT + _base(b) + t - b // 4) * TILE, TILE), TILE)

    def v_tile(b, t):
        return jnp.concatenate([vbuf[rows(b, t, rho), :] for rho in range(2)], axis=0)

    def cols(t):
        return pl.ds(pl.multiple_of(t * 2 * TILE, 2 * TILE), 2 * TILE)

    def s_copy(g, b):
        return remote(acc.at[g], srecv.at[g, b % 2], ss_sem.at[g], sr_sem.at[g, b % 2], xn)

    def weights(g, b):
        if g == 0:

            @pl.when(b % 2 != c)
            def _():
                t_copy(b).wait_recv()

        s_copy(g, b).wait_recv()
        s_sum = acc[g] + srecv[g, b % 2]
        wbuf[...] = _dot(s_sum, tbuf[b % 4], 1, 0)
        s_copy(g, b).wait_send()

    def update(g, b, t):
        if g == 0:
            v_tr = v_tile(b, t).T
            vtr[:, cols(t)] = v_tr
        else:
            v_tr = vtr[:, cols(t)]
        zt[g, :, cols(t)] = zt[g, :, cols(t)] - _dot(wbuf[...], v_tr, 1, 0)

    def partial_s(g, b, t):
        acc[g] += _dot(zt[g, :, cols(t)], v_tile(b, t), 1, 0)

    def sweep(g, k):
        @pl.when(k < NB - 1)
        def _():
            weights(g, k + 1)

        acc[g] = jnp.zeros((HALF, TILE), jnp.float32)
        first = (k + 1) // 4
        late = jnp.where(k % 4 == 3, 0, 1)

        @pl.when(late == 1)
        def _():
            update(g, k + 1, first)

        def both(t):
            partial_s(g, k, t - 1)
            update(g, k + 1, t)

        _pairs(first + late, NT - first - late, both)
        partial_s(g, k, NT - 1)
        s_copy(g, k).start()

    ra = lax.broadcasted_iota(jnp.int32, (HALF, HALF), 0) // W
    rb = lax.broadcasted_iota(jnp.int32, (HALF, HALF), 1) // W

    def u_copy(b):
        return remote(usend.at[b % 2], urecv.at[b % 4], us_sem.at[b % 2], ur_sem.at[b % 4], xn)

    half_copy = remote(uhalf, upack.at[c], hs_sem, hr_sem, sib)

    def t_copy(b):
        return remote(tbuf.at[b % 4], tbuf.at[b % 4], ts_sem, tr_sem.at[b % 4], sib)

    def gram(b):
        def tile(t):
            own = jnp.concatenate(
                [vbuf[rows(b, t, rho), pl.ds(pl.multiple_of(c * HALF, HALF), HALF)] for rho in range(2)], axis=0)
            gacc[...] += _dot(own, v_tile(b, t), 0, 0)

        gacc[...] = jnp.zeros((HALF, TILE), jnp.float32)
        _pairs(b // 4, NT - b // 4, tile)

        def cols_of(par):
            return gacc[:, pl.ds(pl.multiple_of(par * HALF, HALF), HALF)]

        usend[b % 2] = jnp.where(ra <= rb, cols_of(1 - c), cols_of(c))
        u_copy(b).start()

    def u_half(b):
        u_copy(b).wait()
        total = usend[b % 2] + urecv[b % 4]

        @pl.when(b % 2 == c)
        def _():
            upack[c] = total

        @pl.when(b % 2 != c)
        def _():
            @pl.when(b < NB - 2)
            def _():
                half_copy.wait_send()

            uhalf[...] = total
            half_copy.start()

    def merge(b):
        half_copy.wait_recv()
        slot = b % 4

        @pl.when(b < NB - 2)
        def _():
            t_copy(b).wait_send()

        same = ra == rb

        def diagonal(par):
            at = [pl.multiple_of((8 * b + 2 * i + par) * PITCH, 8) for i in range(4)]
            stack = jnp.concatenate([tt[pl.ds(row, W), :] for row in at], axis=0)
            return jnp.where(same, jnp.concatenate([stack] * 4, axis=1), 0.0).T

        lo, hi = slice(0, HALF // 2), slice(HALF // 2, HALF)
        even_part, odd_part = upack[0], upack[1]
        ee, oo = jnp.where(ra > rb, even_part, 0.0), jnp.where(ra > rb, odd_part, 0.0)
        oe, eo = jnp.where(ra <= rb, even_part, 0.0).T, jnp.where(ra < rb, odd_part, 0.0).T

        def quad(a, b_, c_, d, rows_, cols_):
            return jnp.concatenate([
                jnp.concatenate([a[rows_, cols_], b_[rows_, cols_]], axis=1),
                jnp.concatenate([c_[rows_, cols_], d[rows_, cols_]], axis=1)], axis=0)

        even, odd = diagonal(0), diagonal(1)
        cross = -_dot(_dot(odd, jnp.where(same, oe, 0.0), 1, 0), even, 1, 0)
        zero = jnp.zeros((HALF, HALF), jnp.float32)
        pa, pb = ra % 2, rb % 2
        t_diag = []
        for part in (lo, hi):
            t_now = quad(even, zero, cross, odd, part, part)
            u_now = jnp.where(pa > pb, quad(ee, eo, oe, oo, part, part), 0.0)
            t_diag.append(t_now - _dot(_dot(t_now, u_now, 1, 0), t_now, 1, 0))
        t_lo, t_hi = t_diag
        t_off = -_dot(_dot(t_hi, quad(ee, eo, oe, oo, hi, lo), 1, 0), t_lo, 1, 0)
        half0 = jnp.zeros((HALF // 2, HALF // 2), jnp.float32)
        for rows_, out_rows in ((lo, 0), (hi, HALF)):
            tbuf[slot, out_rows : out_rows + HALF // 2, :] = jnp.concatenate(
                [t_lo[rows_, lo], half0, t_lo[rows_, hi], half0], axis=1)
            tbuf[slot, out_rows + HALF // 2 : out_rows + HALF, :] = jnp.concatenate(
                [t_off[rows_, lo], t_hi[rows_, lo], t_off[rows_, hi], t_hi[rows_, hi]], axis=1)
        t_copy(b).start()

    def t_layout():
        t_copy_in.wait()

        def t_row(i, carry):
            tt[pl.ds(i, NB * 8, stride=PITCH), :] = t_raw[i].T
            return carry

        lax.fori_loop(0, W, t_row, 0)

    def z_send(n):
        z_chunk((19 - n) // 4, n % 4, x).start()

    def step(s, carry):
        k = NB + 1 - s
        b_sweep = jnp.where(k == NB, NB - 1, k)
        sweeps = (k < NB - 1) | (k == NB)
        b_in, takes_in = jnp.where(k >= 4, k - 2, k - 1), (k >= 1) & (k != 3)
        b_merge, merges = jnp.where(k >= 3, k - 1, k), (k <= NB) & (k != 2)

        @pl.when(sweeps)
        def _():
            @pl.when(b_sweep % 4 == 3)
            def _():
                for j in range(4):
                    z_chunk(b_sweep // 4, j, 1 - x).wait_recv()
                for rho in range(2):
                    z_own(b_sweep // 4, rho).wait()
                for g in range(2):
                    zt[g, :, cols(b_sweep // 4)] = zst[g, b_sweep // 4].T

            sweep(0, b_sweep)

        @pl.when(takes_in)
        def _():
            def forward(b):
                v_y(b, 1 - y).wait_recv()
                v_fwd(b, c).start()

            static_block(b_in, forward)

        @pl.when(merges & (b_merge % 2 != c))
        def _():
            u_half(b_merge)

        @pl.when(sweeps)
        def _():
            sweep(1, b_sweep)

        @pl.when((k >= AHEAD) & (k < NB))
        def _():
            static_block(k - AHEAD, v_issue)

        @pl.when(takes_in)
        def _():
            def arrived(b):
                v_own(b, 1 - c).wait_recv()
                v_fwd(b, 1 - c).wait_recv()

            static_block(b_in, arrived)
            gram(b_in)

        @pl.when(k >= 18)
        def _():
            z_send(25 - k)

        @pl.when((k == 14) | (k == 15))
        def _():
            z_send(8 + 2 * (15 - k))
            z_send(9 + 2 * (15 - k))

        @pl.when((k <= 12) & (k >= 5))
        def _():
            z_send(24 - k)

        @pl.when(k == NB + 1)
        def _():
            t_layout()

        @pl.when(merges & (b_merge % 2 == c))
        def _():
            u_half(b_merge)
            merge(b_merge)

        return carry

    lax.fori_loop(0, NB + 2, step, 0)

    def out_part(g, t, core):
        return out.at[pl.ds(t * TILE, TILE), pl.ds(pl.multiple_of((2 * g + core) * HALF, HALF), HALF)]

    def z_part(g, t, rho):
        return zst.at[g, t, pl.ds(pl.multiple_of(rho * TILE, TILE), TILE), :]

    def out_local(g, t):
        return pltpu.make_async_copy(z_part(g, t, c), out_part(g, t, c), out_sem.at[g * NT + t])

    def out_sib(g, t):
        return remote(z_part(g, t, 1 - c), out_part(g, t, c), outs_sem.at[g * NT + t], outr_sem.at[g * NT + t], sib)

    def out_from_sib(g, t):
        part = out_part(g, t, 1 - c)
        return remote(part, part, outs_sem.at[g * NT + t], outr_sem.at[g * NT + t], sib)

    for g in range(2):
        weights(g, 0)

        def last(t, g=g):
            update(g, 0, t)
            zst[g, t] = zt[g, :, cols(t)].T

        _pairs(0, NT, last)
        for t in range(NT):
            out_local(g, t).start()
            out_sib(g, t).start()

    half_copy.wait_send()
    t_copy(0).wait_send()
    for b in range(NB):
        v_y(b, y).wait_send()
        v_own(b, c).wait_send()
        v_fwd(b, c).wait_send()
        z_chunk(b // 4, b % 4, x).wait_send()
    for g in range(2):
        for t in range(NT):
            out_local(g, t).wait()
            out_sib(g, t).wait_send()
            out_from_sib(g, t).wait_recv()


def solution(mesh):
    def local_run(z_cols, v_local, t_local):
        f32 = jnp.float32
        any_spec = pl.BlockSpec(memory_space=pl.ANY)
        dma = pltpu.SemaphoreType.DMA
        return pl.pallas_call(
            _kernel,
            out_shape=jax.ShapeDtypeStruct((ROWS, 4 * HALF), f32),
            in_specs=[any_spec] * 3,
            out_specs=any_spec,
            scratch_shapes=[
                pltpu.VMEM((2 * VT * TILE, TILE), f32),
                pltpu.VMEM((TILE, 2 * ROWS), f32),
                pltpu.VMEM((2, HALF, 2 * ROWS), f32),
                pltpu.VMEM((2, NT, 2 * TILE, HALF), f32),
                pltpu.VMEM((W, W, NB * 8), f32),
                pltpu.VMEM((NB * 8 * PITCH, W), f32),
                pltpu.VMEM((2, HALF, TILE), f32),
                pltpu.VMEM((2, 2, HALF, TILE), f32),
                pltpu.VMEM((HALF, TILE), f32),
                pltpu.VMEM((HALF, TILE), f32),
                pltpu.VMEM((2, HALF, HALF), f32),
                pltpu.VMEM((4, HALF, HALF), f32),
                pltpu.VMEM((HALF, HALF), f32),
                pltpu.VMEM((2, HALF, HALF), f32),
                pltpu.VMEM((4, TILE, TILE), f32),
                *[dma((NB,))] * 9,
                dma((2,)), dma((2, 2)), dma((2,)), dma((4,)), dma, dma, dma, dma((4,)), dma, *[dma((2 * NT,))] * 4,
            ],
            compiler_params=pltpu.CompilerParams(collective_id=0, has_side_effects=True, vmem_limit_bytes=63 * 2**20),
            name="backtransform",
        )(z_cols, v_local, t_local.transpose(1, 2, 0))

    return jax.shard_map(
        local_run,
        mesh=mesh,
        in_specs=(P("kpt", ("col", "row")), P(("kpt", "row"), "col"), P("kpt", None, None)),
        out_specs=P(("kpt", "row"), "col"),
        check_vma=False,
    )
```

```python
import jax
import jax.numpy as jnp
from jax import lax
from jax.experimental import pallas as pl
from jax.experimental.pallas import tpu as pltpu
from jax.sharding import PartitionSpec as P

PRECISE = lax.Precision.HIGHEST
MESH = pl.DeviceIdType.MESH

W = 32
ROWS = 1536
TILE = 256
HALF = 128
NT = ROWS // TILE
NB = 24
VT = 4 * sum(range(1, NT + 1))
PITCH = 40
AHEAD = 12


def _dot(a, b, ca, cb):
    return lax.dot_general(a, b, (((ca,), (cb,)), ((), ())), precision=PRECISE, preferred_element_type=jnp.float32)


def _base(b):
    q, i = b // 4, b % 4
    return 4 * (NT * q - (q * (q - 1)) // 2) + i * (NT - q)


def _panel(idx):
    return jnp.where(idx < HALF, 2 * (idx // W), 2 * ((idx - HALF) // W) + 1)


def _tiles(lo, n, body):
    def three(h, carry):
        for u in range(3):
            body(lo + 3 * h + u)
        return carry

    lax.fori_loop(0, n // 3, three, 0)

    @pl.when(n % 3 == 2)
    def _():
        body(lo + n - 2)
        body(lo + n - 1)

    @pl.when(n % 3 == 1)
    def _():
        body(lo + n - 1)


def _kernel(z_in, v_in, t_in, out, vbuf, vtr, zt, zst, t_raw, tt, acc, srecv, wbuf, gacc, usend, urecv, uhalf, upack, tbuf,
            loc_sem, ys_sem, yr_sem, os_sem, or_sem, fs_sem, fr_sem, zs_sem, zr_sem,
            ss_sem, sr_sem, us_sem, ur_sem, hs_sem, hr_sem, ts_sem, tr_sem, tt_sem, zo_sem, out_sem, outs_sem, outr_sem):
    ridx = lax.axis_index("row")
    y = lax.axis_index("col")
    x, c = ridx // 2, ridx % 2
    xn = {"row": (ridx + 2) % 4}
    sib = {"row": ridx + 1 - 2 * c}
    yn = {"col": 1 - y}

    barrier = pltpu.get_barrier_semaphore()
    for dev in (xn, sib, yn):
        pl.semaphore_signal(barrier, inc=1, device_id=dev, device_id_type=MESH)

    def remote(src, dst, send, recv, dev):
        return pltpu.make_async_remote_copy(src, dst, send, recv, device_id=dev, device_id_type=MESH)

    def slab(b, rho, par):
        start = (rho * VT + _base(b)) * TILE + 64 * (b % 4)
        return vbuf.at[pl.ds(pl.multiple_of(start, 64), ROWS - 64 * b), pl.ds(pl.multiple_of(par * HALF, HALF), HALF)]

    def v_local(b):
        return pltpu.make_async_copy(v_in.at[pl.ds(64 * b, ROWS - 64 * b), pl.ds(HALF * b, HALF)], slab(b, c, y), loc_sem.at[b])

    def v_y(b, par):
        return remote(slab(b, c, par), slab(b, c, par), ys_sem.at[b], yr_sem.at[b], yn)

    def v_own(b, rho):
        return remote(slab(b, rho, y), slab(b, rho, y), os_sem.at[b], or_sem.at[b], sib)

    def v_fwd(b, rho):
        return remote(slab(b, rho, 1 - y), slab(b, rho, 1 - y), fs_sem.at[b], fr_sem.at[b], sib)

    def v_issue(b):
        v_local(b).wait()
        v_y(b, y).start()
        v_own(b, c).start()

    def static_block(b, fn):
        for qq in range(NT):

            @pl.when(b // 4 == qq)
            def _(qq=qq):
                for ii in range(4):

                    @pl.when(b % 4 == ii)
                    def _(ii=ii):
                        fn(4 * qq + ii)

    def z_own(t, rho):
        return pltpu.make_async_copy(
            z_in.at[pl.ds(pl.multiple_of((2 * x + rho) * ROWS + t * TILE, TILE), TILE), :],
            zst.at[x, t, pl.ds(rho * TILE, TILE), :], zo_sem.at[2 * t + rho])

    def z_chunk(t, j, g):
        src = (2 * (1 - x) + j // 2) * ROWS + t * TILE + (j % 2) * HALF
        return remote(
            z_in.at[pl.ds(pl.multiple_of(src, HALF), HALF), :],
            zst.at[g, t, pl.ds(pl.multiple_of(j * HALF, HALF), HALF), :],
            zs_sem.at[4 * t + j], zr_sem.at[4 * t + j], xn)

    t_copy_in = pltpu.make_async_copy(t_in, t_raw, tt_sem)

    for b in range(NB - 1, NB - 5, -1):
        v_local(b).start()
    t_copy_in.start()
    for t in range(NT - 1, -1, -1):
        for rho in range(2):
            z_own(t, rho).start()
    for b in range(NB - 5, -1, -1):
        v_local(b).start()
    for b in range(NB):
        if b % 4:
            for rho in range(2):
                vbuf[pl.ds((rho * VT + _base(b)) * TILE, 64 * (b % 4)), :] = jnp.zeros((64 * (b % 4), TILE), jnp.float32)

    pl.semaphore_wait(barrier, 3)
    for b in range(NB - 1, NB - 1 - AHEAD, -1):
        v_issue(b)
        if b == NB - 2:
            for j in range(4):
                z_chunk(NT - 1, j, x).start()

    def rows(b, t, rho):
        return pl.ds(pl.multiple_of((rho * VT + _base(b) + t - b // 4) * TILE, TILE), TILE)

    def v_tile(b, t):
        return jnp.concatenate([vbuf[rows(b, t, rho), :] for rho in range(2)], axis=0)

    def cols(t):
        return pl.ds(pl.multiple_of(t * 2 * TILE, 2 * TILE), 2 * TILE)

    def s_copy(g, b):
        return remote(acc.at[g], srecv.at[g, b % 2], ss_sem.at[g], sr_sem.at[g, b % 2], xn)

    def weights(g, b):
        if g == 0:

            @pl.when(b % 2 != c)
            def _():
                t_copy(b).wait_recv()

        s_copy(g, b).wait_recv()
        s_sum = acc[g] + srecv[g, b % 2]
        wbuf[...] = _dot(s_sum, tbuf[b % 4], 1, 0)
        s_copy(g, b).wait_send()

    def update(g, b, t):
        if g == 0:
            v_tr = v_tile(b, t).T
            vtr[:, cols(t)] = v_tr
        else:
            v_tr = vtr[:, cols(t)]
        zt[g, :, cols(t)] = zt[g, :, cols(t)] - _dot(wbuf[...], v_tr, 1, 0)

    def partial_s(g, b, t):
        acc[g] += _dot(zt[g, :, cols(t)], v_tile(b, t), 1, 0)

    def sweep(g, k):
        @pl.when(k < NB - 1)
        def _():
            weights(g, k + 1)

        acc[g] = jnp.zeros((HALF, TILE), jnp.float32)
        first = (k + 1) // 4
        late = jnp.where(k % 4 == 3, 0, 1)

        @pl.when(late == 1)
        def _():
            update(g, k + 1, first)

        def both(t):
            partial_s(g, k, t - 1)
            update(g, k + 1, t)

        _tiles(first + late, NT - first - late, both)
        partial_s(g, k, NT - 1)
        s_copy(g, k).start()

    ra = lax.broadcasted_iota(jnp.int32, (HALF, HALF), 0) // W
    rb = lax.broadcasted_iota(jnp.int32, (HALF, HALF), 1) // W

    def u_copy(b):
        return remote(usend.at[b % 2], urecv.at[b % 4], us_sem.at[b % 2], ur_sem.at[b % 4], xn)

    half_copy = remote(uhalf, upack.at[c], hs_sem, hr_sem, sib)

    def t_copy(b):
        return remote(tbuf.at[b % 4], tbuf.at[b % 4], ts_sem, tr_sem.at[b % 4], sib)

    def gram(b):
        def tile(t):
            own = jnp.concatenate(
                [vbuf[rows(b, t, rho), pl.ds(pl.multiple_of(c * HALF, HALF), HALF)] for rho in range(2)], axis=0)
            gacc[...] += _dot(own, v_tile(b, t), 0, 0)

        gacc[...] = jnp.zeros((HALF, TILE), jnp.float32)
        _tiles(b // 4, NT - b // 4, tile)

        def cols_of(par):
            return gacc[:, pl.ds(pl.multiple_of(par * HALF, HALF), HALF)]

        usend[b % 2] = jnp.where(ra <= rb, cols_of(1 - c), cols_of(c))
        u_copy(b).start()

    def u_half(b):
        u_copy(b).wait()
        total = usend[b % 2] + urecv[b % 4]

        @pl.when(b % 2 == c)
        def _():
            upack[c] = total

        @pl.when(b % 2 != c)
        def _():
            @pl.when(b < NB - 2)
            def _():
                half_copy.wait_send()

            uhalf[...] = total
            half_copy.start()

    def merge(b):
        half_copy.wait_recv()
        slot = b % 4

        @pl.when(b < NB - 2)
        def _():
            t_copy(b).wait_send()

        same = ra == rb

        def diagonal(par):
            at = [pl.multiple_of((8 * b + 2 * i + par) * PITCH, 8) for i in range(4)]
            stack = jnp.concatenate([tt[pl.ds(row, W), :] for row in at], axis=0)
            return jnp.where(same, jnp.concatenate([stack] * 4, axis=1), 0.0).T

        lo, hi = slice(0, HALF // 2), slice(HALF // 2, HALF)
        even_part, odd_part = upack[0], upack[1]
        ee, oo = jnp.where(ra > rb, even_part, 0.0), jnp.where(ra > rb, odd_part, 0.0)
        oe, eo = jnp.where(ra <= rb, even_part, 0.0).T, jnp.where(ra < rb, odd_part, 0.0).T

        def quad(a, b_, c_, d, rows_, cols_):
            return jnp.concatenate([
                jnp.concatenate([a[rows_, cols_], b_[rows_, cols_]], axis=1),
                jnp.concatenate([c_[rows_, cols_], d[rows_, cols_]], axis=1)], axis=0)

        even, odd = diagonal(0), diagonal(1)
        cross = -_dot(_dot(odd, jnp.where(same, oe, 0.0), 1, 0), even, 1, 0)
        zero = jnp.zeros((HALF, HALF), jnp.float32)
        pa, pb = ra % 2, rb % 2
        t_diag = []
        for part in (lo, hi):
            t_now = quad(even, zero, cross, odd, part, part)
            u_now = jnp.where(pa > pb, quad(ee, eo, oe, oo, part, part), 0.0)
            t_diag.append(t_now - _dot(_dot(t_now, u_now, 1, 0), t_now, 1, 0))
        t_lo, t_hi = t_diag
        t_off = -_dot(_dot(t_hi, quad(ee, eo, oe, oo, hi, lo), 1, 0), t_lo, 1, 0)
        half0 = jnp.zeros((HALF // 2, HALF // 2), jnp.float32)
        for rows_, out_rows in ((lo, 0), (hi, HALF)):
            tbuf[slot, out_rows : out_rows + HALF // 2, :] = jnp.concatenate(
                [t_lo[rows_, lo], half0, t_lo[rows_, hi], half0], axis=1)
            tbuf[slot, out_rows + HALF // 2 : out_rows + HALF, :] = jnp.concatenate(
                [t_off[rows_, lo], t_hi[rows_, lo], t_off[rows_, hi], t_hi[rows_, hi]], axis=1)
        t_copy(b).start()

    def t_layout():
        t_copy_in.wait()

        def t_row(i, carry):
            tt[pl.ds(i, NB * 8, stride=PITCH), :] = t_raw[i].T
            return carry

        lax.fori_loop(0, W, t_row, 0)

    def z_send(n):
        z_chunk((19 - n) // 4, n % 4, x).start()

    def step(s, carry):
        k = NB + 1 - s
        b_sweep = jnp.where(k == NB, NB - 1, k)
        sweeps = (k < NB - 1) | (k == NB)
        b_in, takes_in = jnp.where(k >= 4, k - 2, k - 1), (k >= 1) & (k != 3)
        b_merge, merges = jnp.where(k >= 3, k - 1, k), (k <= NB) & (k != 2)

        @pl.when(sweeps)
        def _():
            @pl.when(b_sweep % 4 == 3)
            def _():
                for j in range(4):
                    z_chunk(b_sweep // 4, j, 1 - x).wait_recv()
                for rho in range(2):
                    z_own(b_sweep // 4, rho).wait()
                for g in range(2):
                    zt[g, :, cols(b_sweep // 4)] = zst[g, b_sweep // 4].T

            sweep(0, b_sweep)

        @pl.when(takes_in)
        def _():
            def forward(b):
                v_y(b, 1 - y).wait_recv()
                v_fwd(b, c).start()

            static_block(b_in, forward)

        @pl.when(merges & (b_merge % 2 != c))
        def _():
            u_half(b_merge)

        @pl.when((k == 1) & (c == 1))
        def _():
            u_half(1)
            merge(1)

        @pl.when(sweeps)
        def _():
            sweep(1, b_sweep)

        @pl.when((k >= AHEAD) & (k < NB))
        def _():
            static_block(k - AHEAD, v_issue)

        @pl.when(takes_in)
        def _():
            def arrived(b):
                v_own(b, 1 - c).wait_recv()
                v_fwd(b, 1 - c).wait_recv()

            static_block(b_in, arrived)
            gram(b_in)

        @pl.when(k >= 18)
        def _():
            z_send(25 - k)

        @pl.when((k == 14) | (k == 15))
        def _():
            z_send(8 + 2 * (15 - k))
            z_send(9 + 2 * (15 - k))

        @pl.when((k <= 12) & (k >= 5))
        def _():
            z_send(24 - k)

        @pl.when(k == NB + 1)
        def _():
            t_layout()

        @pl.when(merges & (k != 1) & (b_merge % 2 == c))
        def _():
            u_half(b_merge)
            merge(b_merge)

        return carry

    lax.fori_loop(0, NB + 2, step, 0)

    def out_part(g, t, core):
        return out.at[pl.ds(t * TILE, TILE), pl.ds(pl.multiple_of((2 * g + core) * HALF, HALF), HALF)]

    def z_part(g, t, rho):
        return zst.at[g, t, pl.ds(pl.multiple_of(rho * TILE, TILE), TILE), :]

    def out_local(g, t):
        return pltpu.make_async_copy(z_part(g, t, c), out_part(g, t, c), out_sem.at[g * NT + t])

    def out_sib(g, t):
        return remote(z_part(g, t, 1 - c), out_part(g, t, c), outs_sem.at[g * NT + t], outr_sem.at[g * NT + t], sib)

    def out_from_sib(g, t):
        part = out_part(g, t, 1 - c)
        return remote(part, part, outs_sem.at[g * NT + t], outr_sem.at[g * NT + t], sib)

    for g in range(2):
        weights(g, 0)

        def last(t, g=g):
            update(g, 0, t)
            zst[g, t] = zt[g, :, cols(t)].T

        _tiles(0, NT, last)
        for t in range(NT):
            out_local(g, t).start()
            out_sib(g, t).start()

    half_copy.wait_send()
    t_copy(0).wait_send()
    for b in range(NB):
        v_y(b, y).wait_send()
        v_own(b, c).wait_send()
        v_fwd(b, c).wait_send()
        z_chunk(b // 4, b % 4, x).wait_send()
    for g in range(2):
        for t in range(NT):
            out_local(g, t).wait()
            out_sib(g, t).wait_send()
            out_from_sib(g, t).wait_recv()


def solution(mesh):
    def local_run(z_cols, v_local, t_local):
        f32 = jnp.float32
        any_spec = pl.BlockSpec(memory_space=pl.ANY)
        dma = pltpu.SemaphoreType.DMA
        return pl.pallas_call(
            _kernel,
            out_shape=jax.ShapeDtypeStruct((ROWS, 4 * HALF), f32),
            in_specs=[any_spec] * 3,
            out_specs=any_spec,
            scratch_shapes=[
                pltpu.VMEM((2 * VT * TILE, TILE), f32),
                pltpu.VMEM((TILE, 2 * ROWS), f32),
                pltpu.VMEM((2, HALF, 2 * ROWS), f32),
                pltpu.VMEM((2, NT, 2 * TILE, HALF), f32),
                pltpu.VMEM((W, W, NB * 8), f32),
                pltpu.VMEM((NB * 8 * PITCH, W), f32),
                pltpu.VMEM((2, HALF, TILE), f32),
                pltpu.VMEM((2, 2, HALF, TILE), f32),
                pltpu.VMEM((HALF, TILE), f32),
                pltpu.VMEM((HALF, TILE), f32),
                pltpu.VMEM((2, HALF, HALF), f32),
                pltpu.VMEM((4, HALF, HALF), f32),
                pltpu.VMEM((HALF, HALF), f32),
                pltpu.VMEM((2, HALF, HALF), f32),
                pltpu.VMEM((4, TILE, TILE), f32),
                *[dma((NB,))] * 9,
                dma((2,)), dma((2, 2)), dma((2,)), dma((4,)), dma, dma, dma, dma((4,)), dma, *[dma((2 * NT,))] * 4,
            ],
            compiler_params=pltpu.CompilerParams(collective_id=0, has_side_effects=True, vmem_limit_bytes=63 * 2**20),
            name="backtransform",
        )(z_cols, v_local, t_local.transpose(1, 2, 0))

    return jax.shard_map(
        local_run,
        mesh=mesh,
        in_specs=(P("kpt", ("col", "row")), P(("kpt", "row"), "col"), P("kpt", None, None)),
        out_specs=P(("kpt", "row"), "col"),
        check_vma=False,
    )
```

```python
import jax
import jax.numpy as jnp
from jax import lax
from jax.experimental import pallas as pl
from jax.experimental.pallas import tpu as pltpu
from jax.sharding import PartitionSpec as P

PRECISE = lax.Precision.HIGHEST
MESH = pl.DeviceIdType.MESH

W = 32
ROWS = 1536
TILE = 256
HALF = 128
NT = ROWS // TILE
NU = ROWS // HALF
NB = 24
VU = 2 * sum(range(1, NU + 1))
PITCH = 40
AHEAD = 12


def _dot(a, b, ca, cb):
    return lax.dot_general(a, b, (((ca,), (cb,)), ((), ())), precision=PRECISE, preferred_element_type=jnp.float32)


def _base(b):
    p = b // 2
    return 2 * NU * p - p * (p - 1) + (b % 2) * (NU - p)


def _panel(idx):
    return jnp.where(idx < HALF, 2 * (idx // W), 2 * ((idx - HALF) // W) + 1)


def _units(lo, n, body):
    def six(h, carry):
        for u in range(6):
            body(lo + 6 * h + u)
        return carry

    lax.fori_loop(0, n // 6, six, 0)
    rest = n % 6
    for size, here, start in ((4, rest >= 4, lo + n - rest), (2, (rest // 2) % 2 == 1, lo + n - rest % 4), (1, rest % 2 == 1, lo + n - 1)):

        @pl.when(here)
        def _(size=size, start=start):
            for u in range(size):
                body(start + u)


def _kernel(z_in, v_in, t_in, out, vbuf, vtr, zt, zst, t_raw, tt, acc, srecv, wbuf, gacc, usend, urecv, uhalf, upack, tbuf,
            loc_sem, ys_sem, yr_sem, os_sem, or_sem, fs_sem, fr_sem, zs_sem, zr_sem,
            ss_sem, sr_sem, us_sem, ur_sem, hs_sem, hr_sem, ts_sem, tr_sem, tt_sem, zo_sem, out_sem, outs_sem, outr_sem):
    ridx = lax.axis_index("row")
    y = lax.axis_index("col")
    x, c = ridx // 2, ridx % 2
    xn = {"row": (ridx + 2) % 4}
    sib = {"row": ridx + 1 - 2 * c}
    yn = {"col": 1 - y}

    barrier = pltpu.get_barrier_semaphore()
    for dev in (xn, sib, yn):
        pl.semaphore_signal(barrier, inc=1, device_id=dev, device_id_type=MESH)

    def remote(src, dst, send, recv, dev):
        return pltpu.make_async_remote_copy(src, dst, send, recv, device_id=dev, device_id_type=MESH)

    def slab(b, rho, par):
        start = (rho * VU + _base(b)) * HALF + 64 * (b % 2)
        return vbuf.at[pl.ds(pl.multiple_of(start, 64), ROWS - 64 * b), pl.ds(pl.multiple_of(par * HALF, HALF), HALF)]

    def v_local(b):
        return pltpu.make_async_copy(v_in.at[pl.ds(64 * b, ROWS - 64 * b), pl.ds(HALF * b, HALF)], slab(b, c, y), loc_sem.at[b])

    def v_y(b, par):
        return remote(slab(b, c, par), slab(b, c, par), ys_sem.at[b], yr_sem.at[b], yn)

    def v_own(b, rho):
        return remote(slab(b, rho, y), slab(b, rho, y), os_sem.at[b], or_sem.at[b], sib)

    def v_fwd(b, rho):
        return remote(slab(b, rho, 1 - y), slab(b, rho, 1 - y), fs_sem.at[b], fr_sem.at[b], sib)

    def v_issue(b):
        v_local(b).wait()
        v_y(b, y).start()
        v_own(b, c).start()

    def static_block(b, fn):
        for qq in range(NT):

            @pl.when(b // 4 == qq)
            def _(qq=qq):
                for ii in range(4):

                    @pl.when(b % 4 == ii)
                    def _(ii=ii):
                        fn(4 * qq + ii)

    def z_own(u, rho):
        return pltpu.make_async_copy(
            z_in.at[pl.ds(pl.multiple_of((2 * x + rho) * ROWS + u * HALF, HALF), HALF), :],
            zst.at[x, u, pl.ds(rho * HALF, HALF), :], zo_sem.at[2 * u + rho])

    def z_chunk(t, j, g):
        src = (2 * (1 - x) + j // 2) * ROWS + t * TILE + (j % 2) * HALF
        return remote(
            z_in.at[pl.ds(pl.multiple_of(src, HALF), HALF), :],
            zst.at[g, 2 * t + j % 2, pl.ds(pl.multiple_of((j // 2) * HALF, HALF), HALF), :],
            zs_sem.at[4 * t + j], zr_sem.at[4 * t + j], xn)

    t_copy_in = pltpu.make_async_copy(t_in, t_raw, tt_sem)

    for b in range(NB - 1, NB - 5, -1):
        v_local(b).start()
    t_copy_in.start()
    for u in range(NU - 1, -1, -1):
        for rho in range(2):
            z_own(u, rho).start()
    for b in range(NB - 5, -1, -1):
        v_local(b).start()
    for b in range(NB):
        if b % 2:
            for rho in range(2):
                vbuf[pl.ds((rho * VU + _base(b)) * HALF, 64), :] = jnp.zeros((64, TILE), jnp.float32)

    pl.semaphore_wait(barrier, 3)
    for b in range(NB - 1, NB - 1 - AHEAD, -1):
        v_issue(b)
        if b == NB - 2:
            for j in range(4):
                z_chunk(NT - 1, j, x).start()

    def rows(b, u, rho):
        return pl.ds(pl.multiple_of((rho * VU + _base(b) + u - b // 2) * HALF, HALF), HALF)

    def v_unit(b, u):
        return jnp.concatenate([vbuf[rows(b, u, rho), :] for rho in range(2)], axis=0)

    def cols(u):
        return pl.ds(pl.multiple_of(u * TILE, TILE), TILE)

    def s_copy(g, b):
        return remote(acc.at[g], srecv.at[g, b % 2], ss_sem.at[g], sr_sem.at[g, b % 2], xn)

    def weights(g, b):
        if g == 0:

            @pl.when(b % 2 != c)
            def _():
                t_copy(b).wait_recv()

        s_copy(g, b).wait_recv()
        s_sum = acc[g] + srecv[g, b % 2]
        wbuf[...] = _dot(s_sum, tbuf[b % 4], 1, 0)
        s_copy(g, b).wait_send()

    def update(g, b, u):
        if g == 0:
            v_tr = v_unit(b, u).T
            vtr[:, cols(u)] = v_tr
        else:
            v_tr = vtr[:, cols(u)]
        zt[g, :, cols(u)] = zt[g, :, cols(u)] - _dot(wbuf[...], v_tr, 1, 0)

    def partial_s(g, b, u):
        acc[g] += _dot(zt[g, :, cols(u)], v_unit(b, u), 1, 0)

    def sweep(g, k):
        @pl.when(k < NB - 1)
        def _():
            weights(g, k + 1)

        acc[g] = jnp.zeros((HALF, TILE), jnp.float32)
        first = (k + 1) // 2
        late = 1 - k % 2

        @pl.when(late == 1)
        def _():
            update(g, k + 1, first)

        def both(u):
            partial_s(g, k, u - 1)
            update(g, k + 1, u)

        _units(first + late, NU - first - late, both)
        partial_s(g, k, NU - 1)
        s_copy(g, k).start()

    ra = lax.broadcasted_iota(jnp.int32, (HALF, HALF), 0) // W
    rb = lax.broadcasted_iota(jnp.int32, (HALF, HALF), 1) // W

    def u_copy(b):
        return remote(usend.at[b % 2], urecv.at[b % 4], us_sem.at[b % 2], ur_sem.at[b % 4], xn)

    half_copy = remote(uhalf, upack.at[c], hs_sem, hr_sem, sib)

    def t_copy(b):
        return remote(tbuf.at[b % 4], tbuf.at[b % 4], ts_sem, tr_sem.at[b % 4], sib)

    def gram(b):
        def unit(u):
            own = jnp.concatenate(
                [vbuf[rows(b, u, rho), pl.ds(pl.multiple_of(c * HALF, HALF), HALF)] for rho in range(2)], axis=0)
            gacc[...] += _dot(own, v_unit(b, u), 0, 0)

        gacc[...] = jnp.zeros((HALF, TILE), jnp.float32)
        _units(b // 2, NU - b // 2, unit)

        def cols_of(par):
            return gacc[:, pl.ds(pl.multiple_of(par * HALF, HALF), HALF)]

        usend[b % 2] = jnp.where(ra <= rb, cols_of(1 - c), cols_of(c))
        u_copy(b).start()

    def u_half(b):
        u_copy(b).wait()
        total = usend[b % 2] + urecv[b % 4]

        @pl.when(b % 2 == c)
        def _():
            upack[c] = total

        @pl.when(b % 2 != c)
        def _():
            @pl.when(b < NB - 2)
            def _():
                half_copy.wait_send()

            uhalf[...] = total
            half_copy.start()

    def merge(b):
        half_copy.wait_recv()
        slot = b % 4

        @pl.when(b < NB - 2)
        def _():
            t_copy(b).wait_send()

        same = ra == rb

        def diagonal(par):
            at = [pl.multiple_of((8 * b + 2 * i + par) * PITCH, 8) for i in range(4)]
            stack = jnp.concatenate([tt[pl.ds(row, W), :] for row in at], axis=0)
            return jnp.where(same, jnp.concatenate([stack] * 4, axis=1), 0.0).T

        lo, hi = slice(0, HALF // 2), slice(HALF // 2, HALF)
        even_part, odd_part = upack[0], upack[1]
        ee, oo = jnp.where(ra > rb, even_part, 0.0), jnp.where(ra > rb, odd_part, 0.0)
        oe, eo = jnp.where(ra <= rb, even_part, 0.0).T, jnp.where(ra < rb, odd_part, 0.0).T

        def quad(a, b_, c_, d, rows_, cols_):
            return jnp.concatenate([
                jnp.concatenate([a[rows_, cols_], b_[rows_, cols_]], axis=1),
                jnp.concatenate([c_[rows_, cols_], d[rows_, cols_]], axis=1)], axis=0)

        even, odd = diagonal(0), diagonal(1)
        cross = -_dot(_dot(odd, jnp.where(same, oe, 0.0), 1, 0), even, 1, 0)
        zero = jnp.zeros((HALF, HALF), jnp.float32)
        pa, pb = ra % 2, rb % 2
        t_diag = []
        for part in (lo, hi):
            t_now = quad(even, zero, cross, odd, part, part)
            u_now = jnp.where(pa > pb, quad(ee, eo, oe, oo, part, part), 0.0)
            t_diag.append(t_now - _dot(_dot(t_now, u_now, 1, 0), t_now, 1, 0))
        t_lo, t_hi = t_diag
        t_off = -_dot(_dot(t_hi, quad(ee, eo, oe, oo, hi, lo), 1, 0), t_lo, 1, 0)
        half0 = jnp.zeros((HALF // 2, HALF // 2), jnp.float32)
        for rows_, out_rows in ((lo, 0), (hi, HALF)):
            tbuf[slot, out_rows : out_rows + HALF // 2, :] = jnp.concatenate(
                [t_lo[rows_, lo], half0, t_lo[rows_, hi], half0], axis=1)
            tbuf[slot, out_rows + HALF // 2 : out_rows + HALF, :] = jnp.concatenate(
                [t_off[rows_, lo], t_hi[rows_, lo], t_off[rows_, hi], t_hi[rows_, hi]], axis=1)
        t_copy(b).start()

    def t_layout():
        t_copy_in.wait()

        def t_row(i, carry):
            tt[pl.ds(i, NB * 8, stride=PITCH), :] = t_raw[i].T
            return carry

        lax.fori_loop(0, W, t_row, 0)

    def z_send(n):
        z_chunk((19 - n) // 4, n % 4, x).start()

    def step(s, carry):
        k = NB + 1 - s
        b_sweep = jnp.where(k == NB, NB - 1, k)
        sweeps = (k < NB - 1) | (k == NB)
        b_in, takes_in = jnp.where(k >= 4, k - 2, k - 1), (k >= 1) & (k != 3)
        b_merge, merges = jnp.where(k >= 3, k - 1, k), (k <= NB) & (k != 2)

        @pl.when(sweeps)
        def _():
            @pl.when(b_sweep % 4 == 3)
            def _():
                for j in range(4):
                    z_chunk(b_sweep // 4, j, 1 - x).wait_recv()
                for h in range(2):
                    u = 2 * (b_sweep // 4) + h
                    for rho in range(2):
                        z_own(u, rho).wait()
                    for g in range(2):
                        zt[g, :, cols(u)] = zst[g, u].T

            sweep(0, b_sweep)

        @pl.when(takes_in)
        def _():
            def forward(b):
                v_y(b, 1 - y).wait_recv()
                v_fwd(b, c).start()

            static_block(b_in, forward)

        @pl.when(merges & (b_merge % 2 != c))
        def _():
            u_half(b_merge)

        @pl.when((k == 1) & (c == 1))
        def _():
            u_half(1)
            merge(1)

        @pl.when(sweeps)
        def _():
            sweep(1, b_sweep)

        @pl.when((k >= AHEAD) & (k < NB))
        def _():
            static_block(k - AHEAD, v_issue)

        @pl.when(takes_in)
        def _():
            def arrived(b):
                v_own(b, 1 - c).wait_recv()
                v_fwd(b, 1 - c).wait_recv()

            static_block(b_in, arrived)
            gram(b_in)

        @pl.when(k >= 18)
        def _():
            z_send(25 - k)

        @pl.when((k == 14) | (k == 15))
        def _():
            z_send(8 + 2 * (15 - k))
            z_send(9 + 2 * (15 - k))

        @pl.when((k <= 12) & (k >= 5))
        def _():
            z_send(24 - k)

        @pl.when(k == NB + 1)
        def _():
            t_layout()

        @pl.when(merges & (k != 1) & (b_merge % 2 == c))
        def _():
            u_half(b_merge)
            merge(b_merge)

        return carry

    lax.fori_loop(0, NB + 2, step, 0)

    def out_part(g, u, core):
        return out.at[pl.ds(u * HALF, HALF), pl.ds(pl.multiple_of((2 * g + core) * HALF, HALF), HALF)]

    def z_part(g, u, rho):
        return zst.at[g, u, pl.ds(pl.multiple_of(rho * HALF, HALF), HALF), :]

    def out_local(g, u):
        return pltpu.make_async_copy(z_part(g, u, c), out_part(g, u, c), out_sem.at[g * NU + u])

    def out_sib(g, u):
        return remote(z_part(g, u, 1 - c), out_part(g, u, c), outs_sem.at[g * NU + u], outr_sem.at[g * NU + u], sib)

    def out_from_sib(g, u):
        part = out_part(g, u, 1 - c)
        return remote(part, part, outs_sem.at[g * NU + u], outr_sem.at[g * NU + u], sib)

    for g in range(2):
        weights(g, 0)

        def last(u, g=g):
            update(g, 0, u)
            zst[g, u] = zt[g, :, cols(u)].T

        _units(0, NU, last)
        for u in range(NU):
            out_local(g, u).start()
            out_sib(g, u).start()

    half_copy.wait_send()
    t_copy(0).wait_send()
    for b in range(NB):
        v_y(b, y).wait_send()
        v_own(b, c).wait_send()
        v_fwd(b, c).wait_send()
        z_chunk(b // 4, b % 4, x).wait_send()
    for g in range(2):
        for u in range(NU):
            out_local(g, u).wait()
            out_sib(g, u).wait_send()
            out_from_sib(g, u).wait_recv()


def solution(mesh):
    def local_run(z_cols, v_local, t_local):
        f32 = jnp.float32
        any_spec = pl.BlockSpec(memory_space=pl.ANY)
        dma = pltpu.SemaphoreType.DMA
        return pl.pallas_call(
            _kernel,
            out_shape=jax.ShapeDtypeStruct((ROWS, 4 * HALF), f32),
            in_specs=[any_spec] * 3,
            out_specs=any_spec,
            scratch_shapes=[
                pltpu.VMEM((2 * VU * HALF, TILE), f32),
                pltpu.VMEM((TILE, 2 * ROWS), f32),
                pltpu.VMEM((2, HALF, 2 * ROWS), f32),
                pltpu.VMEM((2, NU, TILE, HALF), f32),
                pltpu.VMEM((W, W, NB * 8), f32),
                pltpu.VMEM((NB * 8 * PITCH, W), f32),
                pltpu.VMEM((2, HALF, TILE), f32),
                pltpu.VMEM((2, 2, HALF, TILE), f32),
                pltpu.VMEM((HALF, TILE), f32),
                pltpu.VMEM((HALF, TILE), f32),
                pltpu.VMEM((2, HALF, HALF), f32),
                pltpu.VMEM((4, HALF, HALF), f32),
                pltpu.VMEM((HALF, HALF), f32),
                pltpu.VMEM((2, HALF, HALF), f32),
                pltpu.VMEM((4, TILE, TILE), f32),
                *[dma((NB,))] * 9,
                dma((2,)), dma((2, 2)), dma((2,)), dma((4,)), dma, dma, dma, dma((4,)), dma, *[dma((2 * NU,))] * 4,
            ],
            compiler_params=pltpu.CompilerParams(collective_id=0, has_side_effects=True, vmem_limit_bytes=63 * 2**20),
            name="backtransform",
        )(z_cols, v_local, t_local.transpose(1, 2, 0))

    return jax.shard_map(
        local_run,
        mesh=mesh,
        in_specs=(P("kpt", ("col", "row")), P(("kpt", "row"), "col"), P("kpt", None, None)),
        out_specs=P(("kpt", "row"), "col"),
        check_vma=False,
    )
```

```python
import jax
import jax.numpy as jnp
from jax import lax
from jax.experimental import pallas as pl
from jax.experimental.pallas import tpu as pltpu
from jax.sharding import PartitionSpec as P

PRECISE = lax.Precision.HIGHEST
MESH = pl.DeviceIdType.MESH

W = 32
ROWS = 1536
TILE = 256
HALF = 128
NT = ROWS // TILE
NU = ROWS // HALF
NB = 24
VU = 2 * sum(range(1, NU + 1))
PITCH = 40
AHEAD = 12


def _dot(a, b, ca, cb):
    return lax.dot_general(a, b, (((ca,), (cb,)), ((), ())), precision=PRECISE, preferred_element_type=jnp.float32)


def _base(b):
    p = b // 2
    return 2 * NU * p - p * (p - 1) + (b % 2) * (NU - p)


def _panel(idx):
    return jnp.where(idx < HALF, 2 * (idx // W), 2 * ((idx - HALF) // W) + 1)


def _units(lo, n, body, end=None):
    def six(h, carry):
        for u in range(6):
            body(lo + 6 * h + u)
        return carry

    lax.fori_loop(0, n // 6, six, 0)
    for rest in range(6):
        if rest or end:

            @pl.when(n % 6 == rest)
            def _(rest=rest):
                for u in range(rest):
                    body(lo + n - rest + u)
                if end:
                    end()


def _kernel(z_in, v_in, t_in, out, vbuf, vtr, zt, zst, t_raw, tt, acc, srecv, wbuf, gacc, usend, urecv, uhalf, upack, tbuf,
            loc_sem, ys_sem, yr_sem, os_sem, or_sem, fs_sem, fr_sem, zs_sem, zr_sem,
            ss_sem, sr_sem, us_sem, ur_sem, hs_sem, hr_sem, ts_sem, tr_sem, tt_sem, zo_sem, out_sem, outs_sem, outr_sem):
    ridx = lax.axis_index("row")
    y = lax.axis_index("col")
    x, c = ridx // 2, ridx % 2
    xn = {"row": (ridx + 2) % 4}
    sib = {"row": ridx + 1 - 2 * c}
    yn = {"col": 1 - y}

    barrier = pltpu.get_barrier_semaphore()
    for dev in (xn, sib, yn):
        pl.semaphore_signal(barrier, inc=1, device_id=dev, device_id_type=MESH)

    def remote(src, dst, send, recv, dev):
        return pltpu.make_async_remote_copy(src, dst, send, recv, device_id=dev, device_id_type=MESH)

    def slab(b, rho, par):
        start = (rho * VU + _base(b)) * HALF + 64 * (b % 2)
        return vbuf.at[pl.ds(pl.multiple_of(start, 64), ROWS - 64 * b), pl.ds(pl.multiple_of(par * HALF, HALF), HALF)]

    def v_local(b):
        return pltpu.make_async_copy(v_in.at[pl.ds(64 * b, ROWS - 64 * b), pl.ds(HALF * b, HALF)], slab(b, c, y), loc_sem.at[b])

    def v_y(b, par):
        return remote(slab(b, c, par), slab(b, c, par), ys_sem.at[b], yr_sem.at[b], yn)

    def v_own(b, rho):
        return remote(slab(b, rho, y), slab(b, rho, y), os_sem.at[b], or_sem.at[b], sib)

    def v_fwd(b, rho):
        return remote(slab(b, rho, 1 - y), slab(b, rho, 1 - y), fs_sem.at[b], fr_sem.at[b], sib)

    def v_issue(b):
        v_local(b).wait()
        v_y(b, y).start()
        v_own(b, c).start()

    def static_block(b, fn):
        for qq in range(NT):

            @pl.when(b // 4 == qq)
            def _(qq=qq):
                for ii in range(4):

                    @pl.when(b % 4 == ii)
                    def _(ii=ii):
                        fn(4 * qq + ii)

    def z_own(u, rho):
        return pltpu.make_async_copy(
            z_in.at[pl.ds(pl.multiple_of((2 * x + rho) * ROWS + u * HALF, HALF), HALF), :],
            zst.at[x, u, pl.ds(rho * HALF, HALF), :], zo_sem.at[2 * u + rho])

    def z_chunk(t, j, g):
        src = (2 * (1 - x) + j // 2) * ROWS + t * TILE + (j % 2) * HALF
        return remote(
            z_in.at[pl.ds(pl.multiple_of(src, HALF), HALF), :],
            zst.at[g, 2 * t + j % 2, pl.ds(pl.multiple_of((j // 2) * HALF, HALF), HALF), :],
            zs_sem.at[4 * t + j], zr_sem.at[4 * t + j], xn)

    t_copy_in = pltpu.make_async_copy(t_in, t_raw, tt_sem)

    for b in range(NB - 1, NB - 5, -1):
        v_local(b).start()
    t_copy_in.start()
    for u in range(NU - 1, -1, -1):
        for rho in range(2):
            z_own(u, rho).start()
    for b in range(NB - 5, -1, -1):
        v_local(b).start()
    for b in range(NB):
        if b % 2:
            for rho in range(2):
                vbuf[pl.ds((rho * VU + _base(b)) * HALF, 64), :] = jnp.zeros((64, TILE), jnp.float32)

    pl.semaphore_wait(barrier, 3)
    for b in range(NB - 1, NB - 1 - AHEAD, -1):
        v_issue(b)
        if b == NB - 2:
            for j in range(4):
                z_chunk(NT - 1, j, x).start()

    def rows(b, u, rho):
        return pl.ds(pl.multiple_of((rho * VU + _base(b) + u - b // 2) * HALF, HALF), HALF)

    def v_unit(b, u):
        return jnp.concatenate([vbuf[rows(b, u, rho), :] for rho in range(2)], axis=0)

    def cols(u):
        return pl.ds(pl.multiple_of(u * TILE, TILE), TILE)

    def s_copy(g, b):
        return remote(acc.at[g], srecv.at[g, b % 2], ss_sem.at[g], sr_sem.at[g, b % 2], xn)

    def weights(g, b):
        if g == 0:

            @pl.when(b % 2 != c)
            def _():
                t_copy(b).wait_recv()

        s_copy(g, b).wait_recv()
        s_sum = acc[g] + srecv[g, b % 2]
        wbuf[...] = _dot(s_sum, tbuf[b % 4], 1, 0)
        s_copy(g, b).wait_send()

    def update(g, b, u):
        if g == 0:
            v_tr = v_unit(b, u).T
            vtr[:, cols(u)] = v_tr
        else:
            v_tr = vtr[:, cols(u)]
        zt[g, :, cols(u)] = zt[g, :, cols(u)] - _dot(wbuf[...], v_tr, 1, 0)

    def partial_s(g, b, u):
        acc[g] += _dot(zt[g, :, cols(u)], v_unit(b, u), 1, 0)

    def sweep(g, k):
        @pl.when(k < NB - 1)
        def _():
            weights(g, k + 1)

        acc[g] = jnp.zeros((HALF, TILE), jnp.float32)
        first = (k + 1) // 2
        late = 1 - k % 2

        @pl.when(late == 1)
        def _():
            update(g, k + 1, first)

        def both(u):
            partial_s(g, k, u - 1)
            update(g, k + 1, u)

        _units(first + late, NU - first - late, both, lambda: partial_s(g, k, NU - 1))
        s_copy(g, k).start()

    ra = lax.broadcasted_iota(jnp.int32, (HALF, HALF), 0) // W
    rb = lax.broadcasted_iota(jnp.int32, (HALF, HALF), 1) // W

    def u_copy(b):
        return remote(usend.at[b % 2], urecv.at[b % 4], us_sem.at[b % 2], ur_sem.at[b % 4], xn)

    half_copy = remote(uhalf, upack.at[c], hs_sem, hr_sem, sib)

    def t_copy(b):
        return remote(tbuf.at[b % 4], tbuf.at[b % 4], ts_sem, tr_sem.at[b % 4], sib)

    def gram(b):
        def unit(u):
            own = jnp.concatenate(
                [vbuf[rows(b, u, rho), pl.ds(pl.multiple_of(c * HALF, HALF), HALF)] for rho in range(2)], axis=0)
            gacc[...] += _dot(own, v_unit(b, u), 0, 0)

        gacc[...] = jnp.zeros((HALF, TILE), jnp.float32)
        _units(b // 2, NU - b // 2, unit)

        def cols_of(par):
            return gacc[:, pl.ds(pl.multiple_of(par * HALF, HALF), HALF)]

        usend[b % 2] = jnp.where(ra <= rb, cols_of(1 - c), cols_of(c))
        u_copy(b).start()

    def u_half(b):
        u_copy(b).wait()
        total = usend[b % 2] + urecv[b % 4]

        @pl.when(b % 2 == c)
        def _():
            upack[c] = total

        @pl.when(b % 2 != c)
        def _():
            @pl.when(b < NB - 2)
            def _():
                half_copy.wait_send()

            uhalf[...] = total
            half_copy.start()

    def merge(b):
        half_copy.wait_recv()
        slot = b % 4

        @pl.when(b < NB - 2)
        def _():
            t_copy(b).wait_send()

        same = ra == rb

        def diagonal(par):
            at = [pl.multiple_of((8 * b + 2 * i + par) * PITCH, 8) for i in range(4)]
            stack = jnp.concatenate([tt[pl.ds(row, W), :] for row in at], axis=0)
            return jnp.where(same, jnp.concatenate([stack] * 4, axis=1), 0.0).T

        lo, hi = slice(0, HALF // 2), slice(HALF // 2, HALF)
        even_part, odd_part = upack[0], upack[1]
        ee, oo = jnp.where(ra > rb, even_part, 0.0), jnp.where(ra > rb, odd_part, 0.0)
        oe, eo = jnp.where(ra <= rb, even_part, 0.0).T, jnp.where(ra < rb, odd_part, 0.0).T

        def quad(a, b_, c_, d, rows_, cols_):
            return jnp.concatenate([
                jnp.concatenate([a[rows_, cols_], b_[rows_, cols_]], axis=1),
                jnp.concatenate([c_[rows_, cols_], d[rows_, cols_]], axis=1)], axis=0)

        even, odd = diagonal(0), diagonal(1)
        cross = -_dot(_dot(odd, jnp.where(same, oe, 0.0), 1, 0), even, 1, 0)
        zero = jnp.zeros((HALF, HALF), jnp.float32)
        pa, pb = ra % 2, rb % 2
        t_diag = []
        for part in (lo, hi):
            t_now = quad(even, zero, cross, odd, part, part)
            u_now = jnp.where(pa > pb, quad(ee, eo, oe, oo, part, part), 0.0)
            t_diag.append(t_now - _dot(_dot(t_now, u_now, 1, 0), t_now, 1, 0))
        t_lo, t_hi = t_diag
        t_off = -_dot(_dot(t_hi, quad(ee, eo, oe, oo, hi, lo), 1, 0), t_lo, 1, 0)
        half0 = jnp.zeros((HALF // 2, HALF // 2), jnp.float32)
        for rows_, out_rows in ((lo, 0), (hi, HALF)):
            tbuf[slot, out_rows : out_rows + HALF // 2, :] = jnp.concatenate(
                [t_lo[rows_, lo], half0, t_lo[rows_, hi], half0], axis=1)
            tbuf[slot, out_rows + HALF // 2 : out_rows + HALF, :] = jnp.concatenate(
                [t_off[rows_, lo], t_hi[rows_, lo], t_off[rows_, hi], t_hi[rows_, hi]], axis=1)
        t_copy(b).start()

    def t_layout():
        t_copy_in.wait()

        def t_row(i, carry):
            tt[pl.ds(i, NB * 8, stride=PITCH), :] = t_raw[i].T
            return carry

        lax.fori_loop(0, W, t_row, 0)

    def z_send(n):
        z_chunk((19 - n) // 4, n % 4, x).start()

    def step(s, carry):
        k = NB + 1 - s
        b_sweep = jnp.where(k == NB, NB - 1, k)
        sweeps = (k < NB - 1) | (k == NB)
        b_in, takes_in = jnp.where(k >= 4, k - 2, k - 1), (k >= 1) & (k != 3)
        b_merge, merges = jnp.where(k >= 3, k - 1, k), (k <= NB) & (k != 2)

        @pl.when(sweeps)
        def _():
            @pl.when(b_sweep % 4 == 3)
            def _():
                for j in range(4):
                    z_chunk(b_sweep // 4, j, 1 - x).wait_recv()
                for h in range(2):
                    u = 2 * (b_sweep // 4) + h
                    for rho in range(2):
                        z_own(u, rho).wait()
                    for g in range(2):
                        zt[g, :, cols(u)] = zst[g, u].T

            sweep(0, b_sweep)

        @pl.when(takes_in)
        def _():
            def forward(b):
                v_y(b, 1 - y).wait_recv()
                v_fwd(b, c).start()

            static_block(b_in, forward)

        @pl.when(merges & (b_merge % 2 != c))
        def _():
            u_half(b_merge)

        @pl.when((k == 1) & (c == 1))
        def _():
            u_half(1)
            merge(1)

        @pl.when(sweeps)
        def _():
            sweep(1, b_sweep)

        @pl.when((k >= AHEAD) & (k < NB))
        def _():
            static_block(k - AHEAD, v_issue)

        @pl.when(takes_in)
        def _():
            def arrived(b):
                v_own(b, 1 - c).wait_recv()
                v_fwd(b, 1 - c).wait_recv()

            static_block(b_in, arrived)
            gram(b_in)

        @pl.when(k >= 18)
        def _():
            z_send(25 - k)

        @pl.when((k == 14) | (k == 15))
        def _():
            z_send(8 + 2 * (15 - k))
            z_send(9 + 2 * (15 - k))

        @pl.when((k <= 12) & (k >= 5))
        def _():
            z_send(24 - k)

        @pl.when(k == NB + 1)
        def _():
            t_layout()

        @pl.when(merges & (k != 1) & (b_merge % 2 == c))
        def _():
            u_half(b_merge)
            merge(b_merge)

        return carry

    lax.fori_loop(0, NB + 2, step, 0)

    def out_part(g, u, core):
        return out.at[pl.ds(u * HALF, HALF), pl.ds(pl.multiple_of((2 * g + core) * HALF, HALF), HALF)]

    def z_part(g, u, rho):
        return zst.at[g, u, pl.ds(pl.multiple_of(rho * HALF, HALF), HALF), :]

    def out_local(g, u):
        return pltpu.make_async_copy(z_part(g, u, c), out_part(g, u, c), out_sem.at[g * NU + u])

    def out_sib(g, u):
        return remote(z_part(g, u, 1 - c), out_part(g, u, c), outs_sem.at[g * NU + u], outr_sem.at[g * NU + u], sib)

    def out_from_sib(g, u):
        part = out_part(g, u, 1 - c)
        return remote(part, part, outs_sem.at[g * NU + u], outr_sem.at[g * NU + u], sib)

    for g in range(2):
        weights(g, 0)

        def last(u, g=g):
            update(g, 0, u)
            zst[g, u] = zt[g, :, cols(u)].T

        _units(0, NU, last)
        for u in range(NU):
            out_local(g, u).start()
            out_sib(g, u).start()

    half_copy.wait_send()
    t_copy(0).wait_send()
    for b in range(NB):
        v_y(b, y).wait_send()
        v_own(b, c).wait_send()
        v_fwd(b, c).wait_send()
        z_chunk(b // 4, b % 4, x).wait_send()
    for g in range(2):
        for u in range(NU):
            out_local(g, u).wait()
            out_sib(g, u).wait_send()
            out_from_sib(g, u).wait_recv()


def solution(mesh):
    def local_run(z_cols, v_local, t_local):
        f32 = jnp.float32
        any_spec = pl.BlockSpec(memory_space=pl.ANY)
        dma = pltpu.SemaphoreType.DMA
        return pl.pallas_call(
            _kernel,
            out_shape=jax.ShapeDtypeStruct((ROWS, 4 * HALF), f32),
            in_specs=[any_spec] * 3,
            out_specs=any_spec,
            scratch_shapes=[
                pltpu.VMEM((2 * VU * HALF, TILE), f32),
                pltpu.VMEM((TILE, 2 * ROWS), f32),
                pltpu.VMEM((2, HALF, 2 * ROWS), f32),
                pltpu.VMEM((2, NU, TILE, HALF), f32),
                pltpu.VMEM((W, W, NB * 8), f32),
                pltpu.VMEM((NB * 8 * PITCH, W), f32),
                pltpu.VMEM((2, HALF, TILE), f32),
                pltpu.VMEM((2, 2, HALF, TILE), f32),
                pltpu.VMEM((HALF, TILE), f32),
                pltpu.VMEM((HALF, TILE), f32),
                pltpu.VMEM((2, HALF, HALF), f32),
                pltpu.VMEM((4, HALF, HALF), f32),
                pltpu.VMEM((HALF, HALF), f32),
                pltpu.VMEM((2, HALF, HALF), f32),
                pltpu.VMEM((4, TILE, TILE), f32),
                *[dma((NB,))] * 9,
                dma((2,)), dma((2, 2)), dma((2,)), dma((4,)), dma, dma, dma, dma((4,)), dma, *[dma((2 * NU,))] * 4,
            ],
            compiler_params=pltpu.CompilerParams(collective_id=0, has_side_effects=True, vmem_limit_bytes=63 * 2**20),
            name="backtransform",
        )(z_cols, v_local, t_local.transpose(1, 2, 0))

    return jax.shard_map(
        local_run,
        mesh=mesh,
        in_specs=(P("kpt", ("col", "row")), P(("kpt", "row"), "col"), P("kpt", None, None)),
        out_specs=P(("kpt", "row"), "col"),
        check_vma=False,
    )
```

```python
import jax
import jax.numpy as jnp
from jax import lax
from jax.experimental import pallas as pl
from jax.experimental.pallas import tpu as pltpu
from jax.sharding import PartitionSpec as P

PRECISE = lax.Precision.HIGHEST
MESH = pl.DeviceIdType.MESH

W = 32
ROWS = 1536
TILE = 256
HALF = 128
NT = ROWS // TILE
NU = ROWS // HALF
NB = 24
VU = 2 * sum(range(1, NU + 1))
PITCH = 40
AHEAD = 12


def _dot(a, b, ca, cb):
    return lax.dot_general(a, b, (((ca,), (cb,)), ((), ())), precision=PRECISE, preferred_element_type=jnp.float32)


def _base(b):
    p = b // 2
    return 2 * NU * p - p * (p - 1) + (b % 2) * (NU - p)


def _panel(idx):
    return jnp.where(idx < HALF, 2 * (idx // W), 2 * ((idx - HALF) // W) + 1)


def _units(lo, n, body, end=None):
    def six(h, carry):
        for u in range(6):
            body(lo + 6 * h + u)
        return carry

    lax.fori_loop(0, n // 6, six, 0)
    for rest in range(6):
        if rest or end:

            @pl.when(n % 6 == rest)
            def _(rest=rest):
                for u in range(rest):
                    body(lo + n - rest + u)
                if end:
                    end()


def _kernel(z_in, v_in, t_in, out, vbuf, vtr, zt, zst, t_raw, tt, acc, srecv, wbuf, gacc, usend, urecv, uhalf, upack, tbuf,
            loc_sem, ys_sem, yr_sem, os_sem, or_sem, fs_sem, fr_sem, zs_sem, zr_sem,
            ss_sem, sr_sem, us_sem, ur_sem, hs_sem, hr_sem, ts_sem, tr_sem, tt_sem, zo_sem, out_sem, outs_sem, outr_sem):
    ridx = lax.axis_index("row")
    y = lax.axis_index("col")
    x, c = ridx // 2, ridx % 2
    xn = {"row": (ridx + 2) % 4}
    sib = {"row": ridx + 1 - 2 * c}
    yn = {"col": 1 - y}

    barrier = pltpu.get_barrier_semaphore()
    for dev in (xn, sib, yn):
        pl.semaphore_signal(barrier, inc=1, device_id=dev, device_id_type=MESH)

    def remote(src, dst, send, recv, dev):
        return pltpu.make_async_remote_copy(src, dst, send, recv, device_id=dev, device_id_type=MESH)

    def slab(b, rho, par):
        start = (rho * VU + _base(b)) * HALF + 64 * (b % 2)
        return vbuf.at[pl.ds(pl.multiple_of(start, 64), ROWS - 64 * b), pl.ds(pl.multiple_of(par * HALF, HALF), HALF)]

    def v_local(b):
        return pltpu.make_async_copy(v_in.at[pl.ds(64 * b, ROWS - 64 * b), pl.ds(HALF * b, HALF)], slab(b, c, y), loc_sem.at[b])

    def v_y(b, par):
        return remote(slab(b, c, par), slab(b, c, par), ys_sem.at[b], yr_sem.at[b], yn)

    def v_own(b, rho):
        return remote(slab(b, rho, y), slab(b, rho, y), os_sem.at[b], or_sem.at[b], sib)

    def v_fwd(b, rho):
        return remote(slab(b, rho, 1 - y), slab(b, rho, 1 - y), fs_sem.at[b], fr_sem.at[b], sib)

    def v_issue(b):
        v_local(b).wait()
        v_y(b, y).start()
        v_own(b, c).start()

    def static_block(b, fn):
        for qq in range(NT):

            @pl.when(b // 4 == qq)
            def _(qq=qq):
                for ii in range(4):

                    @pl.when(b % 4 == ii)
                    def _(ii=ii):
                        fn(4 * qq + ii)

    def z_own(u, rho):
        return pltpu.make_async_copy(
            z_in.at[pl.ds(pl.multiple_of((2 * x + rho) * ROWS + u * HALF, HALF), HALF), :],
            zst.at[x, u, pl.ds(rho * HALF, HALF), :], zo_sem.at[2 * u + rho])

    def z_chunk(t, j, g):
        src = (2 * (1 - x) + j // 2) * ROWS + t * TILE + (j % 2) * HALF
        return remote(
            z_in.at[pl.ds(pl.multiple_of(src, HALF), HALF), :],
            zst.at[g, 2 * t + j % 2, pl.ds(pl.multiple_of((j // 2) * HALF, HALF), HALF), :],
            zs_sem.at[4 * t + j], zr_sem.at[4 * t + j], xn)

    t_copy_in = pltpu.make_async_copy(t_in, t_raw, tt_sem)

    for b in range(NB - 1, NB - 5, -1):
        v_local(b).start()
    t_copy_in.start()
    for u in range(NU - 1, -1, -1):
        for rho in range(2):
            z_own(u, rho).start()
    for b in range(NB - 5, -1, -1):
        v_local(b).start()
    for b in range(NB):
        if b % 2:
            for rho in range(2):
                vbuf[pl.ds((rho * VU + _base(b)) * HALF, 64), :] = jnp.zeros((64, TILE), jnp.float32)

    pl.semaphore_wait(barrier, 3)
    for b in range(NB - 1, NB - 1 - AHEAD, -1):
        v_issue(b)
        if b == NB - 2:
            for j in range(4):
                z_chunk(NT - 1, j, x).start()

    def rows(b, u, rho):
        return pl.ds(pl.multiple_of((rho * VU + _base(b) + u - b // 2) * HALF, HALF), HALF)

    def v_unit(b, u):
        return jnp.concatenate([vbuf[rows(b, u, rho), :] for rho in range(2)], axis=0)

    def cols(u):
        return pl.ds(pl.multiple_of(u * TILE, TILE), TILE)

    def s_copy(g, b):
        return remote(acc.at[g], srecv.at[g, b % 2], ss_sem.at[g], sr_sem.at[g, b % 2], xn)

    def weights(g, b):
        if g == 0:

            @pl.when(b % 2 != c)
            def _():
                t_copy(b).wait_recv()

        s_copy(g, b).wait_recv()
        s_sum = acc[g] + srecv[g, b % 2]
        wbuf[...] = _dot(s_sum, tbuf[b % 4], 1, 0)
        s_copy(g, b).wait_send()

    def update(g, b, u):
        if g == 0:
            v_tr = v_unit(b, u).T
            vtr[:, cols(u)] = v_tr
        else:
            v_tr = vtr[:, cols(u)]
        zt[g, :, cols(u)] = zt[g, :, cols(u)] - _dot(wbuf[...], v_tr, 1, 0)

    def partial_s(g, b, u):
        acc[g] += _dot(zt[g, :, cols(u)], v_unit(b, u), 1, 0)

    def sweep(g, k):
        @pl.when(k < NB - 1)
        def _():
            weights(g, k + 1)

        acc[g] = jnp.zeros((HALF, TILE), jnp.float32)
        first = (k + 1) // 2
        late = 1 - k % 2

        @pl.when(late == 1)
        def _():
            update(g, k + 1, first)

        def both(u):
            partial_s(g, k, u - 1)
            update(g, k + 1, u)

        _units(first + late, NU - first - late, both, lambda: partial_s(g, k, NU - 1))
        s_copy(g, k).start()

    ra = lax.broadcasted_iota(jnp.int32, (HALF, HALF), 0) // W
    rb = lax.broadcasted_iota(jnp.int32, (HALF, HALF), 1) // W

    def u_copy(b):
        return remote(usend.at[b % 2], urecv.at[b % 4], us_sem.at[b % 2], ur_sem.at[b % 4], xn)

    half_copy = remote(uhalf, upack.at[c], hs_sem, hr_sem, sib)

    def t_copy(b):
        return remote(tbuf.at[b % 4], tbuf.at[b % 4], ts_sem, tr_sem.at[b % 4], sib)

    def gram(b):
        def unit(u):
            own = jnp.concatenate(
                [vbuf[rows(b, u, rho), pl.ds(pl.multiple_of(c * HALF, HALF), HALF)] for rho in range(2)], axis=0)
            gacc[...] += _dot(own, v_unit(b, u), 0, 0)

        gacc[...] = jnp.zeros((HALF, TILE), jnp.float32)
        _units(b // 2, NU - b // 2, unit)

        def cols_of(par):
            return gacc[:, pl.ds(pl.multiple_of(par * HALF, HALF), HALF)]

        usend[b % 2] = jnp.where(ra <= rb, cols_of(1 - c), cols_of(c))
        u_copy(b).start()

    def u_half(b):
        u_copy(b).wait()
        total = usend[b % 2] + urecv[b % 4]

        @pl.when(b % 2 == c)
        def _():
            upack[c] = total

        @pl.when(b % 2 != c)
        def _():
            @pl.when(b < NB - 2)
            def _():
                half_copy.wait_send()

            uhalf[...] = total
            half_copy.start()

    def merge(b):
        half_copy.wait_recv()
        slot = b % 4

        @pl.when(b < NB - 2)
        def _():
            t_copy(b).wait_send()

        same = ra == rb

        def diagonal(par):
            at = [pl.multiple_of((8 * b + 2 * i + par) * PITCH, 8) for i in range(4)]
            stack = jnp.concatenate([tt[pl.ds(row, W), :] for row in at], axis=0)
            return jnp.where(same, jnp.concatenate([stack] * 4, axis=1), 0.0).T

        lo, hi = slice(0, HALF // 2), slice(HALF // 2, HALF)
        even_part, odd_part = upack[0], upack[1]
        ee, oo = jnp.where(ra > rb, even_part, 0.0), jnp.where(ra > rb, odd_part, 0.0)
        oe, eo = jnp.where(ra <= rb, even_part, 0.0).T, jnp.where(ra < rb, odd_part, 0.0).T

        def quad(a, b_, c_, d, rows_, cols_):
            return jnp.concatenate([
                jnp.concatenate([a[rows_, cols_], b_[rows_, cols_]], axis=1),
                jnp.concatenate([c_[rows_, cols_], d[rows_, cols_]], axis=1)], axis=0)

        even, odd = diagonal(0), diagonal(1)
        cross = -_dot(_dot(odd, jnp.where(same, oe, 0.0), 1, 0), even, 1, 0)
        zero = jnp.zeros((HALF, HALF), jnp.float32)
        pa, pb = ra % 2, rb % 2
        t_diag = []
        for part in (lo, hi):
            t_now = quad(even, zero, cross, odd, part, part)
            u_now = jnp.where(pa > pb, quad(ee, eo, oe, oo, part, part), 0.0)
            t_diag.append(t_now - _dot(_dot(t_now, u_now, 1, 0), t_now, 1, 0))
        t_lo, t_hi = t_diag
        t_off = -_dot(_dot(t_hi, quad(ee, eo, oe, oo, hi, lo), 1, 0), t_lo, 1, 0)
        half0 = jnp.zeros((HALF // 2, HALF // 2), jnp.float32)
        for rows_, out_rows in ((lo, 0), (hi, HALF)):
            tbuf[slot, out_rows : out_rows + HALF // 2, :] = jnp.concatenate(
                [t_lo[rows_, lo], half0, t_lo[rows_, hi], half0], axis=1)
            tbuf[slot, out_rows + HALF // 2 : out_rows + HALF, :] = jnp.concatenate(
                [t_off[rows_, lo], t_hi[rows_, lo], t_off[rows_, hi], t_hi[rows_, hi]], axis=1)
        t_copy(b).start()

    def t_layout():
        t_copy_in.wait()

        def t_row(i, carry):
            tt[pl.ds(i, NB * 8, stride=PITCH), :] = t_raw[i].T
            return carry

        lax.fori_loop(0, W, t_row, 0)

    def z_send(n):
        z_chunk((19 - n) // 4, n % 4, x).start()

    def forward(b):
        v_y(b, 1 - y).wait_recv()
        v_fwd(b, c).start()

    def arrived(b):
        v_own(b, 1 - c).wait_recv()
        v_fwd(b, 1 - c).wait_recv()

    def step(s, carry):
        k = NB + 1 - s
        b_sweep = jnp.where(k == NB, NB - 1, k)
        sweeps = (k < NB - 1) | (k == NB)
        b_in, takes_in = jnp.where(k >= 4, k - 2, k - 1), (k >= 2) & (k != 3)
        b_merge, merges = jnp.where(k >= 3, k - 1, k), (k <= NB) & (k != 2)

        @pl.when(sweeps)
        def _():
            @pl.when(b_sweep % 4 == 3)
            def _():
                for j in range(4):
                    z_chunk(b_sweep // 4, j, 1 - x).wait_recv()
                for h in range(2):
                    u = 2 * (b_sweep // 4) + h
                    for rho in range(2):
                        z_own(u, rho).wait()
                    for g in range(2):
                        zt[g, :, cols(u)] = zst[g, u].T

            sweep(0, b_sweep)

        @pl.when(takes_in)
        def _():
            static_block(b_in, forward)

        @pl.when(merges & (b_merge % 2 != c))
        def _():
            u_half(b_merge)

        @pl.when((k == 1) & (c == 1))
        def _():
            u_half(1)
            merge(1)

        @pl.when(sweeps)
        def _():
            sweep(1, b_sweep)

        @pl.when((k >= AHEAD) & (k < NB))
        def _():
            static_block(k - AHEAD, v_issue)

        @pl.when(takes_in)
        def _():
            static_block(b_in, arrived)
            gram(b_in)

        @pl.when(k >= 18)
        def _():
            z_send(25 - k)

        @pl.when((k == 14) | (k == 15))
        def _():
            z_send(8 + 2 * (15 - k))
            z_send(9 + 2 * (15 - k))

        @pl.when((k <= 12) & (k >= 5))
        def _():
            z_send(24 - k)

        @pl.when(k == NB + 1)
        def _():
            t_layout()

        @pl.when(merges & (k != 1) & (b_merge % 2 == c))
        def _():
            u_half(b_merge)
            merge(b_merge)

        return carry

    lax.fori_loop(0, NB + 1, step, 0)

    for g in range(2):
        weights(g, 1)
        _units(0, NU, lambda u, g=g: update(g, 1, u))
    forward(0)
    arrived(0)
    gram(0)
    for g in range(2):
        acc[g] = jnp.zeros((HALF, TILE), jnp.float32)
        _units(0, NU, lambda u, g=g: partial_s(g, 0, u))
        s_copy(g, 0).start()
    u_half(0)

    @pl.when(c == 0)
    def _():
        merge(0)

    def out_part(g, u, core):
        return out.at[pl.ds(u * HALF, HALF), pl.ds(pl.multiple_of((2 * g + core) * HALF, HALF), HALF)]

    def z_part(g, u, rho):
        return zst.at[g, u, pl.ds(pl.multiple_of(rho * HALF, HALF), HALF), :]

    def out_local(g, u):
        return pltpu.make_async_copy(z_part(g, u, c), out_part(g, u, c), out_sem.at[g * NU + u])

    def out_sib(g, u):
        return remote(z_part(g, u, 1 - c), out_part(g, u, c), outs_sem.at[g * NU + u], outr_sem.at[g * NU + u], sib)

    def out_from_sib(g, u):
        part = out_part(g, u, 1 - c)
        return remote(part, part, outs_sem.at[g * NU + u], outr_sem.at[g * NU + u], sib)

    for g in range(2):
        weights(g, 0)

        def last(u, g=g):
            update(g, 0, u)
            zst[g, u] = zt[g, :, cols(u)].T

        _units(0, NU, last)
        for u in range(NU):
            out_local(g, u).start()
            out_sib(g, u).start()

    half_copy.wait_send()
    t_copy(0).wait_send()
    for b in range(NB):
        v_y(b, y).wait_send()
        v_own(b, c).wait_send()
        v_fwd(b, c).wait_send()
        z_chunk(b // 4, b % 4, x).wait_send()
    for g in range(2):
        for u in range(NU):
            out_local(g, u).wait()
            out_sib(g, u).wait_send()
            out_from_sib(g, u).wait_recv()


def solution(mesh):
    def local_run(z_cols, v_local, t_local):
        f32 = jnp.float32
        any_spec = pl.BlockSpec(memory_space=pl.ANY)
        dma = pltpu.SemaphoreType.DMA
        return pl.pallas_call(
            _kernel,
            out_shape=jax.ShapeDtypeStruct((ROWS, 4 * HALF), f32),
            in_specs=[any_spec] * 3,
            out_specs=any_spec,
            scratch_shapes=[
                pltpu.VMEM((2 * VU * HALF, TILE), f32),
                pltpu.VMEM((TILE, 2 * ROWS), f32),
                pltpu.VMEM((2, HALF, 2 * ROWS), f32),
                pltpu.VMEM((2, NU, TILE, HALF), f32),
                pltpu.VMEM((W, W, NB * 8), f32),
                pltpu.VMEM((NB * 8 * PITCH, W), f32),
                pltpu.VMEM((2, HALF, TILE), f32),
                pltpu.VMEM((2, 2, HALF, TILE), f32),
                pltpu.VMEM((HALF, TILE), f32),
                pltpu.VMEM((HALF, TILE), f32),
                pltpu.VMEM((2, HALF, HALF), f32),
                pltpu.VMEM((4, HALF, HALF), f32),
                pltpu.VMEM((HALF, HALF), f32),
                pltpu.VMEM((2, HALF, HALF), f32),
                pltpu.VMEM((4, TILE, TILE), f32),
                *[dma((NB,))] * 9,
                dma((2,)), dma((2, 2)), dma((2,)), dma((4,)), dma, dma, dma, dma((4,)), dma, *[dma((2 * NU,))] * 4,
            ],
            compiler_params=pltpu.CompilerParams(collective_id=0, has_side_effects=True, vmem_limit_bytes=63 * 2**20),
            name="backtransform",
        )(z_cols, v_local, t_local.transpose(1, 2, 0))

    return jax.shard_map(
        local_run,
        mesh=mesh,
        in_specs=(P("kpt", ("col", "row")), P(("kpt", "row"), "col"), P("kpt", None, None)),
        out_specs=P(("kpt", "row"), "col"),
        check_vma=False,
    )
```

```python
import jax
import jax.numpy as jnp
from jax import lax
from jax.experimental import pallas as pl
from jax.experimental.pallas import tpu as pltpu
from jax.sharding import PartitionSpec as P

PRECISE = lax.Precision.HIGHEST
MESH = pl.DeviceIdType.MESH

W = 32
ROWS = 1536
TILE = 256
HALF = 128
NT = ROWS // TILE
NU = ROWS // HALF
NB = 24
VU = 2 * sum(range(1, NU + 1))
PITCH = 40
AHEAD = 12


def _dot(a, b, ca, cb):
    return lax.dot_general(a, b, (((ca,), (cb,)), ((), ())), precision=PRECISE, preferred_element_type=jnp.float32)


def _base(b):
    p = b // 2
    return 2 * NU * p - p * (p - 1) + (b % 2) * (NU - p)


def _panel(idx):
    return jnp.where(idx < HALF, 2 * (idx // W), 2 * ((idx - HALF) // W) + 1)


def _units(lo, n, body, end=None):
    def six(h, carry):
        for u in range(6):
            body(lo + 6 * h + u)
        return carry

    lax.fori_loop(0, n // 6, six, 0)
    for rest in range(6):
        if rest or end:

            @pl.when(n % 6 == rest)
            def _(rest=rest):
                for u in range(rest):
                    body(lo + n - rest + u)
                if end:
                    end()


def _kernel(z_in, v_in, t_in, out, vbuf, vtr, zt, zst, t_raw, tt, acc, srecv, wbuf, gacc, usend, urecv, uhalf, upack, tbuf,
            loc_sem, ys_sem, yr_sem, os_sem, or_sem, fs_sem, fr_sem, zs_sem, zr_sem,
            ss_sem, sr_sem, us_sem, ur_sem, hs_sem, hr_sem, ts_sem, tr_sem, tt_sem, zo_sem, out_sem, outs_sem, outr_sem):
    ridx = lax.axis_index("row")
    y = lax.axis_index("col")
    x, c = ridx // 2, ridx % 2
    xn = {"row": (ridx + 2) % 4}
    sib = {"row": ridx + 1 - 2 * c}
    yn = {"col": 1 - y}

    barrier = pltpu.get_barrier_semaphore()
    for dev in (xn, sib, yn):
        pl.semaphore_signal(barrier, inc=1, device_id=dev, device_id_type=MESH)

    def remote(src, dst, send, recv, dev):
        return pltpu.make_async_remote_copy(src, dst, send, recv, device_id=dev, device_id_type=MESH)

    def slab(b, rho, par):
        start = (rho * VU + _base(b)) * HALF + 64 * (b % 2)
        return vbuf.at[pl.ds(pl.multiple_of(start, 64), ROWS - 64 * b), pl.ds(pl.multiple_of(par * HALF, HALF), HALF)]

    def v_local(b):
        return pltpu.make_async_copy(v_in.at[pl.ds(64 * b, ROWS - 64 * b), pl.ds(HALF * b, HALF)], slab(b, c, y), loc_sem.at[b])

    def v_y(b, par):
        return remote(slab(b, c, par), slab(b, c, par), ys_sem.at[b], yr_sem.at[b], yn)

    def v_own(b, rho):
        return remote(slab(b, rho, y), slab(b, rho, y), os_sem.at[b], or_sem.at[b], sib)

    def v_fwd(b, rho):
        return remote(slab(b, rho, 1 - y), slab(b, rho, 1 - y), fs_sem.at[b], fr_sem.at[b], sib)

    def v_issue(b):
        v_local(b).wait()
        v_y(b, y).start()
        v_own(b, c).start()

    def static_block(b, fn):
        for qq in range(NT):

            @pl.when(b // 4 == qq)
            def _(qq=qq):
                for ii in range(4):

                    @pl.when(b % 4 == ii)
                    def _(ii=ii):
                        fn(4 * qq + ii)

    def z_own(u, rho):
        return pltpu.make_async_copy(
            z_in.at[pl.ds(pl.multiple_of((2 * x + rho) * ROWS + u * HALF, HALF), HALF), :],
            zst.at[x, u, pl.ds(rho * HALF, HALF), :], zo_sem.at[2 * u + rho])

    def z_chunk(t, j, g):
        src = (2 * (1 - x) + j // 2) * ROWS + t * TILE + (j % 2) * HALF
        return remote(
            z_in.at[pl.ds(pl.multiple_of(src, HALF), HALF), :],
            zst.at[g, 2 * t + j % 2, pl.ds(pl.multiple_of((j // 2) * HALF, HALF), HALF), :],
            zs_sem.at[4 * t + j], zr_sem.at[4 * t + j], xn)

    t_copy_in = pltpu.make_async_copy(t_in, t_raw, tt_sem)

    for b in range(NB - 1, NB - 5, -1):
        v_local(b).start()
    t_copy_in.start()
    for u in range(NU - 1, -1, -1):
        for rho in range(2):
            z_own(u, rho).start()
    for b in range(NB - 5, -1, -1):
        v_local(b).start()
    for b in range(NB):
        if b % 2:
            for rho in range(2):
                vbuf[pl.ds((rho * VU + _base(b)) * HALF, 64), :] = jnp.zeros((64, TILE), jnp.float32)

    pl.semaphore_wait(barrier, 3)
    for b in range(NB - 1, NB - 1 - AHEAD, -1):
        v_issue(b)
        if b == NB - 2:
            for j in range(4):
                z_chunk(NT - 1, j, x).start()

    def rows(b, u, rho):
        return pl.ds(pl.multiple_of((rho * VU + _base(b) + u - b // 2) * HALF, HALF), HALF)

    def v_unit(b, u):
        return jnp.concatenate([vbuf[rows(b, u, rho), :] for rho in range(2)], axis=0)

    def cols(u):
        return pl.ds(pl.multiple_of(u * TILE, TILE), TILE)

    def s_copy(g, b):
        return remote(acc.at[g], srecv.at[g, b % 2], ss_sem.at[g], sr_sem.at[g, b % 2], xn)

    def weights(g, b):
        if g == 0:

            @pl.when(b % 2 != c)
            def _():
                t_copy(b).wait_recv()

        s_copy(g, b).wait_recv()
        s_sum = acc[g] + srecv[g, b % 2]
        wbuf[...] = _dot(s_sum, tbuf[b % 4], 1, 0)
        s_copy(g, b).wait_send()

    def update(g, b, u):
        if g == 0:
            v_tr = v_unit(b, u).T
            vtr[:, cols(u)] = v_tr
        else:
            v_tr = vtr[:, cols(u)]
        zt[g, :, cols(u)] = zt[g, :, cols(u)] - _dot(wbuf[...], v_tr, 1, 0)

    def partial_s(g, b, u):
        acc[g] += _dot(zt[g, :, cols(u)], v_unit(b, u), 1, 0)

    def sweep(g, k):
        @pl.when(k < NB - 1)
        def _():
            weights(g, k + 1)

        acc[g] = jnp.zeros((HALF, TILE), jnp.float32)
        first = (k + 1) // 2
        late = 1 - k % 2

        @pl.when(late == 1)
        def _():
            update(g, k + 1, first)

        def both(u):
            partial_s(g, k, u - 1)
            update(g, k + 1, u)

        _units(first + late, NU - first - late, both, lambda: partial_s(g, k, NU - 1))
        s_copy(g, k).start()

    ra = lax.broadcasted_iota(jnp.int32, (HALF, HALF), 0) // W
    rb = lax.broadcasted_iota(jnp.int32, (HALF, HALF), 1) // W

    def u_copy(b):
        return remote(usend.at[b % 2], urecv.at[b % 4], us_sem.at[b % 2], ur_sem.at[b % 4], xn)

    half_copy = remote(uhalf, upack.at[c], hs_sem, hr_sem, sib)

    def t_copy(b):
        return remote(tbuf.at[b % 4], tbuf.at[b % 4], ts_sem, tr_sem.at[b % 4], sib)

    def gram(b):
        def unit(u):
            own = jnp.concatenate(
                [vbuf[rows(b, u, rho), pl.ds(pl.multiple_of(c * HALF, HALF), HALF)] for rho in range(2)], axis=0)
            gacc[...] += _dot(own, v_unit(b, u), 0, 0)

        gacc[...] = jnp.zeros((HALF, TILE), jnp.float32)
        _units(b // 2, NU - b // 2, unit)

        def cols_of(par):
            return gacc[:, pl.ds(pl.multiple_of(par * HALF, HALF), HALF)]

        usend[b % 2] = jnp.where(ra <= rb, cols_of(1 - c), cols_of(c))
        u_copy(b).start()

    def u_half(b):
        u_copy(b).wait()
        total = usend[b % 2] + urecv[b % 4]

        @pl.when(b % 2 == c)
        def _():
            upack[c] = total

        @pl.when(b % 2 != c)
        def _():
            @pl.when(b < NB - 2)
            def _():
                half_copy.wait_send()

            uhalf[...] = total
            half_copy.start()

    def merge(b):
        half_copy.wait_recv()
        slot = b % 4

        @pl.when(b < NB - 2)
        def _():
            t_copy(b).wait_send()

        same = ra == rb

        def diagonal(par):
            at = [pl.multiple_of((8 * b + 2 * i + par) * PITCH, 8) for i in range(4)]
            stack = jnp.concatenate([tt[pl.ds(row, W), :] for row in at], axis=0)
            return jnp.where(same, jnp.concatenate([stack] * 4, axis=1), 0.0).T

        lo, hi = slice(0, HALF // 2), slice(HALF // 2, HALF)
        even_part, odd_part = upack[0], upack[1]
        ee, oo = jnp.where(ra > rb, even_part, 0.0), jnp.where(ra > rb, odd_part, 0.0)
        oe, eo = jnp.where(ra <= rb, even_part, 0.0).T, jnp.where(ra < rb, odd_part, 0.0).T

        def quad(a, b_, c_, d, rows_, cols_):
            return jnp.concatenate([
                jnp.concatenate([a[rows_, cols_], b_[rows_, cols_]], axis=1),
                jnp.concatenate([c_[rows_, cols_], d[rows_, cols_]], axis=1)], axis=0)

        even, odd = diagonal(0), diagonal(1)
        cross = -_dot(_dot(odd, jnp.where(same, oe, 0.0), 1, 0), even, 1, 0)
        zero = jnp.zeros((HALF, HALF), jnp.float32)
        pa, pb = ra % 2, rb % 2
        t_diag = []
        for part in (lo, hi):
            t_now = quad(even, zero, cross, odd, part, part)
            u_now = jnp.where(pa > pb, quad(ee, eo, oe, oo, part, part), 0.0)
            t_diag.append(t_now - _dot(_dot(t_now, u_now, 1, 0), t_now, 1, 0))
        t_lo, t_hi = t_diag
        t_off = -_dot(_dot(t_hi, quad(ee, eo, oe, oo, hi, lo), 1, 0), t_lo, 1, 0)
        half0 = jnp.zeros((HALF // 2, HALF // 2), jnp.float32)
        for rows_, out_rows in ((lo, 0), (hi, HALF)):
            tbuf[slot, out_rows : out_rows + HALF // 2, :] = jnp.concatenate(
                [t_lo[rows_, lo], half0, t_lo[rows_, hi], half0], axis=1)
            tbuf[slot, out_rows + HALF // 2 : out_rows + HALF, :] = jnp.concatenate(
                [t_off[rows_, lo], t_hi[rows_, lo], t_off[rows_, hi], t_hi[rows_, hi]], axis=1)
        t_copy(b).start()

    def t_layout():
        t_copy_in.wait()

        def t_row(i, carry):
            tt[pl.ds(i, NB * 8, stride=PITCH), :] = t_raw[i].T
            return carry

        lax.fori_loop(0, W, t_row, 0)

    def z_send(n):
        z_chunk((19 - n) // 4, n % 4, x).start()

    def forward(b):
        v_y(b, 1 - y).wait_recv()
        v_fwd(b, c).start()

    def arrived(b):
        v_own(b, 1 - c).wait_recv()
        v_fwd(b, 1 - c).wait_recv()

    def step(s, carry):
        k = NB + 1 - s
        b_sweep = jnp.where(k == NB, NB - 1, k)
        sweeps = (k < NB - 1) | (k == NB)
        b_in, takes_in = jnp.where(k >= 4, k - 2, k - 1), (k >= 2) & (k != 3)
        b_merge, merges = jnp.where(k >= 3, k - 1, k), (k <= NB) & (k != 2)

        @pl.when(sweeps)
        def _():
            @pl.when(b_sweep % 4 == 3)
            def _():
                for j in range(4):
                    z_chunk(b_sweep // 4, j, 1 - x).wait_recv()
                for h in range(2):
                    u = 2 * (b_sweep // 4) + h
                    for rho in range(2):
                        z_own(u, rho).wait()
                    for g in range(2):
                        zt[g, :, cols(u)] = zst[g, u].T

            sweep(0, b_sweep)

        @pl.when(takes_in)
        def _():
            static_block(b_in, forward)

        @pl.when(merges & (b_merge % 2 != c))
        def _():
            u_half(b_merge)

        @pl.when((k == 1) & (c == 1))
        def _():
            u_half(1)
            merge(1)

        @pl.when(sweeps)
        def _():
            sweep(1, b_sweep)

        @pl.when((k >= AHEAD) & (k < NB))
        def _():
            static_block(k - AHEAD, v_issue)

        @pl.when(takes_in)
        def _():
            static_block(b_in, arrived)
            gram(b_in)

        @pl.when(k >= 18)
        def _():
            z_send(25 - k)

        @pl.when((k <= 15) & (k >= 4))
        def _():
            z_send(23 - k)

        @pl.when(k == NB + 1)
        def _():
            t_layout()

        @pl.when(merges & (k != 1) & (b_merge % 2 == c))
        def _():
            u_half(b_merge)
            merge(b_merge)

        return carry

    lax.fori_loop(0, NB + 1, step, 0)

    def update_1(g):
        weights(g, 1)
        _units(0, NU, lambda u: update(g, 1, u))

    def s_0(g):
        acc[g] = jnp.zeros((HALF, TILE), jnp.float32)
        _units(0, NU, lambda u: partial_s(g, 0, u))
        s_copy(g, 0).start()

    forward(0)
    update_1(0)
    arrived(0)
    gram(0)
    update_1(1)
    s_0(0)

    @pl.when(c == 1)
    def _():
        u_half(0)

    s_0(1)

    @pl.when(c == 0)
    def _():
        u_half(0)
        merge(0)

    def out_part(g, u, core):
        return out.at[pl.ds(u * HALF, HALF), pl.ds(pl.multiple_of((2 * g + core) * HALF, HALF), HALF)]

    def z_part(g, u, rho):
        return zst.at[g, u, pl.ds(pl.multiple_of(rho * HALF, HALF), HALF), :]

    def out_local(g, u):
        return pltpu.make_async_copy(z_part(g, u, c), out_part(g, u, c), out_sem.at[g * NU + u])

    def out_sib(g, u):
        return remote(z_part(g, u, 1 - c), out_part(g, u, c), outs_sem.at[g * NU + u], outr_sem.at[g * NU + u], sib)

    def out_from_sib(g, u):
        part = out_part(g, u, 1 - c)
        return remote(part, part, outs_sem.at[g * NU + u], outr_sem.at[g * NU + u], sib)

    for g in range(2):
        weights(g, 0)

        def last(u, g=g):
            update(g, 0, u)
            zst[g, u] = zt[g, :, cols(u)].T

        _units(0, NU, last)
        for u in range(NU):
            out_local(g, u).start()
            out_sib(g, u).start()

    half_copy.wait_send()
    t_copy(0).wait_send()
    for b in range(NB):
        v_y(b, y).wait_send()
        v_own(b, c).wait_send()
        v_fwd(b, c).wait_send()
        z_chunk(b // 4, b % 4, x).wait_send()
    for g in range(2):
        for u in range(NU):
            out_local(g, u).wait()
            out_sib(g, u).wait_send()
            out_from_sib(g, u).wait_recv()


def solution(mesh):
    def local_run(z_cols, v_local, t_local):
        f32 = jnp.float32
        any_spec = pl.BlockSpec(memory_space=pl.ANY)
        dma = pltpu.SemaphoreType.DMA
        return pl.pallas_call(
            _kernel,
            out_shape=jax.ShapeDtypeStruct((ROWS, 4 * HALF), f32),
            in_specs=[any_spec] * 3,
            out_specs=any_spec,
            scratch_shapes=[
                pltpu.VMEM((2 * VU * HALF, TILE), f32),
                pltpu.VMEM((TILE, 2 * ROWS), f32),
                pltpu.VMEM((2, HALF, 2 * ROWS), f32),
                pltpu.VMEM((2, NU, TILE, HALF), f32),
                pltpu.VMEM((W, W, NB * 8), f32),
                pltpu.VMEM((NB * 8 * PITCH, W), f32),
                pltpu.VMEM((2, HALF, TILE), f32),
                pltpu.VMEM((2, 2, HALF, TILE), f32),
                pltpu.VMEM((HALF, TILE), f32),
                pltpu.VMEM((HALF, TILE), f32),
                pltpu.VMEM((2, HALF, HALF), f32),
                pltpu.VMEM((4, HALF, HALF), f32),
                pltpu.VMEM((HALF, HALF), f32),
                pltpu.VMEM((2, HALF, HALF), f32),
                pltpu.VMEM((4, TILE, TILE), f32),
                *[dma((NB,))] * 9,
                dma((2,)), dma((2, 2)), dma((2,)), dma((4,)), dma, dma, dma, dma((4,)), dma, *[dma((2 * NU,))] * 4,
            ],
            compiler_params=pltpu.CompilerParams(collective_id=0, has_side_effects=True, vmem_limit_bytes=63 * 2**20),
            name="backtransform",
        )(z_cols, v_local, t_local.transpose(1, 2, 0))

    return jax.shard_map(
        local_run,
        mesh=mesh,
        in_specs=(P("kpt", ("col", "row")), P(("kpt", "row"), "col"), P("kpt", None, None)),
        out_specs=P(("kpt", "row"), "col"),
        check_vma=False,
    )
```

```python
import jax
import jax.numpy as jnp
from jax import lax
from jax.experimental import pallas as pl
from jax.experimental.pallas import tpu as pltpu
from jax.sharding import PartitionSpec as P

PRECISE = lax.Precision.HIGHEST
MESH = pl.DeviceIdType.MESH

W = 32
ROWS = 1536
TILE = 256
HALF = 128
NT = ROWS // TILE
NU = ROWS // HALF
NB = 24
VU = 2 * sum(range(1, NU + 1))
PITCH = 40
AHEAD = 12


def _dot(a, b, ca, cb):
    return lax.dot_general(a, b, (((ca,), (cb,)), ((), ())), precision=PRECISE, preferred_element_type=jnp.float32)


def _base(b):
    p = b // 2
    return 2 * NU * p - p * (p - 1) + (b % 2) * (NU - p)


def _panel(idx):
    return jnp.where(idx < HALF, 2 * (idx // W), 2 * ((idx - HALF) // W) + 1)


def _units(lo, n, body, end=None):
    def six(h, carry):
        for u in range(6):
            body(lo + 6 * h + u)
        return carry

    lax.fori_loop(0, n // 6, six, 0)
    for rest in range(6):
        if rest or end:

            @pl.when(n % 6 == rest)
            def _(rest=rest):
                for u in range(rest):
                    body(lo + n - rest + u)
                if end:
                    end()


def _kernel(z_in, v_in, t_in, out, vbuf, vtr, zt, zst, t_raw, tt, acc, srecv, wbuf, gacc, usend, urecv, uhalf, upack, tbuf,
            loc_sem, ys_sem, yr_sem, os_sem, or_sem, fs_sem, fr_sem, zs_sem, zr_sem,
            ss_sem, sr_sem, us_sem, ur_sem, hs_sem, hr_sem, ts_sem, tr_sem, tt_sem, zo_sem, out_sem, outs_sem, outr_sem):
    ridx = lax.axis_index("row")
    y = lax.axis_index("col")
    x, c = ridx // 2, ridx % 2
    xn = {"row": (ridx + 2) % 4}
    sib = {"row": ridx + 1 - 2 * c}
    yn = {"col": 1 - y}

    barrier = pltpu.get_barrier_semaphore()
    for dev in (xn, sib, yn):
        pl.semaphore_signal(barrier, inc=1, device_id=dev, device_id_type=MESH)

    def remote(src, dst, send, recv, dev):
        return pltpu.make_async_remote_copy(src, dst, send, recv, device_id=dev, device_id_type=MESH)

    def slab(b, rho, par):
        start = (rho * VU + _base(b)) * HALF + 64 * (b % 2)
        return vbuf.at[pl.ds(pl.multiple_of(start, 64), ROWS - 64 * b), pl.ds(pl.multiple_of(par * HALF, HALF), HALF)]

    def v_local(b):
        return pltpu.make_async_copy(v_in.at[pl.ds(64 * b, ROWS - 64 * b), pl.ds(HALF * b, HALF)], slab(b, c, y), loc_sem.at[b])

    def v_y(b, par):
        return remote(slab(b, c, par), slab(b, c, par), ys_sem.at[b], yr_sem.at[b], yn)

    def v_own(b, rho):
        return remote(slab(b, rho, y), slab(b, rho, y), os_sem.at[b], or_sem.at[b], sib)

    def v_fwd(b, rho):
        return remote(slab(b, rho, 1 - y), slab(b, rho, 1 - y), fs_sem.at[b], fr_sem.at[b], sib)

    def v_issue(b):
        v_local(b).wait()
        v_y(b, y).start()
        v_own(b, c).start()

    def static_block(b, fn):
        for qq in range(NT):

            @pl.when(b // 4 == qq)
            def _(qq=qq):
                for ii in range(4):

                    @pl.when(b % 4 == ii)
                    def _(ii=ii):
                        fn(4 * qq + ii)

    def z_own(u, rho):
        return pltpu.make_async_copy(
            z_in.at[pl.ds(pl.multiple_of((2 * x + rho) * ROWS + u * HALF, HALF), HALF), :],
            zst.at[x, u, pl.ds(rho * HALF, HALF), :], zo_sem.at[2 * u + rho])

    def z_chunk(t, j, g):
        src = (2 * (1 - x) + j // 2) * ROWS + t * TILE + (j % 2) * HALF
        return remote(
            z_in.at[pl.ds(pl.multiple_of(src, HALF), HALF), :],
            zst.at[g, 2 * t + j % 2, pl.ds(pl.multiple_of((j // 2) * HALF, HALF), HALF), :],
            zs_sem.at[4 * t + j], zr_sem.at[4 * t + j], xn)

    t_copy_in = pltpu.make_async_copy(t_in, t_raw, tt_sem)

    for b in range(NB - 1, NB - 5, -1):
        v_local(b).start()
    t_copy_in.start()
    for u in range(NU - 1, -1, -1):
        for rho in range(2):
            z_own(u, rho).start()
    for b in range(NB - 5, -1, -1):
        v_local(b).start()
    for b in range(NB):
        if b % 2:
            for rho in range(2):
                vbuf[pl.ds((rho * VU + _base(b)) * HALF, 64), :] = jnp.zeros((64, TILE), jnp.float32)

    pl.semaphore_wait(barrier, 3)
    for b in range(NB - 1, NB - 1 - AHEAD, -1):
        v_issue(b)
        if b == NB - 2:
            for j in range(4):
                z_chunk(NT - 1, j, x).start()

    def rows(b, u, rho):
        return pl.ds(pl.multiple_of((rho * VU + _base(b) + u - b // 2) * HALF, HALF), HALF)

    def v_unit(b, u):
        return jnp.concatenate([vbuf[rows(b, u, rho), :] for rho in range(2)], axis=0)

    def cols(u):
        return pl.ds(pl.multiple_of(u * TILE, TILE), TILE)

    def s_copy(g, b):
        return remote(acc.at[g], srecv.at[g, b % 2], ss_sem.at[g], sr_sem.at[g, b % 2], xn)

    def weights(g, b):
        if g == 0:

            @pl.when(b % 2 != c)
            def _():
                t_copy(b).wait_recv()

        s_copy(g, b).wait_recv()
        s_sum = acc[g] + srecv[g, b % 2]
        wbuf[...] = _dot(s_sum, tbuf[b % 4], 1, 0)
        s_copy(g, b).wait_send()

    def update(g, b, u):
        if g == 0:
            v_tr = v_unit(b, u).T
            vtr[:, cols(u)] = v_tr
        else:
            v_tr = vtr[:, cols(u)]
        zt[g, :, cols(u)] = zt[g, :, cols(u)] - _dot(wbuf[...], v_tr, 1, 0)

    def partial_s(g, b, u):
        acc[g] += _dot(zt[g, :, cols(u)], v_unit(b, u), 1, 0)

    def sweep(g, k):
        @pl.when(k < NB - 1)
        def _():
            weights(g, k + 1)

        acc[g] = jnp.zeros((HALF, TILE), jnp.float32)
        first = (k + 1) // 2
        late = 1 - k % 2

        @pl.when(late == 1)
        def _():
            update(g, k + 1, first)

        def both(u):
            partial_s(g, k, u - 1)
            update(g, k + 1, u)

        _units(first + late, NU - first - late, both, lambda: partial_s(g, k, NU - 1))
        s_copy(g, k).start()

    ra = lax.broadcasted_iota(jnp.int32, (HALF, HALF), 0) // W
    rb = lax.broadcasted_iota(jnp.int32, (HALF, HALF), 1) // W

    def u_copy(b):
        return remote(usend.at[b % 2], urecv.at[b % 4], us_sem.at[b % 2], ur_sem.at[b % 4], xn)

    half_copy = remote(uhalf, upack.at[c], hs_sem, hr_sem, sib)

    def t_copy(b):
        return remote(tbuf.at[b % 4], tbuf.at[b % 4], ts_sem, tr_sem.at[b % 4], sib)

    def gram(b):
        def unit(u):
            own = jnp.concatenate(
                [vbuf[rows(b, u, rho), pl.ds(pl.multiple_of(c * HALF, HALF), HALF)] for rho in range(2)], axis=0)
            gacc[...] += _dot(own, v_unit(b, u), 0, 0)

        gacc[...] = jnp.zeros((HALF, TILE), jnp.float32)
        _units(b // 2, NU - b // 2, unit)

        def cols_of(par):
            return gacc[:, pl.ds(pl.multiple_of(par * HALF, HALF), HALF)]

        usend[b % 2] = jnp.where(ra <= rb, cols_of(1 - c), cols_of(c))
        u_copy(b).start()

    def u_half(b):
        u_copy(b).wait()
        total = usend[b % 2] + urecv[b % 4]

        @pl.when(b % 2 == c)
        def _():
            upack[c] = total

        @pl.when(b % 2 != c)
        def _():
            @pl.when(b < NB - 2)
            def _():
                half_copy.wait_send()

            uhalf[...] = total
            half_copy.start()

    def merge(b):
        half_copy.wait_recv()
        slot = b % 4

        @pl.when(b < NB - 2)
        def _():
            t_copy(b).wait_send()

        same = ra == rb

        def diagonal(par):
            at = [pl.multiple_of((8 * b + 2 * i + par) * PITCH, 8) for i in range(4)]
            stack = jnp.concatenate([tt[pl.ds(row, W), :] for row in at], axis=0)
            return jnp.where(same, jnp.concatenate([stack] * 4, axis=1), 0.0).T

        lo, hi = slice(0, HALF // 2), slice(HALF // 2, HALF)
        even_part, odd_part = upack[0], upack[1]
        ee, oo = jnp.where(ra > rb, even_part, 0.0), jnp.where(ra > rb, odd_part, 0.0)
        oe, eo = jnp.where(ra <= rb, even_part, 0.0).T, jnp.where(ra < rb, odd_part, 0.0).T

        def quad(a, b_, c_, d, rows_, cols_):
            return jnp.concatenate([
                jnp.concatenate([a[rows_, cols_], b_[rows_, cols_]], axis=1),
                jnp.concatenate([c_[rows_, cols_], d[rows_, cols_]], axis=1)], axis=0)

        even, odd = diagonal(0), diagonal(1)
        cross = -_dot(_dot(odd, jnp.where(same, oe, 0.0), 1, 0), even, 1, 0)
        zero = jnp.zeros((HALF, HALF), jnp.float32)
        pa, pb = ra % 2, rb % 2
        t_diag = []
        for part in (lo, hi):
            t_now = quad(even, zero, cross, odd, part, part)
            u_now = jnp.where(pa > pb, quad(ee, eo, oe, oo, part, part), 0.0)
            t_diag.append(t_now - _dot(_dot(t_now, u_now, 1, 0), t_now, 1, 0))
        t_lo, t_hi = t_diag
        t_off = -_dot(_dot(t_hi, quad(ee, eo, oe, oo, hi, lo), 1, 0), t_lo, 1, 0)
        half0 = jnp.zeros((HALF // 2, HALF // 2), jnp.float32)
        for rows_, out_rows in ((lo, 0), (hi, HALF)):
            tbuf[slot, out_rows : out_rows + HALF // 2, :] = jnp.concatenate(
                [t_lo[rows_, lo], half0, t_lo[rows_, hi], half0], axis=1)
            tbuf[slot, out_rows + HALF // 2 : out_rows + HALF, :] = jnp.concatenate(
                [t_off[rows_, lo], t_hi[rows_, lo], t_off[rows_, hi], t_hi[rows_, hi]], axis=1)
        t_copy(b).start()

    def t_layout():
        t_copy_in.wait()

        def t_row(i, carry):
            tt[pl.ds(i, NB * 8, stride=PITCH), :] = t_raw[i].T
            return carry

        lax.fori_loop(0, W, t_row, 0)

    def z_send(n):
        z_chunk((19 - n) // 4, n % 4, x).start()

    def forward(b):
        v_y(b, 1 - y).wait_recv()
        v_fwd(b, c).start()

    def arrived(b):
        v_own(b, 1 - c).wait_recv()
        v_fwd(b, 1 - c).wait_recv()

    def step(s, carry):
        k = NB + 1 - s
        b_sweep = jnp.where(k == NB, NB - 1, k)
        sweeps = (k < NB - 1) | (k == NB)
        b_in, takes_in = jnp.where(k >= 4, k - 2, k - 1), (k >= 2) & (k != 3)
        b_merge, merges = jnp.where(k >= 3, k - 1, k), (k <= NB) & (k != 2)

        @pl.when(sweeps)
        def _():
            @pl.when(b_sweep % 4 == 3)
            def _():
                for j in range(4):
                    z_chunk(b_sweep // 4, j, 1 - x).wait_recv()
                for h in range(2):
                    u = 2 * (b_sweep // 4) + h
                    for rho in range(2):
                        z_own(u, rho).wait()
                    for g in range(2):
                        zt[g, :, cols(u)] = zst[g, u].T

            sweep(0, b_sweep)

        @pl.when(takes_in)
        def _():
            static_block(b_in, forward)

        @pl.when(merges & (b_merge % 2 != c))
        def _():
            u_half(b_merge)

        @pl.when(sweeps)
        def _():
            sweep(1, b_sweep)

        @pl.when((k >= AHEAD) & (k < NB))
        def _():
            static_block(k - AHEAD, v_issue)

        @pl.when(takes_in)
        def _():
            static_block(b_in, arrived)
            gram(b_in)

        @pl.when(k >= 18)
        def _():
            z_send(25 - k)

        @pl.when((k <= 16) & (k >= 5))
        def _():
            z_send(24 - k)

        @pl.when(k == NB + 1)
        def _():
            t_layout()

        @pl.when(merges & (b_merge % 2 == c))
        def _():
            u_half(b_merge)
            merge(b_merge)

        return carry

    lax.fori_loop(0, NB + 1, step, 0)

    def update_1(g):
        weights(g, 1)
        _units(0, NU, lambda u: update(g, 1, u))

    def s_0(g):
        acc[g] = jnp.zeros((HALF, TILE), jnp.float32)
        _units(0, NU, lambda u: partial_s(g, 0, u))
        s_copy(g, 0).start()

    def gram_0(core):
        @pl.when(c == core)
        def _():
            arrived(0)
            gram(0)

    forward(0)
    gram_0(1)
    update_1(0)
    gram_0(0)
    update_1(1)

    @pl.when(c == 1)
    def _():
        u_half(0)

    s_0(0)

    @pl.when(c == 0)
    def _():
        u_half(0)
        merge(0)

    s_0(1)

    def out_part(g, u, core):
        return out.at[pl.ds(u * HALF, HALF), pl.ds(pl.multiple_of((2 * g + core) * HALF, HALF), HALF)]

    def z_part(g, u, rho):
        return zst.at[g, u, pl.ds(pl.multiple_of(rho * HALF, HALF), HALF), :]

    def out_local(g, u):
        return pltpu.make_async_copy(z_part(g, u, c), out_part(g, u, c), out_sem.at[g * NU + u])

    def out_sib(g, u):
        return remote(z_part(g, u, 1 - c), out_part(g, u, c), outs_sem.at[g * NU + u], outr_sem.at[g * NU + u], sib)

    def out_from_sib(g, u):
        part = out_part(g, u, 1 - c)
        return remote(part, part, outs_sem.at[g * NU + u], outr_sem.at[g * NU + u], sib)

    for g in range(2):
        weights(g, 0)

        def last(u, g=g):
            update(g, 0, u)
            zst[g, u] = zt[g, :, cols(u)].T

        _units(0, NU, last)
        for u in range(NU):
            out_local(g, u).start()
            out_sib(g, u).start()

    half_copy.wait_send()
    t_copy(0).wait_send()
    for b in range(NB):
        v_y(b, y).wait_send()
        v_own(b, c).wait_send()
        v_fwd(b, c).wait_send()
        z_chunk(b // 4, b % 4, x).wait_send()
    for g in range(2):
        for u in range(NU):
            out_local(g, u).wait()
            out_sib(g, u).wait_send()
            out_from_sib(g, u).wait_recv()


def solution(mesh):
    def local_run(z_cols, v_local, t_local):
        f32 = jnp.float32
        any_spec = pl.BlockSpec(memory_space=pl.ANY)
        dma = pltpu.SemaphoreType.DMA
        return pl.pallas_call(
            _kernel,
            out_shape=jax.ShapeDtypeStruct((ROWS, 4 * HALF), f32),
            in_specs=[any_spec] * 3,
            out_specs=any_spec,
            scratch_shapes=[
                pltpu.VMEM((2 * VU * HALF, TILE), f32),
                pltpu.VMEM((TILE, 2 * ROWS), f32),
                pltpu.VMEM((2, HALF, 2 * ROWS), f32),
                pltpu.VMEM((2, NU, TILE, HALF), f32),
                pltpu.VMEM((W, W, NB * 8), f32),
                pltpu.VMEM((NB * 8 * PITCH, W), f32),
                pltpu.VMEM((2, HALF, TILE), f32),
                pltpu.VMEM((2, 2, HALF, TILE), f32),
                pltpu.VMEM((HALF, TILE), f32),
                pltpu.VMEM((HALF, TILE), f32),
                pltpu.VMEM((2, HALF, HALF), f32),
                pltpu.VMEM((4, HALF, HALF), f32),
                pltpu.VMEM((HALF, HALF), f32),
                pltpu.VMEM((2, HALF, HALF), f32),
                pltpu.VMEM((4, TILE, TILE), f32),
                *[dma((NB,))] * 9,
                dma((2,)), dma((2, 2)), dma((2,)), dma((4,)), dma, dma, dma, dma((4,)), dma, *[dma((2 * NU,))] * 4,
            ],
            compiler_params=pltpu.CompilerParams(collective_id=0, has_side_effects=True, vmem_limit_bytes=63 * 2**20),
            name="backtransform",
        )(z_cols, v_local, t_local.transpose(1, 2, 0))

    return jax.shard_map(
        local_run,
        mesh=mesh,
        in_specs=(P("kpt", ("col", "row")), P(("kpt", "row"), "col"), P("kpt", None, None)),
        out_specs=P(("kpt", "row"), "col"),
        check_vma=False,
    )
```

```python
import jax
import jax.numpy as jnp
from jax import lax
from jax.experimental import pallas as pl
from jax.experimental.pallas import tpu as pltpu
from jax.sharding import PartitionSpec as P

PRECISE = lax.Precision.HIGHEST
MESH = pl.DeviceIdType.MESH

W = 32
ROWS = 1536
TILE = 256
HALF = 128
NT = ROWS // TILE
NU = ROWS // HALF
NB = 24
VU = 2 * sum(range(1, NU + 1))
PITCH = 40
AHEAD = 12


def _dot(a, b, ca, cb):
    return lax.dot_general(a, b, (((ca,), (cb,)), ((), ())), precision=PRECISE, preferred_element_type=jnp.float32)


def _base(b):
    p = b // 2
    return 2 * NU * p - p * (p - 1) + (b % 2) * (NU - p)


def _panel(idx):
    return jnp.where(idx < HALF, 2 * (idx // W), 2 * ((idx - HALF) // W) + 1)


def _units(lo, n, body, end=None):
    def six(h, carry):
        for u in range(6):
            body(lo + 6 * h + u)
        return carry

    lax.fori_loop(0, n // 6, six, 0)
    for rest in range(6):
        if rest or end:

            @pl.when(n % 6 == rest)
            def _(rest=rest):
                for u in range(rest):
                    body(lo + n - rest + u)
                if end:
                    end()


def _kernel(z_in, v_in, t_in, out, vbuf, vtr, zt, zst, t_raw, tt, acc, srecv, wbuf, gacc, usend, urecv, uhalf, upack, tbuf,
            loc_sem, ys_sem, yr_sem, os_sem, or_sem, fs_sem, fr_sem, zs_sem, zr_sem,
            ss_sem, sr_sem, us_sem, ur_sem, hs_sem, hr_sem, ts_sem, tr_sem, tt_sem, zo_sem, out_sem, outs_sem, outr_sem):
    ridx = lax.axis_index("row")
    y = lax.axis_index("col")
    x, c = ridx // 2, ridx % 2
    xn = {"row": (ridx + 2) % 4}
    sib = {"row": ridx + 1 - 2 * c}
    yn = {"col": 1 - y}

    barrier = pltpu.get_barrier_semaphore()
    for dev in (xn, sib, yn):
        pl.semaphore_signal(barrier, inc=1, device_id=dev, device_id_type=MESH)

    def remote(src, dst, send, recv, dev):
        return pltpu.make_async_remote_copy(src, dst, send, recv, device_id=dev, device_id_type=MESH)

    def slab(b, rho, par):
        start = (rho * VU + _base(b)) * HALF + 64 * (b % 2)
        return vbuf.at[pl.ds(pl.multiple_of(start, 64), ROWS - 64 * b), pl.ds(pl.multiple_of(par * HALF, HALF), HALF)]

    def v_local(b):
        return pltpu.make_async_copy(v_in.at[pl.ds(64 * b, ROWS - 64 * b), pl.ds(HALF * b, HALF)], slab(b, c, y), loc_sem.at[b])

    def v_y(b, par):
        return remote(slab(b, c, par), slab(b, c, par), ys_sem.at[b], yr_sem.at[b], yn)

    def v_own(b, rho):
        return remote(slab(b, rho, y), slab(b, rho, y), os_sem.at[b], or_sem.at[b], sib)

    def v_fwd(b, rho):
        return remote(slab(b, rho, 1 - y), slab(b, rho, 1 - y), fs_sem.at[b], fr_sem.at[b], sib)

    def v_issue(b):
        v_local(b).wait()
        v_y(b, y).start()
        v_own(b, c).start()

    def static_block(b, fn, low=0, high=NB):
        if high - low == 1:
            fn(low)
            return
        mid = (low + high) // 2
        lax.cond(b < mid, lambda: static_block(b, fn, low, mid), lambda: static_block(b, fn, mid, high))

    def z_own(u, rho):
        return pltpu.make_async_copy(
            z_in.at[pl.ds(pl.multiple_of((2 * x + rho) * ROWS + u * HALF, HALF), HALF), :],
            zst.at[x, u, pl.ds(rho * HALF, HALF), :], zo_sem.at[2 * u + rho])

    def z_chunk(t, j, g):
        src = (2 * (1 - x) + j // 2) * ROWS + t * TILE + (j % 2) * HALF
        return remote(
            z_in.at[pl.ds(pl.multiple_of(src, HALF), HALF), :],
            zst.at[g, 2 * t + j % 2, pl.ds(pl.multiple_of((j // 2) * HALF, HALF), HALF), :],
            zs_sem.at[4 * t + j], zr_sem.at[4 * t + j], xn)

    t_copy_in = pltpu.make_async_copy(t_in, t_raw, tt_sem)

    for b in range(NB - 1, NB - 5, -1):
        v_local(b).start()
    t_copy_in.start()
    for u in range(NU - 1, -1, -1):
        for rho in range(2):
            z_own(u, rho).start()
    for b in range(NB - 5, -1, -1):
        v_local(b).start()
    for b in range(NB):
        if b % 2:
            for rho in range(2):
                vbuf[pl.ds((rho * VU + _base(b)) * HALF, 64), :] = jnp.zeros((64, TILE), jnp.float32)

    pl.semaphore_wait(barrier, 3)
    for b in range(NB - 1, NB - 1 - AHEAD, -1):
        v_issue(b)
        if b == NB - 2:
            for j in range(4):
                z_chunk(NT - 1, j, x).start()

    def rows(b, u, rho):
        return pl.ds(pl.multiple_of((rho * VU + _base(b) + u - b // 2) * HALF, HALF), HALF)

    def v_unit(b, u):
        return jnp.concatenate([vbuf[rows(b, u, rho), :] for rho in range(2)], axis=0)

    def cols(u):
        return pl.ds(pl.multiple_of(u * TILE, TILE), TILE)

    def s_copy(g, b):
        return remote(acc.at[g], srecv.at[g, b % 2], ss_sem.at[g], sr_sem.at[g, b % 2], xn)

    def weights(g, b):
        if g == 0:

            @pl.when(b % 2 != c)
            def _():
                t_copy(b).wait_recv()

        s_copy(g, b).wait_recv()
        s_sum = acc[g] + srecv[g, b % 2]
        wbuf[...] = _dot(s_sum, tbuf[b % 4], 1, 0)
        s_copy(g, b).wait_send()

    def update(g, b, u):
        if g == 0:
            v_tr = v_unit(b, u).T
            vtr[:, cols(u)] = v_tr
        else:
            v_tr = vtr[:, cols(u)]
        zt[g, :, cols(u)] = zt[g, :, cols(u)] - _dot(wbuf[...], v_tr, 1, 0)

    def partial_s(g, b, u):
        acc[g] += _dot(zt[g, :, cols(u)], v_unit(b, u), 1, 0)

    def sweep(g, k):
        @pl.when(k < NB - 1)
        def _():
            weights(g, k + 1)

        acc[g] = jnp.zeros((HALF, TILE), jnp.float32)
        first = (k + 1) // 2
        late = 1 - k % 2

        @pl.when(late == 1)
        def _():
            update(g, k + 1, first)

        def both(u):
            partial_s(g, k, u - 1)
            update(g, k + 1, u)

        _units(first + late, NU - first - late, both, lambda: partial_s(g, k, NU - 1))
        s_copy(g, k).start()

    ra = lax.broadcasted_iota(jnp.int32, (HALF, HALF), 0) // W
    rb = lax.broadcasted_iota(jnp.int32, (HALF, HALF), 1) // W

    def u_copy(b):
        return remote(usend.at[b % 2], urecv.at[b % 4], us_sem.at[b % 2], ur_sem.at[b % 4], xn)

    half_copy = remote(uhalf, upack.at[c], hs_sem, hr_sem, sib)

    def t_copy(b):
        return remote(tbuf.at[b % 4], tbuf.at[b % 4], ts_sem, tr_sem.at[b % 4], sib)

    def gram(b):
        def unit(u):
            own = jnp.concatenate(
                [vbuf[rows(b, u, rho), pl.ds(pl.multiple_of(c * HALF, HALF), HALF)] for rho in range(2)], axis=0)
            gacc[...] += _dot(own, v_unit(b, u), 0, 0)

        gacc[...] = jnp.zeros((HALF, TILE), jnp.float32)
        _units(b // 2, NU - b // 2, unit)

        def cols_of(par):
            return gacc[:, pl.ds(pl.multiple_of(par * HALF, HALF), HALF)]

        usend[b % 2] = jnp.where(ra <= rb, cols_of(1 - c), cols_of(c))
        u_copy(b).start()

    def u_half(b):
        u_copy(b).wait()
        total = usend[b % 2] + urecv[b % 4]

        @pl.when(b % 2 == c)
        def _():
            upack[c] = total

        @pl.when(b % 2 != c)
        def _():
            @pl.when(b < NB - 2)
            def _():
                half_copy.wait_send()

            uhalf[...] = total
            half_copy.start()

    def merge(b):
        half_copy.wait_recv()
        slot = b % 4

        @pl.when(b < NB - 2)
        def _():
            t_copy(b).wait_send()

        same = ra == rb

        def diagonal(par):
            at = [pl.multiple_of((8 * b + 2 * i + par) * PITCH, 8) for i in range(4)]
            stack = jnp.concatenate([tt[pl.ds(row, W), :] for row in at], axis=0)
            return jnp.where(same, jnp.concatenate([stack] * 4, axis=1), 0.0).T

        lo, hi = slice(0, HALF // 2), slice(HALF // 2, HALF)
        even_part, odd_part = upack[0], upack[1]
        ee, oo = jnp.where(ra > rb, even_part, 0.0), jnp.where(ra > rb, odd_part, 0.0)
        oe, eo = jnp.where(ra <= rb, even_part, 0.0).T, jnp.where(ra < rb, odd_part, 0.0).T

        def quad(a, b_, c_, d, rows_, cols_):
            return jnp.concatenate([
                jnp.concatenate([a[rows_, cols_], b_[rows_, cols_]], axis=1),
                jnp.concatenate([c_[rows_, cols_], d[rows_, cols_]], axis=1)], axis=0)

        even, odd = diagonal(0), diagonal(1)
        cross = -_dot(_dot(odd, jnp.where(same, oe, 0.0), 1, 0), even, 1, 0)
        zero = jnp.zeros((HALF, HALF), jnp.float32)
        pa, pb = ra % 2, rb % 2
        t_diag = []
        for part in (lo, hi):
            t_now = quad(even, zero, cross, odd, part, part)
            u_now = jnp.where(pa > pb, quad(ee, eo, oe, oo, part, part), 0.0)
            t_diag.append(t_now - _dot(_dot(t_now, u_now, 1, 0), t_now, 1, 0))
        t_lo, t_hi = t_diag
        t_off = -_dot(_dot(t_hi, quad(ee, eo, oe, oo, hi, lo), 1, 0), t_lo, 1, 0)
        half0 = jnp.zeros((HALF // 2, HALF // 2), jnp.float32)
        for rows_, out_rows in ((lo, 0), (hi, HALF)):
            tbuf[slot, out_rows : out_rows + HALF // 2, :] = jnp.concatenate(
                [t_lo[rows_, lo], half0, t_lo[rows_, hi], half0], axis=1)
            tbuf[slot, out_rows + HALF // 2 : out_rows + HALF, :] = jnp.concatenate(
                [t_off[rows_, lo], t_hi[rows_, lo], t_off[rows_, hi], t_hi[rows_, hi]], axis=1)
        t_copy(b).start()

    def t_layout():
        t_copy_in.wait()

        def t_row(i, carry):
            tt[pl.ds(i, NB * 8, stride=PITCH), :] = t_raw[i].T
            return carry

        lax.fori_loop(0, W, t_row, 0)

    def z_send(n):
        z_chunk((19 - n) // 4, n % 4, x).start()

    def forward(b):
        v_y(b, 1 - y).wait_recv()
        v_fwd(b, c).start()

    def arrived(b):
        v_own(b, 1 - c).wait_recv()
        v_fwd(b, 1 - c).wait_recv()

    def step(s, carry):
        k = NB + 1 - s
        b_sweep = jnp.where(k == NB, NB - 1, k)
        sweeps = (k < NB - 1) | (k == NB)
        b_in, takes_in = jnp.where(k >= 4, k - 2, k - 1), (k >= 2) & (k != 3)
        b_merge, merges = jnp.where(k >= 3, k - 1, k), (k <= NB) & (k != 2)

        @pl.when(sweeps)
        def _():
            @pl.when(b_sweep % 4 == 3)
            def _():
                for j in range(4):
                    z_chunk(b_sweep // 4, j, 1 - x).wait_recv()
                for h in range(2):
                    u = 2 * (b_sweep // 4) + h
                    for rho in range(2):
                        z_own(u, rho).wait()
                    for g in range(2):
                        zt[g, :, cols(u)] = zst[g, u].T

            sweep(0, b_sweep)

        @pl.when(takes_in)
        def _():
            static_block(b_in, forward)

        @pl.when(merges & (b_merge % 2 != c))
        def _():
            u_half(b_merge)

        @pl.when(sweeps)
        def _():
            sweep(1, b_sweep)

        @pl.when((k >= AHEAD) & (k < NB))
        def _():
            static_block(k - AHEAD, v_issue)

        @pl.when(takes_in)
        def _():
            static_block(b_in, arrived)
            gram(b_in)

        @pl.when(k >= 18)
        def _():
            z_send(25 - k)

        @pl.when((k <= 16) & (k >= 5))
        def _():
            z_send(24 - k)

        @pl.when(k == NB + 1)
        def _():
            t_layout()

        @pl.when(merges & (b_merge % 2 == c))
        def _():
            u_half(b_merge)
            merge(b_merge)

        return carry

    lax.fori_loop(0, NB + 1, step, 0)

    def update_1(g):
        weights(g, 1)
        _units(0, NU, lambda u: update(g, 1, u))

    def s_0(g):
        acc[g] = jnp.zeros((HALF, TILE), jnp.float32)
        _units(0, NU, lambda u: partial_s(g, 0, u))
        s_copy(g, 0).start()

    def gram_0(core):
        @pl.when(c == core)
        def _():
            arrived(0)
            gram(0)

    forward(0)
    gram_0(1)
    update_1(0)
    gram_0(0)
    update_1(1)

    @pl.when(c == 1)
    def _():
        u_half(0)

    s_0(0)

    @pl.when(c == 0)
    def _():
        u_half(0)
        merge(0)

    s_0(1)

    def out_part(g, u, core):
        return out.at[pl.ds(u * HALF, HALF), pl.ds(pl.multiple_of((2 * g + core) * HALF, HALF), HALF)]

    def z_part(g, u, rho):
        return zst.at[g, u, pl.ds(pl.multiple_of(rho * HALF, HALF), HALF), :]

    def out_local(g, u):
        return pltpu.make_async_copy(z_part(g, u, c), out_part(g, u, c), out_sem.at[g * NU + u])

    def out_sib(g, u):
        return remote(z_part(g, u, 1 - c), out_part(g, u, c), outs_sem.at[g * NU + u], outr_sem.at[g * NU + u], sib)

    def out_from_sib(g, u):
        part = out_part(g, u, 1 - c)
        return remote(part, part, outs_sem.at[g * NU + u], outr_sem.at[g * NU + u], sib)

    for g in range(2):
        weights(g, 0)

        def last(u, g=g):
            update(g, 0, u)
            zst[g, u] = zt[g, :, cols(u)].T

        _units(0, NU, last)
        for u in range(NU):
            out_local(g, u).start()
            out_sib(g, u).start()

    half_copy.wait_send()
    t_copy(0).wait_send()
    for b in range(NB):
        v_y(b, y).wait_send()
        v_own(b, c).wait_send()
        v_fwd(b, c).wait_send()
        z_chunk(b // 4, b % 4, x).wait_send()
    for g in range(2):
        for u in range(NU):
            out_local(g, u).wait()
            out_sib(g, u).wait_send()
            out_from_sib(g, u).wait_recv()


def solution(mesh):
    def local_run(z_cols, v_local, t_local):
        f32 = jnp.float32
        any_spec = pl.BlockSpec(memory_space=pl.ANY)
        dma = pltpu.SemaphoreType.DMA
        return pl.pallas_call(
            _kernel,
            out_shape=jax.ShapeDtypeStruct((ROWS, 4 * HALF), f32),
            in_specs=[any_spec] * 3,
            out_specs=any_spec,
            scratch_shapes=[
                pltpu.VMEM((2 * VU * HALF, TILE), f32),
                pltpu.VMEM((TILE, 2 * ROWS), f32),
                pltpu.VMEM((2, HALF, 2 * ROWS), f32),
                pltpu.VMEM((2, NU, TILE, HALF), f32),
                pltpu.VMEM((W, W, NB * 8), f32),
                pltpu.VMEM((NB * 8 * PITCH, W), f32),
                pltpu.VMEM((2, HALF, TILE), f32),
                pltpu.VMEM((2, 2, HALF, TILE), f32),
                pltpu.VMEM((HALF, TILE), f32),
                pltpu.VMEM((HALF, TILE), f32),
                pltpu.VMEM((2, HALF, HALF), f32),
                pltpu.VMEM((4, HALF, HALF), f32),
                pltpu.VMEM((HALF, HALF), f32),
                pltpu.VMEM((2, HALF, HALF), f32),
                pltpu.VMEM((4, TILE, TILE), f32),
                *[dma((NB,))] * 9,
                dma((2,)), dma((2, 2)), dma((2,)), dma((4,)), dma, dma, dma, dma((4,)), dma, *[dma((2 * NU,))] * 4,
            ],
            compiler_params=pltpu.CompilerParams(collective_id=0, has_side_effects=True, vmem_limit_bytes=63 * 2**20),
            name="backtransform",
        )(z_cols, v_local, t_local.transpose(1, 2, 0))

    return jax.shard_map(
        local_run,
        mesh=mesh,
        in_specs=(P("kpt", ("col", "row")), P(("kpt", "row"), "col"), P("kpt", None, None)),
        out_specs=P(("kpt", "row"), "col"),
        check_vma=False,
    )
```

```python
import jax
import jax.numpy as jnp
from jax import lax
from jax.experimental import pallas as pl
from jax.experimental.pallas import tpu as pltpu
from jax.sharding import PartitionSpec as P

PRECISE = lax.Precision.HIGHEST
MESH = pl.DeviceIdType.MESH

W = 32
ROWS = 1536
TILE = 256
HALF = 128
NT = ROWS // TILE
NU = ROWS // HALF
NB = 24
VU = 2 * sum(range(1, NU + 1))
PITCH = 40
AHEAD = 12


def _dot(a, b, ca, cb):
    return lax.dot_general(a, b, (((ca,), (cb,)), ((), ())), precision=PRECISE, preferred_element_type=jnp.float32)


def _base(b):
    p = b // 2
    return 2 * NU * p - p * (p - 1) + (b % 2) * (NU - p)


def _panel(idx):
    return jnp.where(idx < HALF, 2 * (idx // W), 2 * ((idx - HALF) // W) + 1)


def _units(lo, n, body, end=None):
    def six(h, carry):
        for u in range(6):
            body(lo + 6 * h + u)
        return carry

    lax.fori_loop(0, n // 6, six, 0)
    for rest in range(6):
        if rest or end:

            @pl.when(n % 6 == rest)
            def _(rest=rest):
                for u in range(rest):
                    body(lo + n - rest + u)
                if end:
                    end()


def _kernel(z_in, v_in, t_in, out, vbuf, vtr, zt, zst, t_raw, tt, acc, srecv, wbuf, gacc, usend, urecv, uhalf, upack, tbuf,
            loc_sem, ys_sem, yr_sem, os_sem, or_sem, fs_sem, fr_sem, zs_sem, zr_sem,
            ss_sem, sr_sem, us_sem, ur_sem, hs_sem, hr_sem, ts_sem, tr_sem, tt_sem, zo_sem, out_sem, outs_sem, outr_sem):
    ridx = lax.axis_index("row")
    y = lax.axis_index("col")
    x, c = ridx // 2, ridx % 2
    xn = {"row": (ridx + 2) % 4}
    sib = {"row": ridx + 1 - 2 * c}
    yn = {"col": 1 - y}

    barrier = pltpu.get_barrier_semaphore()
    for dev in (xn, sib, yn):
        pl.semaphore_signal(barrier, inc=1, device_id=dev, device_id_type=MESH)

    def remote(src, dst, send, recv, dev):
        return pltpu.make_async_remote_copy(src, dst, send, recv, device_id=dev, device_id_type=MESH)

    def slab(b, rho, par):
        start = (rho * VU + _base(b)) * HALF + 64 * (b % 2)
        return vbuf.at[pl.ds(pl.multiple_of(start, 64), ROWS - 64 * b), pl.ds(pl.multiple_of(par * HALF, HALF), HALF)]

    def v_local(b):
        return pltpu.make_async_copy(v_in.at[pl.ds(64 * b, ROWS - 64 * b), pl.ds(HALF * b, HALF)], slab(b, c, y), loc_sem.at[b])

    def v_y(b, par):
        return remote(slab(b, c, par), slab(b, c, par), ys_sem.at[b], yr_sem.at[b], yn)

    def v_own(b, rho):
        return remote(slab(b, rho, y), slab(b, rho, y), os_sem.at[b], or_sem.at[b], sib)

    def v_fwd(b, rho):
        return remote(slab(b, rho, 1 - y), slab(b, rho, 1 - y), fs_sem.at[b], fr_sem.at[b], sib)

    def v_issue(b):
        v_local(b).wait()
        v_y(b, y).start()
        v_own(b, c).start()

    def static_block(b, fn, low=0, high=NB):
        if high - low == 1:
            fn(low)
            return
        mid = (low + high) // 2
        lax.cond(b < mid, lambda: static_block(b, fn, low, mid), lambda: static_block(b, fn, mid, high))

    def z_own(u, rho):
        return pltpu.make_async_copy(
            z_in.at[pl.ds(pl.multiple_of((2 * x + rho) * ROWS + u * HALF, HALF), HALF), :],
            zst.at[x, u, pl.ds(rho * HALF, HALF), :], zo_sem.at[2 * u + rho])

    def z_chunk(t, j, g):
        src = (2 * (1 - x) + j // 2) * ROWS + t * TILE + (j % 2) * HALF
        return remote(
            z_in.at[pl.ds(pl.multiple_of(src, HALF), HALF), :],
            zst.at[g, 2 * t + j % 2, pl.ds(pl.multiple_of((j // 2) * HALF, HALF), HALF), :],
            zs_sem.at[4 * t + j], zr_sem.at[4 * t + j], xn)

    t_copy_in = pltpu.make_async_copy(t_in, t_raw, tt_sem)

    for b in range(NB - 1, NB - 5, -1):
        v_local(b).start()
    t_copy_in.start()
    for u in range(NU - 1, -1, -1):
        for rho in range(2):
            z_own(u, rho).start()
    for b in range(NB - 5, -1, -1):
        v_local(b).start()
    for b in range(NB):
        if b % 2:
            for rho in range(2):
                vbuf[pl.ds((rho * VU + _base(b)) * HALF, 64), :] = jnp.zeros((64, TILE), jnp.float32)

    pl.semaphore_wait(barrier, 3)
    for b in range(NB - 1, NB - 1 - AHEAD, -1):
        v_issue(b)
        if b == NB - 2:
            for j in range(4):
                z_chunk(NT - 1, j, x).start()

    def rows(b, u, rho):
        return pl.ds(pl.multiple_of((rho * VU + _base(b) + u - b // 2) * HALF, HALF), HALF)

    def v_unit(b, u):
        return jnp.concatenate([vbuf[rows(b, u, rho), :] for rho in range(2)], axis=0)

    def cols(u):
        return pl.ds(pl.multiple_of(u * TILE, TILE), TILE)

    def s_copy(g, b):
        return remote(acc.at[g], srecv.at[g, b % 2], ss_sem.at[g], sr_sem.at[g, b % 2], xn)

    def weights(g, b):
        if g == 0:

            @pl.when(b % 2 != c)
            def _():
                t_copy(b).wait_recv()

        s_copy(g, b).wait_recv()
        s_sum = acc[g] + srecv[g, b % 2]
        wbuf[...] = _dot(s_sum, tbuf[b % 4], 1, 0)
        s_copy(g, b).wait_send()

    def update(g, b, u):
        if g == 0:
            v_tr = v_unit(b, u).T
            vtr[:, cols(u)] = v_tr
        else:
            v_tr = vtr[:, cols(u)]
        zt[g, :, cols(u)] = zt[g, :, cols(u)] - _dot(wbuf[...], v_tr, 1, 0)

    def partial_s(g, b, u):
        acc[g] += _dot(zt[g, :, cols(u)], v_unit(b, u), 1, 0)

    def sweep(g, k):
        @pl.when(k < NB - 1)
        def _():
            weights(g, k + 1)

        acc[g] = jnp.zeros((HALF, TILE), jnp.float32)
        first = (k + 1) // 2
        late = 1 - k % 2

        @pl.when(late == 1)
        def _():
            update(g, k + 1, first)

        def both(u):
            partial_s(g, k, u - 1)
            update(g, k + 1, u)

        _units(first + late, NU - first - late, both, lambda: partial_s(g, k, NU - 1))
        s_copy(g, k).start()

    ra = lax.broadcasted_iota(jnp.int32, (HALF, HALF), 0) // W
    rb = lax.broadcasted_iota(jnp.int32, (HALF, HALF), 1) // W

    def u_copy(b):
        return remote(usend.at[b % 2], urecv.at[b % 4], us_sem.at[b % 2], ur_sem.at[b % 4], xn)

    half_copy = remote(uhalf, upack.at[c], hs_sem, hr_sem, sib)

    def t_copy(b):
        return remote(tbuf.at[b % 4], tbuf.at[b % 4], ts_sem, tr_sem.at[b % 4], sib)

    def gram(b):
        def unit(u):
            own = jnp.concatenate(
                [vbuf[rows(b, u, rho), pl.ds(pl.multiple_of(c * HALF, HALF), HALF)] for rho in range(2)], axis=0)
            gacc[...] += _dot(own, v_unit(b, u), 0, 0)

        gacc[...] = jnp.zeros((HALF, TILE), jnp.float32)
        _units(b // 2, NU - b // 2, unit)

        def cols_of(par):
            return gacc[:, pl.ds(pl.multiple_of(par * HALF, HALF), HALF)]

        usend[b % 2] = jnp.where(ra <= rb, cols_of(1 - c), cols_of(c))
        u_copy(b).start()

    def u_half(b):
        u_copy(b).wait()
        total = usend[b % 2] + urecv[b % 4]

        @pl.when(b % 2 == c)
        def _():
            upack[c] = total

        @pl.when(b % 2 != c)
        def _():
            @pl.when(b < NB - 2)
            def _():
                half_copy.wait_send()

            uhalf[...] = total
            half_copy.start()

    def merge(b):
        half_copy.wait_recv()
        slot = b % 4

        @pl.when(b < NB - 2)
        def _():
            t_copy(b).wait_send()

        same = ra == rb

        def diagonal(par):
            at = [pl.multiple_of((8 * b + 2 * i + par) * PITCH, 8) for i in range(4)]
            stack = jnp.concatenate([tt[pl.ds(row, W), :] for row in at], axis=0)
            return jnp.where(same, jnp.concatenate([stack] * 4, axis=1), 0.0).T

        lo, hi = slice(0, HALF // 2), slice(HALF // 2, HALF)
        even_part, odd_part = upack[0], upack[1]
        ee, oo = jnp.where(ra > rb, even_part, 0.0), jnp.where(ra > rb, odd_part, 0.0)
        oe, eo = jnp.where(ra <= rb, even_part, 0.0).T, jnp.where(ra < rb, odd_part, 0.0).T

        def quad(a, b_, c_, d, rows_, cols_):
            return jnp.concatenate([
                jnp.concatenate([a[rows_, cols_], b_[rows_, cols_]], axis=1),
                jnp.concatenate([c_[rows_, cols_], d[rows_, cols_]], axis=1)], axis=0)

        even, odd = diagonal(0), diagonal(1)
        cross = -_dot(_dot(odd, jnp.where(same, oe, 0.0), 1, 0), even, 1, 0)
        zero = jnp.zeros((HALF, HALF), jnp.float32)
        pa, pb = ra % 2, rb % 2
        t_diag = []
        for part in (lo, hi):
            t_now = quad(even, zero, cross, odd, part, part)
            u_now = jnp.where(pa > pb, quad(ee, eo, oe, oo, part, part), 0.0)
            t_diag.append(t_now - _dot(_dot(t_now, u_now, 1, 0), t_now, 1, 0))
        t_lo, t_hi = t_diag
        t_off = -_dot(_dot(t_hi, quad(ee, eo, oe, oo, hi, lo), 1, 0), t_lo, 1, 0)
        half0 = jnp.zeros((HALF // 2, HALF // 2), jnp.float32)
        for rows_, out_rows in ((lo, 0), (hi, HALF)):
            tbuf[slot, out_rows : out_rows + HALF // 2, :] = jnp.concatenate(
                [t_lo[rows_, lo], half0, t_lo[rows_, hi], half0], axis=1)
            tbuf[slot, out_rows + HALF // 2 : out_rows + HALF, :] = jnp.concatenate(
                [t_off[rows_, lo], t_hi[rows_, lo], t_off[rows_, hi], t_hi[rows_, hi]], axis=1)
        t_copy(b).start()

    def t_layout():
        t_copy_in.wait()

        def t_row(i, carry):
            tt[pl.ds(i, NB * 8, stride=PITCH), :] = t_raw[i].T
            return carry

        lax.fori_loop(0, W, t_row, 0)

    def z_send(n):
        z_chunk((19 - n) // 4, n % 4, x).start()

    def forward(b):
        v_y(b, 1 - y).wait_recv()
        v_fwd(b, c).start()

    def arrived(b):
        v_own(b, 1 - c).wait_recv()
        v_fwd(b, 1 - c).wait_recv()

    def step(s, carry):
        k = NB + 1 - s
        b_sweep = jnp.where(k == NB, NB - 1, k)
        sweeps = (k < NB - 1) | (k == NB)
        b_in, takes_in = jnp.where(k >= 4, k - 2, k - 1), (k >= 2) & (k != 3)
        b_merge, merges = jnp.where(k >= 3, k - 1, k), (k <= NB) & (k != 2)

        @pl.when(sweeps)
        def _():
            @pl.when(b_sweep % 4 == 3)
            def _():
                for j in range(4):
                    z_chunk(b_sweep // 4, j, 1 - x).wait_recv()
                for h in range(2):
                    u = 2 * (b_sweep // 4) + h
                    for rho in range(2):
                        z_own(u, rho).wait()
                    for g in range(2):
                        zt[g, :, cols(u)] = zst[g, u].T

            sweep(0, b_sweep)

        @pl.when(takes_in)
        def _():
            static_block(b_in, forward)

        @pl.when(merges & (b_merge % 2 != c))
        def _():
            u_half(b_merge)

        @pl.when(sweeps)
        def _():
            sweep(1, b_sweep)

        @pl.when((k >= AHEAD) & (k < NB))
        def _():
            static_block(k - AHEAD, v_issue)

        @pl.when(takes_in)
        def _():
            static_block(b_in, arrived)
            gram(b_in)

        @pl.when(k >= 18)
        def _():
            z_send(25 - k)

        @pl.when((k <= 16) & (k >= 5))
        def _():
            z_send(24 - k)

        @pl.when(k == NB + 1)
        def _():
            t_layout()

        @pl.when(merges & (b_merge % 2 == c))
        def _():
            u_half(b_merge)
            merge(b_merge)

        return carry

    lax.fori_loop(0, NB + 1, step, 0)

    def update_1(g):
        weights(g, 1)
        _units(0, NU, lambda u: update(g, 1, u))

    def s_0(g):
        acc[g] = jnp.zeros((HALF, TILE), jnp.float32)
        _units(0, NU, lambda u: partial_s(g, 0, u))
        s_copy(g, 0).start()

    def gram_0(core):
        @pl.when(c == core)
        def _():
            arrived(0)
            gram(0)

    forward(0)
    gram_0(1)
    update_1(0)
    gram_0(0)
    s_0(0)

    @pl.when(c == 1)
    def _():
        u_half(0)

    update_1(1)
    s_0(1)

    @pl.when(c == 0)
    def _():
        u_half(0)
        merge(0)

    def out_part(g, u, core):
        return out.at[pl.ds(u * HALF, HALF), pl.ds(pl.multiple_of((2 * g + core) * HALF, HALF), HALF)]

    def z_part(g, u, rho):
        return zst.at[g, u, pl.ds(pl.multiple_of(rho * HALF, HALF), HALF), :]

    def out_local(g, u):
        return pltpu.make_async_copy(z_part(g, u, c), out_part(g, u, c), out_sem.at[g * NU + u])

    def out_sib(g, u):
        return remote(z_part(g, u, 1 - c), out_part(g, u, c), outs_sem.at[g * NU + u], outr_sem.at[g * NU + u], sib)

    def out_from_sib(g, u):
        part = out_part(g, u, 1 - c)
        return remote(part, part, outs_sem.at[g * NU + u], outr_sem.at[g * NU + u], sib)

    for g in range(2):
        weights(g, 0)

        def last(u, g=g):
            update(g, 0, u)
            zst[g, u] = zt[g, :, cols(u)].T

        _units(0, NU, last)
        for u in range(NU):
            out_local(g, u).start()
            out_sib(g, u).start()

    half_copy.wait_send()
    t_copy(0).wait_send()
    for b in range(NB):
        v_y(b, y).wait_send()
        v_own(b, c).wait_send()
        v_fwd(b, c).wait_send()
        z_chunk(b // 4, b % 4, x).wait_send()
    for g in range(2):
        for u in range(NU):
            out_local(g, u).wait()
            out_sib(g, u).wait_send()
            out_from_sib(g, u).wait_recv()


def solution(mesh):
    def local_run(z_cols, v_local, t_local):
        f32 = jnp.float32
        any_spec = pl.BlockSpec(memory_space=pl.ANY)
        dma = pltpu.SemaphoreType.DMA
        return pl.pallas_call(
            _kernel,
            out_shape=jax.ShapeDtypeStruct((ROWS, 4 * HALF), f32),
            in_specs=[any_spec] * 3,
            out_specs=any_spec,
            scratch_shapes=[
                pltpu.VMEM((2 * VU * HALF, TILE), f32),
                pltpu.VMEM((TILE, 2 * ROWS), f32),
                pltpu.VMEM((2, HALF, 2 * ROWS), f32),
                pltpu.VMEM((2, NU, TILE, HALF), f32),
                pltpu.VMEM((W, W, NB * 8), f32),
                pltpu.VMEM((NB * 8 * PITCH, W), f32),
                pltpu.VMEM((2, HALF, TILE), f32),
                pltpu.VMEM((2, 2, HALF, TILE), f32),
                pltpu.VMEM((HALF, TILE), f32),
                pltpu.VMEM((HALF, TILE), f32),
                pltpu.VMEM((2, HALF, HALF), f32),
                pltpu.VMEM((4, HALF, HALF), f32),
                pltpu.VMEM((HALF, HALF), f32),
                pltpu.VMEM((2, HALF, HALF), f32),
                pltpu.VMEM((4, TILE, TILE), f32),
                *[dma((NB,))] * 9,
                dma((2,)), dma((2, 2)), dma((2,)), dma((4,)), dma, dma, dma, dma((4,)), dma, *[dma((2 * NU,))] * 4,
            ],
            compiler_params=pltpu.CompilerParams(collective_id=0, has_side_effects=True, vmem_limit_bytes=63 * 2**20),
            name="backtransform",
        )(z_cols, v_local, t_local.transpose(1, 2, 0))

    return jax.shard_map(
        local_run,
        mesh=mesh,
        in_specs=(P("kpt", ("col", "row")), P(("kpt", "row"), "col"), P("kpt", None, None)),
        out_specs=P(("kpt", "row"), "col"),
        check_vma=False,
    )
```

```python
import jax
import jax.numpy as jnp
from jax import lax
from jax.experimental import pallas as pl
from jax.experimental.pallas import tpu as pltpu
from jax.sharding import PartitionSpec as P

PRECISE = lax.Precision.HIGHEST
MESH = pl.DeviceIdType.MESH

W = 32
ROWS = 1536
TILE = 256
HALF = 128
NT = ROWS // TILE
NU = ROWS // HALF
NB = 24
VU = 2 * sum(range(1, NU + 1))
PITCH = 40
AHEAD = 12


def _dot(a, b, ca, cb):
    return lax.dot_general(a, b, (((ca,), (cb,)), ((), ())), precision=PRECISE, preferred_element_type=jnp.float32)


def _base(b):
    p = b // 2
    return 2 * NU * p - p * (p - 1) + (b % 2) * (NU - p)


def _panel(idx):
    return jnp.where(idx < HALF, 2 * (idx // W), 2 * ((idx - HALF) // W) + 1)


def _units(lo, n, body, end=None):
    def six(h, carry):
        for u in range(6):
            body(lo + 6 * h + u)
        return carry

    lax.fori_loop(0, n // 6, six, 0)
    for rest in range(6):
        if rest or end:

            @pl.when(n % 6 == rest)
            def _(rest=rest):
                for u in range(rest):
                    body(lo + n - rest + u)
                if end:
                    end()


def _kernel(z_in, v_in, t_in, out, vbuf, vtr, zt, zst, t_raw, tt, acc, srecv, wbuf, gacc, usend, urecv, uhalf, upack, tbuf,
            loc_sem, ys_sem, yr_sem, os_sem, or_sem, fs_sem, fr_sem, zs_sem, zr_sem,
            ss_sem, sr_sem, us_sem, ur_sem, hs_sem, hr_sem, ts_sem, tr_sem, tt_sem, zo_sem, out_sem, outs_sem, outr_sem):
    ridx = lax.axis_index("row")
    y = lax.axis_index("col")
    x, c = ridx // 2, ridx % 2
    xn = {"row": (ridx + 2) % 4}
    sib = {"row": ridx + 1 - 2 * c}
    yn = {"col": 1 - y}

    barrier = pltpu.get_barrier_semaphore()
    for dev in (xn, sib, yn):
        pl.semaphore_signal(barrier, inc=1, device_id=dev, device_id_type=MESH)

    def remote(src, dst, send, recv, dev):
        return pltpu.make_async_remote_copy(src, dst, send, recv, device_id=dev, device_id_type=MESH)

    def slab(b, rho, par):
        start = (rho * VU + _base(b)) * HALF + 64 * (b % 2)
        return vbuf.at[pl.ds(pl.multiple_of(start, 64), ROWS - 64 * b), pl.ds(pl.multiple_of(par * HALF, HALF), HALF)]

    def v_local(b):
        return pltpu.make_async_copy(v_in.at[pl.ds(64 * b, ROWS - 64 * b), pl.ds(HALF * b, HALF)], slab(b, c, y), loc_sem.at[b])

    def v_y(b, par):
        return remote(slab(b, c, par), slab(b, c, par), ys_sem.at[b], yr_sem.at[b], yn)

    def v_own(b, rho):
        return remote(slab(b, rho, y), slab(b, rho, y), os_sem.at[b], or_sem.at[b], sib)

    def v_fwd(b, rho):
        return remote(slab(b, rho, 1 - y), slab(b, rho, 1 - y), fs_sem.at[b], fr_sem.at[b], sib)

    def v_issue(b):
        v_local(b).wait()
        v_y(b, y).start()
        v_own(b, c).start()

    def static_block(b, fn, low=0, high=NB):
        if high - low == 1:
            fn(low)
            return
        mid = (low + high) // 2
        lax.cond(b < mid, lambda: static_block(b, fn, low, mid), lambda: static_block(b, fn, mid, high))

    def z_own(u, rho):
        return pltpu.make_async_copy(
            z_in.at[pl.ds(pl.multiple_of((2 * x + rho) * ROWS + u * HALF, HALF), HALF), :],
            zst.at[x, u, pl.ds(rho * HALF, HALF), :], zo_sem.at[2 * u + rho])

    def z_chunk(t, j, g):
        src = (2 * (1 - x) + j // 2) * ROWS + t * TILE + (j % 2) * HALF
        return remote(
            z_in.at[pl.ds(pl.multiple_of(src, HALF), HALF), :],
            zst.at[g, 2 * t + j % 2, pl.ds(pl.multiple_of((j // 2) * HALF, HALF), HALF), :],
            zs_sem.at[4 * t + j], zr_sem.at[4 * t + j], xn)

    t_copy_in = pltpu.make_async_copy(t_in, t_raw, tt_sem)

    for b in range(NB - 1, NB - 5, -1):
        v_local(b).start()
    t_copy_in.start()
    for u in range(NU - 1, -1, -1):
        for rho in range(2):
            z_own(u, rho).start()
    for b in range(NB - 5, -1, -1):
        v_local(b).start()
    for b in range(NB):
        if b % 2:
            for rho in range(2):
                vbuf[pl.ds((rho * VU + _base(b)) * HALF, 64), :] = jnp.zeros((64, TILE), jnp.float32)

    pl.semaphore_wait(barrier, 3)
    for b in range(NB - 1, NB - 1 - AHEAD, -1):
        v_issue(b)
        if b == NB - 2:
            for j in range(4):
                z_chunk(NT - 1, j, x).start()

    def rows(b, u, rho):
        return pl.ds(pl.multiple_of((rho * VU + _base(b) + u - b // 2) * HALF, HALF), HALF)

    def v_unit(b, u):
        return jnp.concatenate([vbuf[rows(b, u, rho), :] for rho in range(2)], axis=0)

    def cols(u):
        return pl.ds(pl.multiple_of(u * TILE, TILE), TILE)

    def s_copy(g, b):
        return remote(acc.at[g], srecv.at[g, b % 2], ss_sem.at[g], sr_sem.at[g, b % 2], xn)

    def weights(g, b):
        if g == 0:

            @pl.when(b % 2 != c)
            def _():
                t_copy(b).wait_recv()

        s_copy(g, b).wait_recv()
        s_sum = acc[g] + srecv[g, b % 2]
        wbuf[...] = _dot(s_sum, tbuf[b % 4], 1, 0)
        s_copy(g, b).wait_send()

    def update(g, b, u):
        if g == 0:
            v_tr = v_unit(b, u).T
            vtr[:, cols(u)] = v_tr
        else:
            v_tr = vtr[:, cols(u)]
        zt[g, :, cols(u)] = zt[g, :, cols(u)] - _dot(wbuf[...], v_tr, 1, 0)

    def partial_s(g, b, u):
        acc[g] += _dot(zt[g, :, cols(u)], v_unit(b, u), 1, 0)

    def sweep(g, k):
        @pl.when(k < NB - 1)
        def _():
            weights(g, k + 1)

        acc[g] = jnp.zeros((HALF, TILE), jnp.float32)
        first = (k + 1) // 2
        late = 1 - k % 2

        @pl.when(late == 1)
        def _():
            update(g, k + 1, first)

        def both(u):
            partial_s(g, k, u - 1)
            update(g, k + 1, u)

        _units(first + late, NU - first - late, both, lambda: partial_s(g, k, NU - 1))
        s_copy(g, k).start()

    ra = lax.broadcasted_iota(jnp.int32, (HALF, HALF), 0) // W
    rb = lax.broadcasted_iota(jnp.int32, (HALF, HALF), 1) // W

    def u_copy(b):
        return remote(usend.at[b % 2], urecv.at[b % 4], us_sem.at[b % 2], ur_sem.at[b % 4], xn)

    half_copy = remote(uhalf, upack.at[c], hs_sem, hr_sem, sib)

    def t_copy(b):
        return remote(tbuf.at[b % 4], tbuf.at[b % 4], ts_sem, tr_sem.at[b % 4], sib)

    def gram(b):
        def unit(u):
            own = jnp.concatenate(
                [vbuf[rows(b, u, rho), pl.ds(pl.multiple_of(c * HALF, HALF), HALF)] for rho in range(2)], axis=0)
            gacc[...] += _dot(own, v_unit(b, u), 0, 0)

        gacc[...] = jnp.zeros((HALF, TILE), jnp.float32)
        _units(b // 2, NU - b // 2, unit)

        def cols_of(par):
            return gacc[:, pl.ds(pl.multiple_of(par * HALF, HALF), HALF)]

        usend[b % 2] = jnp.where(ra <= rb, cols_of(1 - c), cols_of(c))
        u_copy(b).start()

    def u_half(b):
        u_copy(b).wait()
        total = usend[b % 2] + urecv[b % 4]

        @pl.when(b % 2 == c)
        def _():
            upack[c] = total

        @pl.when(b % 2 != c)
        def _():
            @pl.when(b < NB - 2)
            def _():
                half_copy.wait_send()

            uhalf[...] = total
            half_copy.start()

    def merge(b):
        half_copy.wait_recv()
        slot = b % 4

        @pl.when(b < NB - 2)
        def _():
            t_copy(b).wait_send()

        same = ra == rb

        def diagonal(par):
            at = [pl.multiple_of((8 * b + 2 * i + par) * PITCH, 8) for i in range(4)]
            stack = jnp.concatenate([tt[pl.ds(row, W), :] for row in at], axis=0)
            return jnp.where(same, jnp.concatenate([stack] * 4, axis=1), 0.0).T

        lo, hi = slice(0, HALF // 2), slice(HALF // 2, HALF)
        even_part, odd_part = upack[0], upack[1]
        ee, oo = jnp.where(ra > rb, even_part, 0.0), jnp.where(ra > rb, odd_part, 0.0)
        oe, eo = jnp.where(ra <= rb, even_part, 0.0).T, jnp.where(ra < rb, odd_part, 0.0).T

        def quad(a, b_, c_, d, rows_, cols_):
            return jnp.concatenate([
                jnp.concatenate([a[rows_, cols_], b_[rows_, cols_]], axis=1),
                jnp.concatenate([c_[rows_, cols_], d[rows_, cols_]], axis=1)], axis=0)

        even, odd = diagonal(0), diagonal(1)
        cross = -_dot(_dot(odd, jnp.where(same, oe, 0.0), 1, 0), even, 1, 0)
        zero = jnp.zeros((HALF, HALF), jnp.float32)
        pa, pb = ra % 2, rb % 2
        t_diag = []
        for part in (lo, hi):
            t_now = quad(even, zero, cross, odd, part, part)
            u_now = jnp.where(pa > pb, quad(ee, eo, oe, oo, part, part), 0.0)
            t_diag.append(t_now - _dot(_dot(t_now, u_now, 1, 0), t_now, 1, 0))
        t_lo, t_hi = t_diag
        t_off = -_dot(_dot(t_hi, quad(ee, eo, oe, oo, hi, lo), 1, 0), t_lo, 1, 0)
        half0 = jnp.zeros((HALF // 2, HALF // 2), jnp.float32)
        for rows_, out_rows in ((lo, 0), (hi, HALF)):
            tbuf[slot, out_rows : out_rows + HALF // 2, :] = jnp.concatenate(
                [t_lo[rows_, lo], half0, t_lo[rows_, hi], half0], axis=1)
            tbuf[slot, out_rows + HALF // 2 : out_rows + HALF, :] = jnp.concatenate(
                [t_off[rows_, lo], t_hi[rows_, lo], t_off[rows_, hi], t_hi[rows_, hi]], axis=1)
        t_copy(b).start()

    def t_layout():
        t_copy_in.wait()

        def t_row(i, carry):
            tt[pl.ds(i, NB * 8, stride=PITCH), :] = t_raw[i].T
            return carry

        lax.fori_loop(0, W, t_row, 0)

    def z_send(n):
        z_chunk((19 - n) // 4, n % 4, x).start()

    def forward(b):
        v_y(b, 1 - y).wait_recv()
        v_fwd(b, c).start()

    def arrived(b):
        v_own(b, 1 - c).wait_recv()
        v_fwd(b, 1 - c).wait_recv()

    def step(s, carry):
        k = NB + 1 - s
        b_sweep = jnp.where(k == NB, NB - 1, k)
        sweeps = (k < NB - 1) | (k == NB)
        b_in, takes_in = jnp.where(k >= 4, k - 2, k - 1), (k >= 2) & (k != 3)
        b_merge, merges = jnp.where(k >= 3, k - 1, k), (k <= NB) & (k != 2)

        @pl.when(sweeps)
        def _():
            @pl.when(b_sweep % 4 == 3)
            def _():
                for j in range(4):
                    z_chunk(b_sweep // 4, j, 1 - x).wait_recv()
                for h in range(2):
                    u = 2 * (b_sweep // 4) + h
                    for rho in range(2):
                        z_own(u, rho).wait()
                    for g in range(2):
                        zt[g, :, cols(u)] = zst[g, u].T

            sweep(0, b_sweep)

        @pl.when(takes_in)
        def _():
            static_block(b_in, forward)

        @pl.when(merges & (b_merge % 2 != c))
        def _():
            u_half(b_merge)

        @pl.when(sweeps)
        def _():
            sweep(1, b_sweep)

        @pl.when(k == 1)
        def _():
            forward(0)

        @pl.when((k >= AHEAD) & (k < NB))
        def _():
            static_block(k - AHEAD, v_issue)

        @pl.when(takes_in)
        def _():
            static_block(b_in, arrived)
            gram(b_in)

        @pl.when(k >= 18)
        def _():
            z_send(25 - k)

        @pl.when((k <= 16) & (k >= 5))
        def _():
            z_send(24 - k)

        @pl.when(k == NB + 1)
        def _():
            t_layout()

        @pl.when(merges & (b_merge % 2 == c))
        def _():
            u_half(b_merge)
            merge(b_merge)

        return carry

    lax.fori_loop(0, NB + 1, step, 0)

    def update_1(g):
        weights(g, 1)
        _units(0, NU, lambda u: update(g, 1, u))

    def s_0(g):
        acc[g] = jnp.zeros((HALF, TILE), jnp.float32)
        _units(0, NU, lambda u: partial_s(g, 0, u))
        s_copy(g, 0).start()

    def gram_0(core):
        @pl.when(c == core)
        def _():
            arrived(0)
            gram(0)

    gram_0(0)
    update_1(0)
    gram_0(1)
    s_0(0)
    update_1(1)

    @pl.when(c == 1)
    def _():
        u_half(0)

    s_0(1)

    @pl.when(c == 0)
    def _():
        u_half(0)
        merge(0)

    def out_part(g, u, core):
        return out.at[pl.ds(u * HALF, HALF), pl.ds(pl.multiple_of((2 * g + core) * HALF, HALF), HALF)]

    def z_part(g, u, rho):
        return zst.at[g, u, pl.ds(pl.multiple_of(rho * HALF, HALF), HALF), :]

    def out_local(g, u):
        return pltpu.make_async_copy(z_part(g, u, c), out_part(g, u, c), out_sem.at[g * NU + u])

    def out_sib(g, u):
        return remote(z_part(g, u, 1 - c), out_part(g, u, c), outs_sem.at[g * NU + u], outr_sem.at[g * NU + u], sib)

    def out_from_sib(g, u):
        part = out_part(g, u, 1 - c)
        return remote(part, part, outs_sem.at[g * NU + u], outr_sem.at[g * NU + u], sib)

    for g in range(2):
        weights(g, 0)

        def last(u, g=g):
            update(g, 0, u)
            zst[g, u] = zt[g, :, cols(u)].T

        _units(0, NU, last)
        for u in range(NU):
            out_local(g, u).start()
            out_sib(g, u).start()

    half_copy.wait_send()
    t_copy(0).wait_send()
    for b in range(NB):
        v_y(b, y).wait_send()
        v_own(b, c).wait_send()
        v_fwd(b, c).wait_send()
        z_chunk(b // 4, b % 4, x).wait_send()
    for g in range(2):
        for u in range(NU):
            out_local(g, u).wait()
            out_sib(g, u).wait_send()
            out_from_sib(g, u).wait_recv()


def solution(mesh):
    def local_run(z_cols, v_local, t_local):
        f32 = jnp.float32
        any_spec = pl.BlockSpec(memory_space=pl.ANY)
        dma = pltpu.SemaphoreType.DMA
        return pl.pallas_call(
            _kernel,
            out_shape=jax.ShapeDtypeStruct((ROWS, 4 * HALF), f32),
            in_specs=[any_spec] * 3,
            out_specs=any_spec,
            scratch_shapes=[
                pltpu.VMEM((2 * VU * HALF, TILE), f32),
                pltpu.VMEM((TILE, 2 * ROWS), f32),
                pltpu.VMEM((2, HALF, 2 * ROWS), f32),
                pltpu.VMEM((2, NU, TILE, HALF), f32),
                pltpu.VMEM((W, W, NB * 8), f32),
                pltpu.VMEM((NB * 8 * PITCH, W), f32),
                pltpu.VMEM((2, HALF, TILE), f32),
                pltpu.VMEM((2, 2, HALF, TILE), f32),
                pltpu.VMEM((HALF, TILE), f32),
                pltpu.VMEM((HALF, TILE), f32),
                pltpu.VMEM((2, HALF, HALF), f32),
                pltpu.VMEM((4, HALF, HALF), f32),
                pltpu.VMEM((HALF, HALF), f32),
                pltpu.VMEM((2, HALF, HALF), f32),
                pltpu.VMEM((4, TILE, TILE), f32),
                *[dma((NB,))] * 9,
                dma((2,)), dma((2, 2)), dma((2,)), dma((4,)), dma, dma, dma, dma((4,)), dma, *[dma((2 * NU,))] * 4,
            ],
            compiler_params=pltpu.CompilerParams(collective_id=0, has_side_effects=True, vmem_limit_bytes=63 * 2**20),
            name="backtransform",
        )(z_cols, v_local, t_local.transpose(1, 2, 0))

    return jax.shard_map(
        local_run,
        mesh=mesh,
        in_specs=(P("kpt", ("col", "row")), P(("kpt", "row"), "col"), P("kpt", None, None)),
        out_specs=P(("kpt", "row"), "col"),
        check_vma=False,
    )
```

```python
import jax
import jax.numpy as jnp
from jax import lax
from jax.experimental import pallas as pl
from jax.experimental.pallas import tpu as pltpu
from jax.sharding import PartitionSpec as P

PRECISE = lax.Precision.HIGHEST
MESH = pl.DeviceIdType.MESH

W = 32
ROWS = 1536
TILE = 256
HALF = 128
NT = ROWS // TILE
NU = ROWS // HALF
NB = 24
VU = 2 * sum(range(1, NU + 1))
PITCH = 40
AHEAD = 12


def _dot(a, b, ca, cb):
    return lax.dot_general(a, b, (((ca,), (cb,)), ((), ())), precision=PRECISE, preferred_element_type=jnp.float32)


def _base(b):
    p = b // 2
    return 2 * NU * p - p * (p - 1) + (b % 2) * (NU - p)


def _panel(idx):
    return jnp.where(idx < HALF, 2 * (idx // W), 2 * ((idx - HALF) // W) + 1)


def _units(lo, n, body, end=None):
    def six(h, carry):
        for u in range(6):
            body(lo + 6 * h + u)
        return carry

    lax.fori_loop(0, n // 6, six, 0)
    for rest in range(6):
        if rest or end:

            @pl.when(n % 6 == rest)
            def _(rest=rest):
                for u in range(rest):
                    body(lo + n - rest + u)
                if end:
                    end()


def _kernel(z_in, v_in, t_in, out, vbuf, vtr, zt, zst, t_raw, tt, acc, srecv, wbuf, gacc, usend, urecv, uhalf, upack, tbuf,
            loc_sem, ys_sem, yr_sem, os_sem, or_sem, fs_sem, fr_sem, zs_sem, zr_sem,
            ss_sem, sr_sem, us_sem, ur_sem, hs_sem, hr_sem, ts_sem, tr_sem, tt_sem, zo_sem, out_sem, outs_sem, outr_sem):
    ridx = lax.axis_index("row")
    y = lax.axis_index("col")
    x, c = ridx // 2, ridx % 2
    xn = {"row": (ridx + 2) % 4}
    sib = {"row": ridx + 1 - 2 * c}
    yn = {"col": 1 - y}

    barrier = pltpu.get_barrier_semaphore()
    for dev in (xn, sib, yn):
        pl.semaphore_signal(barrier, inc=1, device_id=dev, device_id_type=MESH)

    def remote(src, dst, send, recv, dev):
        return pltpu.make_async_remote_copy(src, dst, send, recv, device_id=dev, device_id_type=MESH)

    def slab(b, rho, par):
        start = (rho * VU + _base(b)) * HALF + 64 * (b % 2)
        return vbuf.at[pl.ds(pl.multiple_of(start, 64), ROWS - 64 * b), pl.ds(pl.multiple_of(par * HALF, HALF), HALF)]

    def v_local(b):
        return pltpu.make_async_copy(v_in.at[pl.ds(64 * b, ROWS - 64 * b), pl.ds(HALF * b, HALF)], slab(b, c, y), loc_sem.at[b])

    def v_y(b, par):
        return remote(slab(b, c, par), slab(b, c, par), ys_sem.at[b], yr_sem.at[b], yn)

    def v_own(b, rho):
        return remote(slab(b, rho, y), slab(b, rho, y), os_sem.at[b], or_sem.at[b], sib)

    def v_fwd(b, rho):
        return remote(slab(b, rho, 1 - y), slab(b, rho, 1 - y), fs_sem.at[b], fr_sem.at[b], sib)

    def v_issue(b):
        v_local(b).wait()
        v_y(b, y).start()
        v_own(b, c).start()

    def static_block(b, fn, low=0, high=NB):
        if high - low == 1:
            fn(low)
            return
        mid = (low + high) // 2
        lax.cond(b < mid, lambda: static_block(b, fn, low, mid), lambda: static_block(b, fn, mid, high))

    def z_own(u, rho):
        return pltpu.make_async_copy(
            z_in.at[pl.ds(pl.multiple_of((2 * x + rho) * ROWS + u * HALF, HALF), HALF), :],
            zst.at[x, u, pl.ds(rho * HALF, HALF), :], zo_sem.at[2 * u + rho])

    def z_chunk(t, j, g):
        src = (2 * (1 - x) + j // 2) * ROWS + t * TILE + (j % 2) * HALF
        return remote(
            z_in.at[pl.ds(pl.multiple_of(src, HALF), HALF), :],
            zst.at[g, 2 * t + j % 2, pl.ds(pl.multiple_of((j // 2) * HALF, HALF), HALF), :],
            zs_sem.at[4 * t + j], zr_sem.at[4 * t + j], xn)

    t_copy_in = pltpu.make_async_copy(t_in, t_raw, tt_sem)

    for b in range(NB - 1, NB - 5, -1):
        v_local(b).start()
    t_copy_in.start()
    for u in range(NU - 1, -1, -1):
        for rho in range(2):
            z_own(u, rho).start()
    for b in range(NB - 5, -1, -1):
        v_local(b).start()
    for b in range(NB):
        if b % 2:
            for rho in range(2):
                vbuf[pl.ds((rho * VU + _base(b)) * HALF, 64), :] = jnp.zeros((64, TILE), jnp.float32)

    pl.semaphore_wait(barrier, 3)
    for b in range(NB - 1, NB - 1 - AHEAD, -1):
        v_issue(b)
        if b == NB - 2:
            for j in range(4):
                z_chunk(NT - 1, j, x).start()

    def rows(b, u, rho):
        return pl.ds(pl.multiple_of((rho * VU + _base(b) + u - b // 2) * HALF, HALF), HALF)

    def v_unit(b, u):
        return jnp.concatenate([vbuf[rows(b, u, rho), :] for rho in range(2)], axis=0)

    def cols(u):
        return pl.ds(pl.multiple_of(u * TILE, TILE), TILE)

    def s_copy(g, b):
        return remote(acc.at[g], srecv.at[g, b % 2], ss_sem.at[g], sr_sem.at[g, b % 2], xn)

    def weights(g, b):
        if g == 0:

            @pl.when(b % 2 != c)
            def _():
                t_copy(b).wait_recv()

        s_copy(g, b).wait_recv()
        s_sum = acc[g] + srecv[g, b % 2]
        wbuf[...] = _dot(s_sum, tbuf[b % 4], 1, 0)
        s_copy(g, b).wait_send()

    def update(g, b, u):
        if g == 0:
            v_tr = v_unit(b, u).T
            vtr[:, cols(u)] = v_tr
        else:
            v_tr = vtr[:, cols(u)]
        zt[g, :, cols(u)] = zt[g, :, cols(u)] - _dot(wbuf[...], v_tr, 1, 0)

    def partial_s(g, b, u):
        acc[g] += _dot(zt[g, :, cols(u)], v_unit(b, u), 1, 0)

    def sweep(g, k):
        @pl.when(k < NB - 1)
        def _():
            weights(g, k + 1)

        acc[g] = jnp.zeros((HALF, TILE), jnp.float32)
        first = (k + 1) // 2
        late = 1 - k % 2

        @pl.when(late == 1)
        def _():
            update(g, k + 1, first)

        def both(u):
            partial_s(g, k, u - 1)
            update(g, k + 1, u)

        _units(first + late, NU - first - late, both, lambda: partial_s(g, k, NU - 1))
        s_copy(g, k).start()

    ra = lax.broadcasted_iota(jnp.int32, (HALF, HALF), 0) // W
    rb = lax.broadcasted_iota(jnp.int32, (HALF, HALF), 1) // W

    def u_copy(b):
        return remote(usend.at[b % 2], urecv.at[b % 4], us_sem.at[b % 2], ur_sem.at[b % 4], xn)

    half_copy = remote(uhalf, upack.at[c], hs_sem, hr_sem, sib)

    def t_copy(b):
        return remote(tbuf.at[b % 4], tbuf.at[b % 4], ts_sem, tr_sem.at[b % 4], sib)

    def gram(b):
        def unit(u):
            own = jnp.concatenate(
                [vbuf[rows(b, u, rho), pl.ds(pl.multiple_of(c * HALF, HALF), HALF)] for rho in range(2)], axis=0)
            gacc[...] += _dot(own, v_unit(b, u), 0, 0)

        gacc[...] = jnp.zeros((HALF, TILE), jnp.float32)
        _units(b // 2, NU - b // 2, unit)

        def cols_of(par):
            return gacc[:, pl.ds(pl.multiple_of(par * HALF, HALF), HALF)]

        usend[b % 2] = jnp.where(ra <= rb, cols_of(1 - c), cols_of(c))
        u_copy(b).start()

    def u_half(b):
        u_copy(b).wait()
        total = usend[b % 2] + urecv[b % 4]

        @pl.when(b % 2 == c)
        def _():
            upack[c] = total

        @pl.when(b % 2 != c)
        def _():
            @pl.when(b < NB - 2)
            def _():
                half_copy.wait_send()

            uhalf[...] = total
            half_copy.start()

    def merge(b):
        half_copy.wait_recv()
        slot = b % 4

        @pl.when(b < NB - 2)
        def _():
            t_copy(b).wait_send()

        same = ra == rb

        def diagonal(par):
            at = [pl.multiple_of((8 * b + 2 * i + par) * PITCH, 8) for i in range(4)]
            stack = jnp.concatenate([tt[pl.ds(row, W), :] for row in at], axis=0)
            return jnp.where(same, jnp.concatenate([stack] * 4, axis=1), 0.0).T

        lo, hi = slice(0, HALF // 2), slice(HALF // 2, HALF)
        even_part, odd_part = upack[0], upack[1]
        ee, oo = jnp.where(ra > rb, even_part, 0.0), jnp.where(ra > rb, odd_part, 0.0)
        oe, eo = jnp.where(ra <= rb, even_part, 0.0).T, jnp.where(ra < rb, odd_part, 0.0).T

        def quad(a, b_, c_, d, rows_, cols_):
            return jnp.concatenate([
                jnp.concatenate([a[rows_, cols_], b_[rows_, cols_]], axis=1),
                jnp.concatenate([c_[rows_, cols_], d[rows_, cols_]], axis=1)], axis=0)

        even, odd = diagonal(0), diagonal(1)
        cross = -_dot(_dot(odd, jnp.where(same, oe, 0.0), 1, 0), even, 1, 0)
        zero = jnp.zeros((HALF, HALF), jnp.float32)
        pa, pb = ra % 2, rb % 2
        t_diag = []
        for part in (lo, hi):
            t_now = quad(even, zero, cross, odd, part, part)
            u_now = jnp.where(pa > pb, quad(ee, eo, oe, oo, part, part), 0.0)
            t_diag.append(t_now - _dot(_dot(t_now, u_now, 1, 0), t_now, 1, 0))
        t_lo, t_hi = t_diag
        t_off = -_dot(_dot(t_hi, quad(ee, eo, oe, oo, hi, lo), 1, 0), t_lo, 1, 0)
        half0 = jnp.zeros((HALF // 2, HALF // 2), jnp.float32)
        for rows_, out_rows in ((lo, 0), (hi, HALF)):
            tbuf[slot, out_rows : out_rows + HALF // 2, :] = jnp.concatenate(
                [t_lo[rows_, lo], half0, t_lo[rows_, hi], half0], axis=1)
            tbuf[slot, out_rows + HALF // 2 : out_rows + HALF, :] = jnp.concatenate(
                [t_off[rows_, lo], t_hi[rows_, lo], t_off[rows_, hi], t_hi[rows_, hi]], axis=1)
        t_copy(b).start()

    def t_layout():
        t_copy_in.wait()

        def t_row(i, carry):
            tt[pl.ds(i, NB * 8, stride=PITCH), :] = t_raw[i].T
            return carry

        lax.fori_loop(0, W, t_row, 0)

    def z_send(n):
        z_chunk((19 - n) // 4, n % 4, x).start()

    def forward(b):
        v_y(b, 1 - y).wait_recv()
        v_fwd(b, c).start()

    def arrived(b):
        v_own(b, 1 - c).wait_recv()
        v_fwd(b, 1 - c).wait_recv()

    def step(s, carry):
        k = NB + 1 - s
        b_sweep = jnp.where(k == NB, NB - 1, k)
        sweeps = (k < NB - 1) | (k == NB)
        b_in, takes_in = jnp.where(k >= 4, k - 2, k - 1), (k >= 2) & (k != 3)
        b_merge, merges = jnp.where(k >= 3, k - 1, k), (k <= NB) & (k != 2)

        @pl.when(sweeps)
        def _():
            @pl.when(b_sweep % 4 == 3)
            def _():
                for j in range(4):
                    z_chunk(b_sweep // 4, j, 1 - x).wait_recv()
                for h in range(2):
                    u = 2 * (b_sweep // 4) + h
                    for rho in range(2):
                        z_own(u, rho).wait()
                    for g in range(2):
                        zt[g, :, cols(u)] = zst[g, u].T

            sweep(0, b_sweep)

        @pl.when(takes_in)
        def _():
            static_block(b_in, forward)

        @pl.when(merges & (b_merge % 2 != c))
        def _():
            u_half(b_merge)

        @pl.when(sweeps)
        def _():
            sweep(1, b_sweep)

        @pl.when(k == 1)
        def _():
            forward(0)

        @pl.when((k >= AHEAD) & (k < NB))
        def _():
            static_block(k - AHEAD, v_issue)

        @pl.when(takes_in)
        def _():
            static_block(b_in, arrived)
            gram(b_in)

        @pl.when(k >= 18)
        def _():
            z_send(25 - k)

        @pl.when((k <= 16) & (k >= 5))
        def _():
            z_send(24 - k)

        @pl.when(k == NB + 1)
        def _():
            t_layout()

        @pl.when(merges & (b_merge % 2 == c))
        def _():
            u_half(b_merge)
            merge(b_merge)

        return carry

    lax.fori_loop(0, NB + 1, step, 0)

    def update_1(g):
        weights(g, 1)
        _units(0, NU, lambda u: update(g, 1, u))

    def s_0(g):
        acc[g] = jnp.zeros((HALF, TILE), jnp.float32)
        _units(0, NU, lambda u: partial_s(g, 0, u))
        s_copy(g, 0).start()

    def gram_0(core):
        @pl.when(c == core)
        def _():
            arrived(0)
            gram(0)

    gram_0(0)
    update_1(0)
    gram_0(1)
    s_0(0)
    update_1(1)

    @pl.when(c == 1)
    def _():
        u_half(0)

    s_0(1)

    @pl.when(c == 0)
    def _():
        u_half(0)
        merge(0)

    def out_part(g, u, core):
        return out.at[pl.ds(u * HALF if isinstance(u, int) else pl.multiple_of(u * HALF, HALF), HALF), pl.ds(pl.multiple_of((2 * g + core) * HALF, HALF), HALF)]

    def z_part(g, u, rho):
        return zst.at[g, u, pl.ds(pl.multiple_of(rho * HALF, HALF), HALF), :]

    def out_local(g, u):
        return pltpu.make_async_copy(z_part(g, u, c), out_part(g, u, c), out_sem.at[g * NU + u])

    def out_sib(g, u):
        return remote(z_part(g, u, 1 - c), out_part(g, u, c), outs_sem.at[g * NU + u], outr_sem.at[g * NU + u], sib)

    def out_from_sib(g, u):
        part = out_part(g, u, 1 - c)
        return remote(part, part, outs_sem.at[g * NU + u], outr_sem.at[g * NU + u], sib)

    for g in range(2):
        weights(g, 0)

        def last(u, g=g):
            update(g, 0, u)
            zst[g, u] = zt[g, :, cols(u)].T

        def last_half(h, carry, g=g):
            for u in range(NU // 2):
                last(h * (NU // 2) + u)
            for u in range(NU // 2):
                out_local(g, h * (NU // 2) + u).start()
                out_sib(g, h * (NU // 2) + u).start()
            return carry

        lax.fori_loop(0, 2, last_half, 0)

    half_copy.wait_send()
    t_copy(0).wait_send()
    for b in range(NB):
        v_y(b, y).wait_send()
        v_own(b, c).wait_send()
        v_fwd(b, c).wait_send()
        z_chunk(b // 4, b % 4, x).wait_send()
    for g in range(2):
        for u in range(NU):
            out_local(g, u).wait()
            out_sib(g, u).wait_send()
            out_from_sib(g, u).wait_recv()


def solution(mesh):
    def local_run(z_cols, v_local, t_local):
        f32 = jnp.float32
        any_spec = pl.BlockSpec(memory_space=pl.ANY)
        dma = pltpu.SemaphoreType.DMA
        return pl.pallas_call(
            _kernel,
            out_shape=jax.ShapeDtypeStruct((ROWS, 4 * HALF), f32),
            in_specs=[any_spec] * 3,
            out_specs=any_spec,
            scratch_shapes=[
                pltpu.VMEM((2 * VU * HALF, TILE), f32),
                pltpu.VMEM((TILE, 2 * ROWS), f32),
                pltpu.VMEM((2, HALF, 2 * ROWS), f32),
                pltpu.VMEM((2, NU, TILE, HALF), f32),
                pltpu.VMEM((W, W, NB * 8), f32),
                pltpu.VMEM((NB * 8 * PITCH, W), f32),
                pltpu.VMEM((2, HALF, TILE), f32),
                pltpu.VMEM((2, 2, HALF, TILE), f32),
                pltpu.VMEM((HALF, TILE), f32),
                pltpu.VMEM((HALF, TILE), f32),
                pltpu.VMEM((2, HALF, HALF), f32),
                pltpu.VMEM((4, HALF, HALF), f32),
                pltpu.VMEM((HALF, HALF), f32),
                pltpu.VMEM((2, HALF, HALF), f32),
                pltpu.VMEM((4, TILE, TILE), f32),
                *[dma((NB,))] * 9,
                dma((2,)), dma((2, 2)), dma((2,)), dma((4,)), dma, dma, dma, dma((4,)), dma, *[dma((2 * NU,))] * 4,
            ],
            compiler_params=pltpu.CompilerParams(collective_id=0, has_side_effects=True, vmem_limit_bytes=63 * 2**20),
            name="backtransform",
        )(z_cols, v_local, t_local.transpose(1, 2, 0))

    return jax.shard_map(
        local_run,
        mesh=mesh,
        in_specs=(P("kpt", ("col", "row")), P(("kpt", "row"), "col"), P("kpt", None, None)),
        out_specs=P(("kpt", "row"), "col"),
        check_vma=False,
    )
```
